32 devices in a mesh: gx: 4 (over z), gy: 4 (over y, core), gz: 2 (over x).
Axes of the slice: x: 2, y: 2, z: 4, core: 2. Of those that a mesh axis runs over, the one named last changes fastest.
Arguments:
- positions: float32 [8, 4, 16, 3, 128], P(('gx', 'gz'), 'gy'), may hold values from 0 to 1
- masses: float32 [8, 4, 16, 128], P(('gx', 'gz'), 'gy'), may hold values from 0.2 to 2
- velocities: float32 [8, 4, 16, 3, 128], P(('gx', 'gz'), 'gy'), may hold values from -6 to 6
- tile_counts: int32 [8, 4, 16], P(('gx', 'gz'), 'gy'), may hold values from 32 to 128
- neighbour_list: int32 [8, 4, 16, 6], P(('gx', 'gz'), 'gy'), may hold values from 0 to 143, as said below
Outputs:
- kicked: float32 [8, 4, 16, 3, 128], P(('gx', 'gz'), 'gy')
The draws below stay inside these ranges and needn't reach their ends.
Inputs may be any that keep to these rules, and one draw needn't show every extreme that they name: `neighbour_list`: each entry is ((dx + 1) * 3 + dy + 1) * 16 + (t + dz) mod 16 for the tile t it belongs to, dx, dy, dz each in -1, 0, 1; the 6 entries of one tile name distinct shell tiles.
All inputs are finite; a program needn't handle non-finite values.
Results may differ from the reference program's by a relative error of at most 0.0003.
Values sent between devices are 32-bit elements; how exact they have to be, the bound alone decides.
A program may use at most 64 MiB of HBM per device.

```python
import math
import jax
import jax.numpy as jnp
from jax import lax

CX = 2
CY = 6
NZ = 1024
TZ = 16
NB = 6
GRID_X = 8
GRID_Y = 4
NX = 16
NY = 24


def draw_neighbour_list(key, part):
    scores = jax.random.randint(jax.random.fold_in(key, 17), (GRID_X, GRID_Y, TZ, 27), 0, 1 << 20) * 32 + jnp.arange(27, dtype=jnp.int32)
    chosen = jnp.argsort(scores, axis=-1)[..., :NB].astype(jnp.int32)
    groups = chosen // 3
    step_z = chosen % 3 - 1
    tile_row = jnp.arange(TZ, dtype=jnp.int32)[:, None]
    return (groups * TZ + (tile_row + step_z) % TZ).astype(jnp.int32)


def set_ends(result, own_key, smallest, high):
    shape = result.shape
    spot = [jax.random.randint(jax.random.fold_in(own_key, axis), (), 0, shape[axis]) for axis in range(len(shape))]
    result = result.at[tuple(spot)].set(smallest)
    longest = shape.index(max(shape))
    spot[longest] = (spot[longest] + 1) % shape[longest]
    return result.at[tuple(spot)].set(high)


def shard_levels(key, dims, split, least, high):
    factor_of = 1.0
    for axis_at, shards_of in split:
        draws = jax.random.uniform(jax.random.fold_in(jax.random.fold_in(key, 6), axis_at), (shards_of,), jnp.float32, least / len(split), high / len(split))
        factor_of = factor_of * jnp.repeat(jnp.exp(draws), dims[axis_at] // shards_of).reshape((-1,) + (1,) * (len(dims) - 1 - axis_at))
    return factor_of


def bell_draw(stream_key, dims, deviation, most, shards=(), held_as=jnp.bfloat16):
    result = deviation * jax.random.normal(stream_key, dims, jnp.float32)
    if shards:
        result = result * shard_levels(stream_key, dims, shards, -0.22, 0.18)
    return jnp.clip(result, -most, most).astype(held_as)


def setup_inputs(seed: int = 0) -> dict:
    keys = jax.random.split(jax.random.key(seed), 6)
    positions = jnp.clip(1.0 * jax.random.uniform(keys[0], (GRID_X, GRID_Y, TZ, 3, 128), jnp.float32) ** shard_levels(keys[0], (GRID_X, GRID_Y, TZ, 3, 128), ((0, 8), (1, 4)), -0.2, 0.2), 0.0, 1.0)
    masses = jnp.clip(jnp.exp(math.log(2.0) - 2.3025851 * jax.random.uniform(keys[1], (GRID_X, GRID_Y, TZ, 128), jnp.float32) ** shard_levels(keys[1], (GRID_X, GRID_Y, TZ, 128), ((0, 8), (1, 4)), -0.2, 0.2)), 0.2, 2.0)
    velocities = bell_draw(keys[2], (GRID_X, GRID_Y, TZ, 3, 128), 1.0, 6.0, ((0, 8), (1, 4)), jnp.float32)
    tile_counts = set_ends(jax.random.randint(keys[3], (GRID_X, GRID_Y, TZ), 32, 129), jax.random.fold_in(keys[3], 1), 32, 128).astype(jnp.int32)
    neighbour_list = draw_neighbour_list(jax.random.fold_in(keys[5], 71), 0)
    return {"positions": positions, "masses": masses, "velocities": velocities, "tile_counts": tile_counts, "neighbour_list": neighbour_list}


smoothing = 0.1
screening = 0.01
split_scale = 2.0
softening = 0.05
long_kick = 1.0
short_kick = 0.05


def wave_terms(length, first_index, extent):
    wavenum = (first_index + jnp.arange(extent, dtype=jnp.int32)).astype(jnp.float32)
    angles = wavenum * (2.0 * jnp.pi / length)
    return 4.0 * jnp.sin(0.5 * angles) ** 2, jnp.sin(angles)


def cloud_stencil(positions, cells_x, cells_y, cells_z, tiles):
    span = cells_z // tiles
    tile_row = jnp.arange(tiles, dtype=jnp.int32)[:, None]
    coord_x = positions[..., 0, :] * cells_x - 0.5
    base_x = jnp.clip(jnp.floor(coord_x), 0, cells_x - 2)
    frac_x = jnp.clip(coord_x - base_x, 0.0, 1.0)
    coord_y = positions[..., 1, :] * cells_y - 0.5
    base_y = jnp.clip(jnp.floor(coord_y), 0, cells_y - 2)
    frac_y = jnp.clip(coord_y - base_y, 0.0, 1.0)
    coord_z = (tile_row + positions[..., 2, :]) * span - 0.5
    base_z = jnp.floor(coord_z)
    frac_z = coord_z - base_z
    index_x = base_x.astype(jnp.int32)
    index_y = base_y.astype(jnp.int32)
    index_z = base_z.astype(jnp.int32) % cells_z
    cell_list = []
    weight_list = []
    for offset_x in (0, 1):
        for offset_y in (0, 1):
            for offset_z in (0, 1):
                weight_x = frac_x if offset_x else 1.0 - frac_x
                weight_y = frac_y if offset_y else 1.0 - frac_y
                weight_z = frac_z if offset_z else 1.0 - frac_z
                cell_list.append((((index_x + offset_x) * cells_y + index_y + offset_y) * cells_z + (index_z + offset_z) % cells_z).astype(jnp.int32))
                weight_list.append(weight_x * weight_y * weight_z)
    return jnp.stack(cell_list, axis=-2), jnp.stack(weight_list, axis=-2)


def pair_accel(receivers, sources, shifts):
    parts = []
    for comp in range(3):
        parts.append(shifts[:, :, comp, None, None] + sources[:, :, comp, None, :] - receivers[:, None, comp, :, None])
    square = parts[0] * parts[0] + parts[1] * parts[1] + parts[2] * parts[2]
    strength = sources[:, :, 3, None, :] * jnp.exp(-square / split_scale) * (square + softening) ** -1.5
    return jnp.stack([jnp.sum(strength * parts[comp], axis=(1, 3)) for comp in range(3)], axis=1)


def reference(positions, masses, velocities, tile_counts, neighbour_list):
    slot_index = jnp.arange(128, dtype=jnp.int32)
    live_mask = (slot_index < tile_counts[..., None]).astype(jnp.float32)
    mass_live = masses * live_mask
    cell_index, cloud_weights = cloud_stencil(positions, CX, CY, NZ, TZ)
    row_index = jnp.arange(GRID_X, dtype=jnp.int32)[:, None, None, None, None]
    column_index = jnp.arange(GRID_Y, dtype=jnp.int32)[None, :, None, None, None]
    cell_x = row_index * CX + cell_index // (CY * NZ)
    cell_y = column_index * CY + (cell_index // NZ) % CY
    flat_cells = ((cell_x * NY + cell_y) * NZ + cell_index % NZ).astype(jnp.int32)
    amounts = cloud_weights * mass_live[:, :, :, None, :]
    density = jax.ops.segment_sum(amounts.reshape(-1), flat_cells.reshape(-1), num_segments=NX * NY * NZ).reshape(NX, NY, NZ)
    spectrum = jnp.fft.fftn(density)
    kappa_x, sine_x = wave_terms(NX, 0, NX)
    kappa_y, sine_y = wave_terms(NY, 0, NY)
    kappa_z, sine_z = wave_terms(NZ, 0, NZ)
    kappa_sum = kappa_x[:, None, None] + kappa_y[None, :, None] + kappa_z[None, None, :]
    potential = spectrum * (-jnp.exp(-smoothing * kappa_sum) / (kappa_sum + screening))
    sine_list = (sine_x[:, None, None], sine_y[None, :, None], sine_z[None, None, :])
    picked = []
    for sine_part in sine_list:
        force_field = jnp.real(jnp.fft.ifftn(-1j * sine_part * potential)).reshape(-1)
        picked.append(jnp.sum(cloud_weights * force_field[flat_cells], axis=3))
    long_accel = jnp.stack(picked, axis=3)
    packed = jnp.concatenate([positions, mass_live[:, :, :, None, :]], axis=3)
    shell = jnp.stack([jnp.roll(packed, (-step_x, -step_y), axis=(0, 1)) for step_x in (-1, 0, 1) for step_y in (-1, 0, 1)])
    groups = neighbour_list // TZ
    layers = neighbour_list % TZ
    rows_four = jnp.arange(GRID_X, dtype=jnp.int32)[:, None, None, None]
    columns_four = jnp.arange(GRID_Y, dtype=jnp.int32)[None, :, None, None]
    sources = shell[groups, rows_four, columns_four, layers]
    tile_row = jnp.arange(TZ, dtype=jnp.int32)[:, None]
    shifts = jnp.stack([groups // 3 - 1, groups % 3 - 1, (layers - tile_row + 1) % TZ - 1], axis=-1).astype(jnp.float32)
    tile_total = GRID_X * GRID_Y * TZ
    listed = neighbour_list.shape[-1]
    short_accel = lax.map(lambda pieces: pair_accel(*pieces), (positions.reshape(tile_total // 16, 16, 3, 128), sources.reshape(tile_total // 16, 16, listed, 4, 128), shifts.reshape(tile_total // 16, 16, listed, 3)))
    short_accel = short_accel.reshape(GRID_X, GRID_Y, TZ, 3, 128)
    return velocities + live_mask[:, :, :, None, :] * (long_kick * long_accel + short_kick * short_accel)
```

```python
import functools
import math

import jax
import jax.numpy as jnp
import numpy as np
from jax import lax
from jax.experimental import pallas as pl
from jax.experimental.pallas import tpu as pltpu
from jax.sharding import PartitionSpec as P

CX = 2
CY = 6
NZ = 1024


smoothing = 0.1
screening = 0.01
split_scale = 2.0
softening = 0.05
long_kick = 1.0
short_kick = 0.05
highest = lax.Precision.HIGHEST


def padded(cells, sides, width):
    for axis, dim in sides:
        count = lax.axis_size(axis)
        head = lax.slice_in_dim(cells, 0, width, axis=dim)
        tail = lax.slice_in_dim(cells, cells.shape[dim] - width, cells.shape[dim], axis=dim)
        cells = jnp.concatenate(
            [
                lax.ppermute(tail, axis, [(i, (i + 1) % count) for i in range(count)]),
                cells,
                lax.ppermute(head, axis, [((i + 1) % count, i) for i in range(count)]),
            ],
            axis=dim,
        )
    return cells


def wave_terms(length, first_index, extent):
    wavenum = (first_index + jnp.arange(extent, dtype=jnp.int32)).astype(jnp.float32)
    angles = wavenum * (2.0 * jnp.pi / length)
    return (4.0 * jnp.sin(0.5 * angles) ** 2, jnp.sin(angles))


def cloud_stencil(positions, cells_x, cells_y, cells_z, tiles):
    span = cells_z // tiles
    tile_row = jnp.arange(tiles, dtype=jnp.int32)[:, None]
    coord_x = positions[..., 0, :] * cells_x - 0.5
    base_x = jnp.clip(jnp.floor(coord_x), 0, cells_x - 2)
    frac_x = jnp.clip(coord_x - base_x, 0.0, 1.0)
    coord_y = positions[..., 1, :] * cells_y - 0.5
    base_y = jnp.clip(jnp.floor(coord_y), 0, cells_y - 2)
    frac_y = jnp.clip(coord_y - base_y, 0.0, 1.0)
    coord_z = (tile_row + positions[..., 2, :]) * span - 0.5
    base_z = jnp.floor(coord_z)
    frac_z = coord_z - base_z
    index_x = base_x.astype(jnp.int32)
    index_y = base_y.astype(jnp.int32)
    index_z = base_z.astype(jnp.int32) % cells_z
    cell_list = []
    weight_list = []
    for offset_x in (0, 1):
        for offset_y in (0, 1):
            for offset_z in (0, 1):
                weight_x = frac_x if offset_x else 1.0 - frac_x
                weight_y = frac_y if offset_y else 1.0 - frac_y
                weight_z = frac_z if offset_z else 1.0 - frac_z
                cell_list.append(
                    ((index_x + offset_x) * cells_y + index_y + offset_y) * cells_z
                    + (index_z + offset_z) % cells_z
                )
                weight_list.append(weight_x * weight_y * weight_z)
    return (jnp.stack(cell_list, axis=-2), jnp.stack(weight_list, axis=-2))


def pair_accel(receivers, sources, shifts):
    parts = []
    for comp in range(3):
        parts.append(
            shifts[:, :, comp, None, None]
            + sources[:, :, comp, None, :]
            - receivers[:, None, comp, :, None]
        )
    square = parts[0] * parts[0] + parts[1] * parts[1] + parts[2] * parts[2]
    strength = (
        sources[:, :, 3, None, :] * jnp.exp(-square / split_scale) * (square + softening) ** (-1.5)
    )
    return jnp.stack([jnp.sum(strength * parts[comp], axis=(1, 3)) for comp in range(3)], axis=1)


def split_length(length):
    divisor = 1
    for factor in range(1, math.isqrt(length) + 1):
        if length % factor == 0:
            divisor = factor
    return divisor


def dft_table(length):
    indices = jnp.arange(length, dtype=jnp.int32)
    phases = indices[:, None] * indices[None, :] % length
    angles = phases.astype(jnp.float32) * (2.0 * jnp.pi / length)
    return (jnp.cos(angles), jnp.sin(angles))


def twiddle_table(outer, inner):
    length = outer * inner
    phases = (
        jnp.arange(outer, dtype=jnp.int32)[:, None]
        * jnp.arange(inner, dtype=jnp.int32)[None, :]
        % length
    )
    angles = phases.astype(jnp.float32) * (2.0 * jnp.pi / length)
    return (jnp.cos(angles), jnp.sin(angles))


def complex_mix(real, imag, cosine, sine_table, sign, form):
    real_cos = jnp.einsum(form, real, cosine, precision=highest)
    real_sin = jnp.einsum(form, real, sine_table, precision=highest)
    imag_cos = jnp.einsum(form, imag, cosine, precision=highest)
    imag_sin = jnp.einsum(form, imag, sine_table, precision=highest)
    return (real_cos - sign * imag_sin, imag_cos + sign * real_sin)


def transform_last(real, imag, sign):
    length = real.shape[-1]
    outer = split_length(length)
    inner = length // outer
    leading = real.shape[:-1]
    real = real.reshape(leading + (outer, inner))
    imag = imag.reshape(leading + (outer, inner))
    cos_outer, sin_outer = dft_table(outer)
    real, imag = complex_mix(real, imag, cos_outer, sin_outer, sign, "...pq,pk->...kq")
    turn_cos, turn_sin = twiddle_table(outer, inner)
    real, imag = (
        real * turn_cos - sign * imag * turn_sin,
        imag * turn_cos + sign * real * turn_sin,
    )
    cos_inner, sin_inner = dft_table(inner)
    real, imag = complex_mix(real, imag, cos_inner, sin_inner, sign, "...kq,qm->...mk")
    return (real.reshape(leading + (length,)), imag.reshape(leading + (length,)))


def transform_axis(fields, axis, sign):
    real = jnp.moveaxis(fields[:, 0], axis, -1)
    imag = jnp.moveaxis(fields[:, 1], axis, -1)
    real, imag = transform_last(real, imag, sign)
    return jnp.stack([jnp.moveaxis(real, -1, axis), jnp.moveaxis(imag, -1, axis)], axis=1)


def rotate(fields, factor):
    return jnp.stack([factor * fields[:, 1], -factor * fields[:, 0]], axis=1)


def shards(positions, masses, velocities, tile_counts, neighbour_list):
    tiles = positions.shape[2]
    listed = neighbour_list.shape[3]
    slot_index = jnp.arange(128, dtype=jnp.int32)
    live_mask = (slot_index < tile_counts[..., None]).astype(jnp.float32)
    mass_live = masses * live_mask
    packed = jnp.concatenate([positions, mass_live[:, :, :, None, :]], axis=3)
    shell = padded(packed, ((("gx", "gz"), 0), ("gy", 1)), 1)
    cell_index, cloud_weights = cloud_stencil(positions, CX, CY, NZ, tiles)
    amounts = cloud_weights * mass_live[:, :, :, None, :]
    density = jax.ops.segment_sum(
        amounts.reshape(-1), cell_index.reshape(-1), num_segments=CX * CY * NZ
    ).reshape(CX, CY, NZ)
    spectrum = jnp.stack([density, jnp.zeros_like(density)], axis=0)[None]
    spectrum = transform_axis(spectrum, 3, -1.0)
    spectrum = lax.all_to_all(spectrum, "gy", split_axis=4, concat_axis=3, tiled=True)
    span_y = spectrum.shape[3]
    spectrum = transform_axis(spectrum, 2, -1.0)
    spectrum = lax.all_to_all(spectrum, ("gx", "gz"), split_axis=3, concat_axis=2, tiled=True)
    span_x = spectrum.shape[2]
    spectrum = transform_axis(spectrum, 1, -1.0)
    block_y = spectrum.shape[3]
    block_z = spectrum.shape[4]
    kappa_x, sine_x = wave_terms(span_x, 0, span_x)
    kappa_y, sine_y = wave_terms(span_y, lax.axis_index(("gx", "gz")) * block_y, block_y)
    kappa_z, sine_z = wave_terms(NZ, lax.axis_index("gy") * block_z, block_z)
    kappa_sum = kappa_x[:, None, None] + kappa_y[None, :, None] + kappa_z[None, None, :]
    potential = spectrum * (-jnp.exp(-smoothing * kappa_sum) / (kappa_sum + screening))
    fields = jnp.concatenate([rotate(potential, sine_x[:, None, None]), potential], axis=0)
    fields = transform_axis(fields, 1, 1.0) / span_x
    fields = lax.all_to_all(fields, ("gx", "gz"), split_axis=2, concat_axis=3, tiled=True)
    whole_sine_y = wave_terms(span_y, 0, span_y)[1]
    fields = jnp.concatenate(
        [fields[0:1], rotate(fields[1:2], whole_sine_y[None, :, None]), fields[1:2]], axis=0
    )
    fields = transform_axis(fields, 2, 1.0) / span_y
    fields = lax.all_to_all(fields, "gy", split_axis=3, concat_axis=4, tiled=True)
    whole_sine_z = wave_terms(NZ, 0, NZ)[1]
    fields = jnp.concatenate(
        [fields[0:2], rotate(fields[2:3], whole_sine_z[None, None, :])], axis=0
    )
    fields = transform_axis(fields, 3, 1.0) / NZ
    forces = fields[:, 0]
    flat_forces = forces.reshape(3, -1)
    picked = flat_forces[:, cell_index]
    long_accel = jnp.moveaxis(jnp.sum(cloud_weights[None] * picked, axis=4), 0, 3)
    flat_shell = shell.reshape(9 * tiles, 4, 128)
    own_list = neighbour_list[0, 0]
    sources = flat_shell[own_list]
    groups = own_list // tiles
    layers = own_list % tiles
    tile_row = jnp.arange(tiles, dtype=jnp.int32)[:, None]
    shifts = jnp.stack(
        [groups // 3 - 1, groups % 3 - 1, (layers - tile_row + 1) % tiles - 1], axis=-1
    ).astype(jnp.float32)
    short_accel = lax.map(
        lambda pieces: pair_accel(*pieces),
        (
            positions[0, 0].reshape(tiles, 1, 3, 128),
            sources.reshape(tiles, 1, listed, 4, 128),
            shifts.reshape(tiles, 1, listed, 3),
        ),
    )
    short_accel = short_accel.reshape(1, 1, tiles, 3, 128)
    return velocities + live_mask[:, :, :, None, :] * (
        long_kick * long_accel + short_kick * short_accel
    )


MESH = pl.DeviceIdType.MESH
LOGICAL = pl.DeviceIdType.LOGICAL
f32 = jnp.float32
bf16 = jnp.bfloat16


def halves(x):
    high = x.astype(bf16)
    return high, (x - high.astype(f32)).astype(bf16)


def dot3(a, b, dims=((1,), (0,))):
    dot = functools.partial(
        lax.dot_general, dimension_numbers=(dims, ((), ())), preferred_element_type=f32
    )
    return dot(a[0], b[0]) + dot(a[1], b[0]) + dot(a[0], b[1])


def hat(coord, cell):
    return jnp.maximum(0.0, 1.0 - jnp.abs(coord - cell))


def np_halves(table):
    table = jnp.asarray(np.asarray(table, np.float32))
    return jnp.stack(halves(table))


def tables(size_x, size_y, size_z, tiles):
    rows, cols = size_x * size_z, size_y
    count = rows * cols
    modes = NZ // 2 // count
    pack = 128 // (2 * modes)
    span = NZ // tiles
    lane = np.arange(NZ)
    block, inside = lane // (2 * modes), lane % (2 * modes)
    imag = inside >= modes
    mode = block * modes + inside % modes
    nyquist = (mode == 0) & imag
    cells = np.arange(128) - 1
    angle = 2 * np.pi * ((cells[:, None] * mode[None, :]) % NZ) / NZ
    wave = np.where(imag[None], -np.sin(angle), np.cos(angle))
    wave = np.where(nyquist[None], np.cos(np.pi * (cells % 2))[:, None], wave)
    wave = np.where((cells <= span)[:, None], wave, 0.0)
    groups = NZ // 128
    forward = wave.reshape(128, groups, 128).transpose(1, 0, 2)
    scale = np.where(mode == 0, 1.0, 2.0) / (NZ * rows * CX * cols * CY)
    inverse = (wave * scale[None]).T
    turn = 2 * np.pi * ((mode[None] * np.arange(tiles)[:, None] * span) % NZ) / NZ
    cosine = np.cos(turn)
    sine = np.where(imag[None], 1.0, -1.0) * np.sin(turn)
    turns = np.stack([cosine, sine]).reshape(2, tiles, groups, 128)
    turns = turns.transpose(0, 2, 1, 3).reshape(2 * groups, tiles, 128)
    index = np.arange(3 * count * 4)
    device, row = index // 4 % count, index // (4 * count) * 4 + index % 4
    real = row < CX * CY
    place_x = device // (size_y * size_z) * size_z + device % size_z
    place_y = device // size_z % size_y
    nx, ny = rows * CX, cols * CY
    x = np.where(real, place_x * CX + row // CY, 0)
    y = np.where(real, place_y * CY + row % CY, 0)
    phase = (x[:, None] * x[None] * ny + y[:, None] * y[None] * nx) % (nx * ny)
    phase = 2 * np.pi * phase / (nx * ny)
    both = (real[:, None] & real[None]).astype(np.float64)
    plane = np.concatenate([np.cos(phase) * both, np.sin(phase) * both])
    lanes = np.zeros((8, 3 * count * 4))
    lanes[0] = 4 * np.sin(np.pi * x / nx) ** 2 + 4 * np.sin(np.pi * y / ny) ** 2
    lanes[1] = np.sin(2 * np.pi * x / nx)
    lanes[2] = np.sin(2 * np.pi * y / ny)
    return (
        np_halves(forward),
        np_halves(inverse),
        np_halves(plane),
        jnp.asarray(turns, f32),
        jnp.asarray(lanes, f32),
    )


def kick_kernel(
    sizes,
    pos_ref, mass_ref, vel_ref, turns_ref, lanes_ref, counts_ref, list_ref,
    forward_hbm, inverse_hbm, plane_hbm,
    out_ref,
    forward_ref, inverse_ref, plane_ref, shell_ref, rho_ref, spec_ref, got_ref,
    back_ref, home_ref, line_ref, swap_ref, field_ref, spread_ref, accum_ref, short_ref,
    table_sem, halo_send, halo_recv, out_send, out_recv, back_send, back_recv,
):
    size_x, size_y, size_z, tiles, listed = sizes
    rows, cols = size_x * size_z, size_y
    count = rows * cols
    modes = NZ // 2 // count
    width = 2 * modes
    pack = 128 // width
    groups = NZ // 128
    span = NZ // tiles
    gx, gy, gz = lax.axis_index("gx"), lax.axis_index("gy"), lax.axis_index("gz")
    row, col = gx * size_z + gz, gy
    me = (gx * size_y + gy) * size_z + gz

    def place(r, c):
        return (r // size_z, c, r % size_z)

    def other(i):
        d = me + i
        return jnp.where(d >= count, d - count, d)

    barrier = pltpu.get_barrier_semaphore()

    def greet(i, carry):
        pl.semaphore_signal(
            barrier, inc=1, device_id=other(i), device_id_type=LOGICAL
        )
        return carry

    lax.fori_loop(1, count, greet, 0)
    table_copies = [
        pltpu.make_async_copy(a, b, table_sem.at[i])
        for i, (a, b) in enumerate(
            ((forward_hbm, forward_ref), (plane_hbm, plane_ref), (inverse_hbm, inverse_ref))
        )
    ]
    for copy in table_copies:
        copy.start()

    slot = lax.broadcasted_iota(jnp.int32, (1, 128), 1)
    row_of = lax.broadcasted_iota(jnp.int32, (16, 128), 0)
    cell_x = (row_of // CY).astype(f32)
    cell_y = (row_of % CY).astype(f32)
    cell_z = lax.broadcasted_iota(jnp.int32, (128, 128), 0).astype(f32) - 1.0

    def weights(t):
        spot = [pos_ref[comp, pl.ds(t, 1), :] for comp in range(3)]
        coord_x = jnp.clip(spot[0] * CX - 0.5, 0.0, CX - 1.0)
        coord_y = jnp.clip(spot[1] * CY - 0.5, 0.0, CY - 1.0)
        start = jnp.asarray(t, jnp.int32).astype(f32)
        coord_z = (start + spot[2]) * span - 0.5 - start * span
        plane = hat(coord_x, cell_x) * hat(coord_y, cell_y)
        return plane, hat(coord_z, cell_z)

    own = 4 * tiles

    def gather(t, carry):
        live = (slot < counts_ref[t]).astype(f32)
        for comp in range(3):
            shell_ref[own + t, comp:comp + 1, :] = pos_ref[comp, pl.ds(t, 1), :]
        shell_ref[own + t, 3:4, :] = mass_ref[pl.ds(t, 1), :] * live
        return carry

    lax.fori_loop(0, tiles, gather, 0, unroll=4)
    def deposit(t, carry):
        mass = shell_ref[own + t, 3:4, :]
        plane, wz = weights(t)
        rho_ref[pl.ds(pl.multiple_of(t * 16, 16), 16), :] = dot3(
            halves(plane * mass), halves(wz), ((1,), (1,))
        )
        return carry

    lax.fori_loop(0, tiles, deposit, 0, unroll=4)
    def swapped(x):
        lane = lax.broadcasted_iota(jnp.int32, x.shape, 1)
        return jnp.where(
            (lane % width) < modes, pltpu.roll(x, 128 - modes, 1), pltpu.roll(x, modes, 1)
        )

    quarter = lax.broadcasted_iota(jnp.int32, (8, 128), 1) // width

    table_copies[0].wait()
    rho = halves(rho_ref[...])

    def transform(g, carry):
        wide = dot3(rho, (forward_ref[0, g], forward_ref[1, g]))
        cosine, sine = turns_ref[g], turns_ref[groups + g]
        straight = jnp.zeros((16, 128), f32)
        crossed = jnp.zeros((16, 128), f32)
        for t in range(tiles):
            part = wide[t * 16:(t + 1) * 16]
            straight = straight + part * cosine[t:t + 1]
            crossed = crossed + part * sine[t:t + 1]
        lines = straight + swapped(crossed)
        thirds = (lines[0:8], pltpu.roll(lines[0:8], 4, 0), lines[8:16])
        for i in range(pack):
            packed = jnp.zeros((8, 128), f32)
            for a, third in enumerate(thirds):
                shift = (a - i) * width % 128
                piece = pltpu.roll(third, shift, 1) if shift else third
                packed = jnp.where(quarter == a, piece, packed)
            spec_ref[g * pack + i] = packed[0:4]
        return carry

    lax.fori_loop(0, groups, transform, 0)

    def out_copy(d):
        return pltpu.make_async_remote_copy(
            src_ref=spec_ref.at[d],
            dst_ref=got_ref.at[me],
            send_sem=out_send,
            recv_sem=out_recv,
            device_id=d,
            device_id_type=LOGICAL,
        )

    def back_copy(d):
        return pltpu.make_async_remote_copy(
            src_ref=back_ref.at[d],
            dst_ref=home_ref.at[me],
            send_sem=back_send,
            recv_sem=back_recv,
            device_id=d,
            device_id_type=LOGICAL,
        )

    def start_all(make):
        def step(i, carry):
            make(other(i)).start()
            return carry

        lax.fori_loop(1, count, step, 0)

    def wait_all(ref, sem):
        rest = ref.at[pl.ds(0, count - 1)]
        pltpu.make_async_copy(rest, rest, sem).wait()

    pl.semaphore_wait(barrier, count - 1)
    start_all(out_copy)
    halos = []
    for step_x in (-1, 0, 1):
        for step_y in (-1, 0, 1):
            if step_x == 0 and step_y == 0:
                continue
            slot_there = (1 - step_x) * 3 + 1 - step_y
            halos.append(
                pltpu.make_async_remote_copy(
                    src_ref=shell_ref.at[pl.ds(own, tiles)],
                    dst_ref=shell_ref.at[pl.ds(slot_there * tiles, tiles)],
                    send_sem=halo_send.at[slot_there],
                    recv_sem=halo_recv.at[slot_there],
                    device_id=place((row + step_x + rows) % rows, (col + step_y + cols) % cols),
                    device_id_type=MESH,
                )
            )
    for copy in halos:
        copy.start()
    got_ref[me] = spec_ref[me]

    ones = jnp.ones((8, 128), bf16)
    block = 32

    def spread(t, carry):
        for comp in range(3):
            spread_ref[t, comp] = jnp.transpose(
                jnp.broadcast_to(pos_ref[comp, pl.ds(t, 1), :], (128, 128)), (1, 0)
            )
        return carry

    lax.fori_loop(0, tiles, spread, 0)

    def pairs(t, carry):
        sources = []
        for n in range(listed):
            entry = list_ref[n, 0, t]
            group, layer = entry // tiles, entry % tiles
            away = (layer - t + 1 + tiles) % tiles - 1
            tile = shell_ref[entry]
            sources.append(
                (
                    tile[0:1] + (group // 3 - 1).astype(f32),
                    tile[1:2] + (group % 3 - 1).astype(f32),
                    tile[2:3] + away.astype(f32),
                    tile[3:4],
                )
            )
        for b in range(128 // block):
            here = [spread_ref[t, comp, b * block:(b + 1) * block, :] for comp in range(3)]
            totals = [jnp.zeros((block, 128), f32) for comp in range(3)]
            for source in sources:
                parts = [source[comp] - here[comp] for comp in range(3)]
                square = parts[0] * parts[0] + parts[1] * parts[1] + parts[2] * parts[2]
                root = lax.rsqrt(square + softening)
                strength = source[3] * jnp.exp2(square * (-1.0 / (split_scale * math.log(2.0)))) * (root * root * root)
                totals = [totals[comp] + strength * parts[comp] for comp in range(3)]
            for comp in range(3):
                accum_ref[comp * 128 + b * block:comp * 128 + (b + 1) * block, :] = totals[comp]
        high, low = halves(accum_ref[...])
        dot = functools.partial(
            lax.dot_general,
            dimension_numbers=(((1,), (1,)), ((), ())),
            preferred_element_type=f32,
        )
        sums = dot(ones, high) + dot(ones, low)
        for comp in range(3):
            short_ref[comp, pl.ds(t, 1), :] = sums[0:1, comp * 128:(comp + 1) * 128]
        return carry

    depth = 3 * count * 4
    mode_of = lax.broadcasted_iota(jnp.int32, (modes, depth), 0) + me * modes
    packed = mode_of == 0
    keep = jnp.where(packed, 0.0, 1.0)
    kappa_xy, sine_x, sine_y = (lanes_ref[i:i + 1, :] for i in range(3))

    def green(which):
        kappa = kappa_xy + 4.0 * jnp.sin(which.astype(f32) * (jnp.pi / NZ)) ** 2
        return -jnp.exp(-smoothing * kappa) / (kappa + screening)

    g1 = green(mode_of)
    g2 = green(jnp.where(packed, NZ // 2, mode_of))
    sine_z = jnp.sin(mode_of.astype(f32) * (2.0 * jnp.pi / NZ))
    sine_z = jnp.concatenate([sine_z, sine_z], axis=0)
    wait_all(got_ref, out_recv)
    table_copies[1].wait()
    turned = jnp.transpose(got_ref[...].reshape(count * 4, 128), (1, 0))
    mine = halves(
        jnp.concatenate([turned[a * width:(a + 1) * width] for a in range(3)], axis=1)
    )
    by_cos = dot3(mine, (plane_ref[0, :depth], plane_ref[1, :depth]))
    by_sin = dot3(mine, (plane_ref[0, depth:], plane_ref[1, depth:]))
    cr, ci = by_cos[:modes], by_cos[modes:]
    sr, si = by_sin[:modes], by_sin[modes:]
    for_cos = jnp.concatenate([g1 * (keep * ci - sr), -g2 * (keep * cr + si)], axis=0)
    for_sin = jnp.concatenate([g1 * (cr + keep * si), g2 * (ci - keep * sr)], axis=0)
    stacked_cos = jnp.concatenate([for_cos * sine_x, for_cos * sine_y, for_cos * sine_z], axis=0)
    stacked_sin = jnp.concatenate([for_sin * sine_x, for_sin * sine_y, for_sin * sine_z], axis=0)
    result = dot3(halves(stacked_cos), (plane_ref[0, :depth], plane_ref[1, :depth])) + dot3(
        halves(stacked_sin), (plane_ref[0, depth:], plane_ref[1, depth:])
    )
    result = jnp.concatenate([result, jnp.zeros((128 - 3 * width, depth), f32)], axis=0)
    for a in range(3):
        third = jnp.transpose(result[:, a * count * 4:(a + 1) * count * 4], (1, 0))
        back_ref[:, a] = third.reshape(count, 4, 128)
    start_all(back_copy)
    home_ref[me] = back_ref[me]

    for copy in halos:
        copy.wait_recv()
    lax.fori_loop(0, tiles, pairs, 0, unroll=2)
    wait_all(home_ref, back_recv)
    table_copies[2].wait()

    near = quarter[0:4]
    for g in range(groups):
        for a in range(3):
            blocks = [home_ref[g * pack + i, a] for i in range(pack)]
            for f in range(3):
                merged = jnp.zeros((4, 128), f32)
                for i in range(pack):
                    shift = ((i - f) * width) % 128
                    piece = pltpu.roll(blocks[i], shift, 1) if shift else blocks[i]
                    merged = jnp.where(near == i, piece, merged)
                line_ref[g, f * 16 + a * 4:f * 16 + (a + 1) * 4, :] = merged
        for f in range(3):
            line_ref[g, f * 16 + 12:(f + 1) * 16, :] = jnp.zeros((4, 128), f32)
        swap_ref[g] = swapped(line_ref[g])

    together = 4

    def invert(q, carry):
        pieces = []
        total = jnp.zeros((together * 48, 128), f32)
        for g in range(groups):
            line, swap = line_ref[g], swap_ref[g]
            turned = []
            for i in range(together):
                t = q * together + i
                turned.append(
                    line * turns_ref[g, pl.ds(t, 1), :]
                    + swap * turns_ref[groups + g, pl.ds(t, 1), :]
                )
            part = halves(jnp.concatenate(turned, axis=0))
            at = slice(g * 128, (g + 1) * 128)
            total = total + dot3(part, (inverse_ref[0, at], inverse_ref[1, at]))
        field_ref[pl.ds(q * together, together)] = total.reshape(together, 48, 128)
        return carry

    lax.fori_loop(0, tiles // together, invert, 0)

    def interpolate(t, carry):
        plane, wz = weights(t)
        here = dot3(halves(field_ref[t]), halves(wz))
        live = (slot < counts_ref[t]).astype(f32)
        for f in range(3):
            pull = jnp.sum(here[f * 16:(f + 1) * 16] * plane, axis=0, keepdims=True)
            at = (f, pl.ds(t, 1), slice(None))
            out_ref[at] = vel_ref[at] + live * (long_kick * pull + short_kick * short_ref[at])
        return carry

    lax.fori_loop(0, tiles, interpolate, 0, unroll=4)
    for copy in halos:
        copy.wait_send()
    wait_all(got_ref, out_send)
    wait_all(home_ref, back_send)


def fused_shards(sizes, positions, masses, velocities, tile_counts, neighbour_list):
    size_x, size_y, size_z, tiles, listed = sizes
    rows, cols = size_x * size_z, size_y
    count = rows * cols
    groups = NZ // 128
    with jax.ensure_compile_time_eval():
        forward, inverse, plane, turns, lanes = tables(size_x, size_y, size_z, tiles)
    vmem = pl.BlockSpec(memory_space=pltpu.VMEM)
    smem = pl.BlockSpec(memory_space=pltpu.SMEM)
    anywhere = pl.BlockSpec(memory_space=pl.ANY)
    dma = pltpu.SemaphoreType.DMA
    kicked = pl.pallas_call(
        functools.partial(kick_kernel, sizes),
        out_shape=pltpu.VMEM((3, tiles, 128), f32),
        in_specs=[vmem] * 5 + [smem] * 2 + [anywhere] * 3,
        out_specs=vmem,
        scratch_shapes=[
            pltpu.VMEM(forward.shape, bf16),
            pltpu.VMEM(inverse.shape, bf16),
            pltpu.VMEM(plane.shape, bf16),
            pltpu.VMEM((9 * tiles, 4, 128), f32),
            pltpu.VMEM((tiles * 16, 128), f32),
            pltpu.VMEM((count, 4, 128), f32),
            pltpu.VMEM((count, 4, 128), f32),
            pltpu.VMEM((count, 3, 4, 128), f32),
            pltpu.VMEM((count, 3, 4, 128), f32),
            pltpu.VMEM((groups, 48, 128), f32),
            pltpu.VMEM((groups, 48, 128), f32),
            pltpu.VMEM((tiles, 48, 128), f32),
            pltpu.VMEM((tiles, 3, 128, 128), f32),
            pltpu.VMEM((384, 128), f32),
            pltpu.VMEM((3, tiles, 128), f32),
            dma((3,)),
            dma((9,)),
            dma((9,)),
            dma,
            dma,
            dma,
            dma,
        ],
        compiler_params=pltpu.CompilerParams(collective_id=0, has_side_effects=True),
        name="kick",
    )(
        jnp.transpose(positions[0, 0], (1, 0, 2)),
        masses.reshape(tiles, 128),
        jnp.transpose(velocities[0, 0], (1, 0, 2)),
        turns,
        lanes,
        tile_counts.reshape(tiles),
        jnp.transpose(neighbour_list[0], (2, 0, 1)),
        forward,
        inverse,
        plane,
    )
    return jnp.transpose(kicked, (1, 0, 2))[None, None]


def fits(sizes):
    size_x, size_y, size_z, tiles, listed = sizes
    count = size_x * size_y * size_z
    if (NZ // 2) % count or count * 4 % 128 or CX * CY > 12 or count > 64:
        return False
    modes = NZ // 2 // count
    return modes == 16 and tiles % 4 == 0


def solution(mesh):
    placed = (
        P(("gx", "gz"), "gy", None, None, None),
        P(("gx", "gz"), "gy", None, None),
        P(("gx", "gz"), "gy", None, None, None),
        P(("gx", "gz"), "gy", None),
        P(("gx", "gz"), "gy", None, None),
    )

    def local(positions, masses, velocities, tile_counts, neighbour_list):
        sizes = tuple(mesh.shape[axis] for axis in ("gx", "gy", "gz"))
        sizes = sizes + (positions.shape[2], neighbour_list.shape[3])
        part = functools.partial(fused_shards, sizes) if fits(sizes) else shards
        return part(positions, masses, velocities, tile_counts, neighbour_list)

    return jax.shard_map(
        local,
        mesh=mesh,
        in_specs=placed,
        out_specs=P(("gx", "gz"), "gy", None, None, None),
        check_vma=False,
    )
```

```python
import contextlib
import functools
import math

import jax
import jax.numpy as jnp
import numpy as np
from jax import lax
from jax.experimental import pallas as pl
from jax.experimental.pallas import tpu as pltpu
from jax.sharding import PartitionSpec as P

CX = 2
CY = 6
NZ = 1024


smoothing = 0.1
screening = 0.01
split_scale = 2.0
softening = 0.05
long_kick = 1.0
short_kick = 0.05
highest = lax.Precision.HIGHEST


def padded(cells, sides, width):
    for axis, dim in sides:
        count = lax.axis_size(axis)
        head = lax.slice_in_dim(cells, 0, width, axis=dim)
        tail = lax.slice_in_dim(cells, cells.shape[dim] - width, cells.shape[dim], axis=dim)
        cells = jnp.concatenate(
            [
                lax.ppermute(tail, axis, [(i, (i + 1) % count) for i in range(count)]),
                cells,
                lax.ppermute(head, axis, [((i + 1) % count, i) for i in range(count)]),
            ],
            axis=dim,
        )
    return cells


def wave_terms(length, first_index, extent):
    wavenum = (first_index + jnp.arange(extent, dtype=jnp.int32)).astype(jnp.float32)
    angles = wavenum * (2.0 * jnp.pi / length)
    return (4.0 * jnp.sin(0.5 * angles) ** 2, jnp.sin(angles))


def cloud_stencil(positions, cells_x, cells_y, cells_z, tiles):
    span = cells_z // tiles
    tile_row = jnp.arange(tiles, dtype=jnp.int32)[:, None]
    coord_x = positions[..., 0, :] * cells_x - 0.5
    base_x = jnp.clip(jnp.floor(coord_x), 0, cells_x - 2)
    frac_x = jnp.clip(coord_x - base_x, 0.0, 1.0)
    coord_y = positions[..., 1, :] * cells_y - 0.5
    base_y = jnp.clip(jnp.floor(coord_y), 0, cells_y - 2)
    frac_y = jnp.clip(coord_y - base_y, 0.0, 1.0)
    coord_z = (tile_row + positions[..., 2, :]) * span - 0.5
    base_z = jnp.floor(coord_z)
    frac_z = coord_z - base_z
    index_x = base_x.astype(jnp.int32)
    index_y = base_y.astype(jnp.int32)
    index_z = base_z.astype(jnp.int32) % cells_z
    cell_list = []
    weight_list = []
    for offset_x in (0, 1):
        for offset_y in (0, 1):
            for offset_z in (0, 1):
                weight_x = frac_x if offset_x else 1.0 - frac_x
                weight_y = frac_y if offset_y else 1.0 - frac_y
                weight_z = frac_z if offset_z else 1.0 - frac_z
                cell_list.append(
                    ((index_x + offset_x) * cells_y + index_y + offset_y) * cells_z
                    + (index_z + offset_z) % cells_z
                )
                weight_list.append(weight_x * weight_y * weight_z)
    return (jnp.stack(cell_list, axis=-2), jnp.stack(weight_list, axis=-2))


def pair_accel(receivers, sources, shifts):
    parts = []
    for comp in range(3):
        parts.append(
            shifts[:, :, comp, None, None]
            + sources[:, :, comp, None, :]
            - receivers[:, None, comp, :, None]
        )
    square = parts[0] * parts[0] + parts[1] * parts[1] + parts[2] * parts[2]
    strength = (
        sources[:, :, 3, None, :] * jnp.exp(-square / split_scale) * (square + softening) ** (-1.5)
    )
    return jnp.stack([jnp.sum(strength * parts[comp], axis=(1, 3)) for comp in range(3)], axis=1)


def split_length(length):
    divisor = 1
    for factor in range(1, math.isqrt(length) + 1):
        if length % factor == 0:
            divisor = factor
    return divisor


def dft_table(length):
    indices = jnp.arange(length, dtype=jnp.int32)
    phases = indices[:, None] * indices[None, :] % length
    angles = phases.astype(jnp.float32) * (2.0 * jnp.pi / length)
    return (jnp.cos(angles), jnp.sin(angles))


def twiddle_table(outer, inner):
    length = outer * inner
    phases = (
        jnp.arange(outer, dtype=jnp.int32)[:, None]
        * jnp.arange(inner, dtype=jnp.int32)[None, :]
        % length
    )
    angles = phases.astype(jnp.float32) * (2.0 * jnp.pi / length)
    return (jnp.cos(angles), jnp.sin(angles))


def complex_mix(real, imag, cosine, sine_table, sign, form):
    real_cos = jnp.einsum(form, real, cosine, precision=highest)
    real_sin = jnp.einsum(form, real, sine_table, precision=highest)
    imag_cos = jnp.einsum(form, imag, cosine, precision=highest)
    imag_sin = jnp.einsum(form, imag, sine_table, precision=highest)
    return (real_cos - sign * imag_sin, imag_cos + sign * real_sin)


def transform_last(real, imag, sign):
    length = real.shape[-1]
    outer = split_length(length)
    inner = length // outer
    leading = real.shape[:-1]
    real = real.reshape(leading + (outer, inner))
    imag = imag.reshape(leading + (outer, inner))
    cos_outer, sin_outer = dft_table(outer)
    real, imag = complex_mix(real, imag, cos_outer, sin_outer, sign, "...pq,pk->...kq")
    turn_cos, turn_sin = twiddle_table(outer, inner)
    real, imag = (
        real * turn_cos - sign * imag * turn_sin,
        imag * turn_cos + sign * real * turn_sin,
    )
    cos_inner, sin_inner = dft_table(inner)
    real, imag = complex_mix(real, imag, cos_inner, sin_inner, sign, "...kq,qm->...mk")
    return (real.reshape(leading + (length,)), imag.reshape(leading + (length,)))


def transform_axis(fields, axis, sign):
    real = jnp.moveaxis(fields[:, 0], axis, -1)
    imag = jnp.moveaxis(fields[:, 1], axis, -1)
    real, imag = transform_last(real, imag, sign)
    return jnp.stack([jnp.moveaxis(real, -1, axis), jnp.moveaxis(imag, -1, axis)], axis=1)


def rotate(fields, factor):
    return jnp.stack([factor * fields[:, 1], -factor * fields[:, 0]], axis=1)


def shards(positions, masses, velocities, tile_counts, neighbour_list):
    tiles = positions.shape[2]
    listed = neighbour_list.shape[3]
    slot_index = jnp.arange(128, dtype=jnp.int32)
    live_mask = (slot_index < tile_counts[..., None]).astype(jnp.float32)
    mass_live = masses * live_mask
    packed = jnp.concatenate([positions, mass_live[:, :, :, None, :]], axis=3)
    shell = padded(packed, ((("gx", "gz"), 0), ("gy", 1)), 1)
    cell_index, cloud_weights = cloud_stencil(positions, CX, CY, NZ, tiles)
    amounts = cloud_weights * mass_live[:, :, :, None, :]
    density = jax.ops.segment_sum(
        amounts.reshape(-1), cell_index.reshape(-1), num_segments=CX * CY * NZ
    ).reshape(CX, CY, NZ)
    spectrum = jnp.stack([density, jnp.zeros_like(density)], axis=0)[None]
    spectrum = transform_axis(spectrum, 3, -1.0)
    spectrum = lax.all_to_all(spectrum, "gy", split_axis=4, concat_axis=3, tiled=True)
    span_y = spectrum.shape[3]
    spectrum = transform_axis(spectrum, 2, -1.0)
    spectrum = lax.all_to_all(spectrum, ("gx", "gz"), split_axis=3, concat_axis=2, tiled=True)
    span_x = spectrum.shape[2]
    spectrum = transform_axis(spectrum, 1, -1.0)
    block_y = spectrum.shape[3]
    block_z = spectrum.shape[4]
    kappa_x, sine_x = wave_terms(span_x, 0, span_x)
    kappa_y, sine_y = wave_terms(span_y, lax.axis_index(("gx", "gz")) * block_y, block_y)
    kappa_z, sine_z = wave_terms(NZ, lax.axis_index("gy") * block_z, block_z)
    kappa_sum = kappa_x[:, None, None] + kappa_y[None, :, None] + kappa_z[None, None, :]
    potential = spectrum * (-jnp.exp(-smoothing * kappa_sum) / (kappa_sum + screening))
    fields = jnp.concatenate([rotate(potential, sine_x[:, None, None]), potential], axis=0)
    fields = transform_axis(fields, 1, 1.0) / span_x
    fields = lax.all_to_all(fields, ("gx", "gz"), split_axis=2, concat_axis=3, tiled=True)
    whole_sine_y = wave_terms(span_y, 0, span_y)[1]
    fields = jnp.concatenate(
        [fields[0:1], rotate(fields[1:2], whole_sine_y[None, :, None]), fields[1:2]], axis=0
    )
    fields = transform_axis(fields, 2, 1.0) / span_y
    fields = lax.all_to_all(fields, "gy", split_axis=3, concat_axis=4, tiled=True)
    whole_sine_z = wave_terms(NZ, 0, NZ)[1]
    fields = jnp.concatenate(
        [fields[0:2], rotate(fields[2:3], whole_sine_z[None, None, :])], axis=0
    )
    fields = transform_axis(fields, 3, 1.0) / NZ
    forces = fields[:, 0]
    flat_forces = forces.reshape(3, -1)
    picked = flat_forces[:, cell_index]
    long_accel = jnp.moveaxis(jnp.sum(cloud_weights[None] * picked, axis=4), 0, 3)
    flat_shell = shell.reshape(9 * tiles, 4, 128)
    own_list = neighbour_list[0, 0]
    sources = flat_shell[own_list]
    groups = own_list // tiles
    layers = own_list % tiles
    tile_row = jnp.arange(tiles, dtype=jnp.int32)[:, None]
    shifts = jnp.stack(
        [groups // 3 - 1, groups % 3 - 1, (layers - tile_row + 1) % tiles - 1], axis=-1
    ).astype(jnp.float32)
    short_accel = lax.map(
        lambda pieces: pair_accel(*pieces),
        (
            positions[0, 0].reshape(tiles, 1, 3, 128),
            sources.reshape(tiles, 1, listed, 4, 128),
            shifts.reshape(tiles, 1, listed, 3),
        ),
    )
    short_accel = short_accel.reshape(1, 1, tiles, 3, 128)
    return velocities + live_mask[:, :, :, None, :] * (
        long_kick * long_accel + short_kick * short_accel
    )


MESH = pl.DeviceIdType.MESH
LOGICAL = pl.DeviceIdType.LOGICAL
f32 = jnp.float32
bf16 = jnp.bfloat16


def halves(x):
    high = x.astype(bf16)
    return high, (x - high.astype(f32)).astype(bf16)


def dot3(a, b, dims=((1,), (0,))):
    dot = functools.partial(
        lax.dot_general, dimension_numbers=(dims, ((), ())), preferred_element_type=f32
    )
    return dot(a[0], b[0]) + dot(a[1], b[0]) + dot(a[0], b[1])


def scope(name):
    return contextlib.nullcontext()


def hat(coord, cell):
    return jnp.maximum(0.0, 1.0 - jnp.abs(coord - cell))


def np_halves(table):
    table = jnp.asarray(np.asarray(table, np.float32))
    return jnp.stack(halves(table))


def stacked_dot(high, low, table_high, table_low, dims=((1,), (0,))):
    dot = functools.partial(
        lax.dot_general, dimension_numbers=(dims, ((), ())), preferred_element_type=f32
    )
    rows = high.shape[0]
    both = dot(jnp.concatenate([high, low], axis=0), table_high)
    return both[:rows] + both[rows:] + dot(high, table_low)


def tables(size_x, size_y, size_z, tiles):
    rows, cols = size_x * size_z, size_y
    count = rows * cols
    modes = NZ // 2 // count
    pack = 128 // (2 * modes)
    groups = tiles // 2
    lane = np.arange(128)
    member, imag, slot = lane // (2 * modes), lane % (2 * modes) >= modes, lane % modes
    cells = np.arange(128) - 1
    cells[127] = -2
    used = cells <= NZ // tiles + 1
    waves = []
    for g in range(groups):
        plus = member < pack // 2
        residue = np.where(plus, g, tiles - g if g else tiles // 2)
        mode = tiles * (member % (pack // 2) * modes + slot) + residue
        angle = 2 * np.pi * ((cells[:, None] * mode[None]) % NZ) / NZ
        direct = np.where(imag[None], -np.sin(angle), np.cos(angle))
        crossed = np.where(imag[None], np.cos(angle), np.sin(angle))
        crossed = np.where(plus[None], -crossed, crossed)
        if g == 0:
            nyquist = (mode == 0) & imag
            direct = np.where(nyquist[None], np.cos(np.pi * (cells % 2))[:, None], direct)
            direct, crossed = (
                np.where(plus[None], direct, 0.0),
                np.where(plus[None], 0.0, direct),
            )
        both = np.stack([direct, crossed])
        waves.append(np.where(used[None, :, None], both, 0.0).reshape(256, 128))
    nx, ny = rows * CX, cols * CY
    index = np.arange(4 * count * 4)
    device, row = index // 4 % count, index // (4 * count) * (CX * CY // 4) + index % 4
    real = index % 4 < CX * CY // 4
    place_x = device // (size_y * size_z) * size_z + device % size_z
    place_y = device // size_z % size_y
    here_x = np.where(real, place_x * CX + row // CY, 0)
    here_y = np.where(real, place_y * CY + row % CY, 0)
    wave_x, wave_y = np.arange(nx * ny) // ny, np.arange(nx * ny) % ny

    def cas(x, y):
        ax = 2 * np.pi * (x[:, None] * wave_x[None] % nx) / nx
        ay = 2 * np.pi * (y[:, None] * wave_y[None] % ny) / ny
        return (np.cos(ax) + np.sin(ax)) * (np.cos(ay) + np.sin(ay))

    into = cas(here_x, here_y) * real[:, None]
    outof = cas(wave_x, wave_y)
    lanes = np.zeros((8, nx * ny))
    lanes[:] = 4 * np.sin(np.pi * wave_x / nx) ** 2 + 4 * np.sin(np.pi * wave_y / ny) ** 2
    return np_halves(np.stack(waves)), np_halves(into), np_halves(outof), jnp.asarray(lanes, f32)


def tile_waves(even, odd):
    half = len(even) - 1
    ring, quarter = 2 * half, half // 2

    def total(terms):
        result = None
        for factor, value in terms:
            if abs(factor) < 1e-12:
                continue
            if abs(abs(factor) - 1.0) < 1e-12:
                if result is None:
                    result = value if factor > 0 else -value
                else:
                    result = result + value if factor > 0 else result - value
            else:
                part = value * float(abs(factor))
                if result is None:
                    result = part if factor > 0 else -part
                else:
                    result = result + part if factor > 0 else result - part
        return result

    sums = [even[t] + even[half - t] for t in range(quarter)]
    gaps = [even[t] - even[half - t] for t in range(quarter)]
    odd_sums = {t: odd[t] + odd[half - t] for t in range(1, quarter)}
    odd_gaps = {t: odd[t] - odd[half - t] for t in range(1, quarter)}
    cosines, sines = [], {}
    for r in range(half + 1):
        cos = [math.cos(2 * math.pi * r * t / ring) for t in range(quarter + 1)]
        sin = [math.sin(2 * math.pi * r * t / ring) for t in range(quarter + 1)]
        terms = [(cos[t], (gaps if r % 2 else sums)[t]) for t in range(quarter)]
        if r % 2 == 0:
            terms.append((cos[quarter], even[quarter]))
        cosines.append(total(terms))
        if 0 < r < half:
            terms = [(sin[t], (odd_sums if r % 2 else odd_gaps)[t]) for t in range(1, quarter)]
            if r % 2:
                terms.append((sin[quarter], odd[quarter]))
            sines[r] = total(terms)
    return cosines, sines


def kick_kernel(
    sizes,
    pos_hbm, mass_hbm, vel_hbm, lanes_hbm, counts_hbm, list_hbm, wave_hbm, into_hbm, outof_hbm,
    out_ref,
    pos_ref, mass_ref, vel_ref, lanes_ref, counts_ref, list_ref, wave_ref, into_ref, outof_ref,
    shell_ref, rho_ref, weight_ref, spec_ref, got_ref, window_ref,
    back_ref, home_ref, part_ref, field_ref, spread_ref, accum_ref, short_ref,
    input_sem, halo_send, halo_recv, out_send, out_recv, back_send, back_recv,
):
    size_x, size_y, size_z, tiles, listed = sizes
    rows, cols = size_x * size_z, size_y
    count = rows * cols
    modes = NZ // 2 // count
    width = 2 * modes
    pack = 128 // width
    groups = tiles // 2
    span = NZ // tiles
    near_cells = -(-(span + 3) // 16) * 16
    share = CX * CY // 4
    flat = size_y * size_z
    gx, gy, gz = lax.axis_index("gx"), lax.axis_index("gy"), lax.axis_index("gz")
    row, col = gx * size_z + gz, gy
    me = (gx * size_y + gy) * size_z + gz

    copies = [
        pltpu.make_async_copy(a, b, input_sem.at[i])
        for i, (a, b) in enumerate(
            (
                (pos_hbm, pos_ref),
                (mass_hbm, mass_ref),
                (counts_hbm, counts_ref),
                (wave_hbm, wave_ref),
                (list_hbm, list_ref),
                (lanes_hbm, lanes_ref),
                (into_hbm, into_ref),
                (outof_hbm, outof_ref),
                (vel_hbm, vel_ref),
            )
        )
    ]
    for copy in copies[:3]:
        copy.start()

    def place(r, c):
        return (r // size_z, c, r % size_z)

    first = size_x - 1 - gx
    second = lax.rem(gx + size_x // 2, size_x)
    third = size_x - 1 - second
    spot_here = gy * size_z + gz

    def other(i):
        if size_x != 4:
            return lax.rem(me + 1 + i, count)
        block = i // flat
        away = lax.rem(i, flat) + jnp.where(block == 3, 1, 0)
        plane = jnp.where(
            block == 0, first, jnp.where(block == 1, second, jnp.where(block == 2, third, gx))
        )
        return plane * flat + lax.rem(spot_here + away, flat)

    got_ref[...] = jnp.zeros((count, 4, 128), f32)
    barrier = pltpu.get_barrier_semaphore()

    def greet(i, carry):
        pl.semaphore_signal(
            barrier, inc=1, device_id=other(i), device_id_type=LOGICAL
        )
        return carry

    with scope("a_greet"):
        lax.fori_loop(0, count - 1, greet, 0)
    for copy in copies[3:]:
        copy.start()

    slot = lax.broadcasted_iota(jnp.int32, (1, 128), 1)
    row_of = lax.broadcasted_iota(jnp.int32, (16, 128), 0)
    cell_of = row_of // 4 * share + row_of % 4
    cell_x = jnp.where(row_of % 4 < share, cell_of // CY, -8).astype(f32)
    cell_y = (cell_of % CY).astype(f32)
    cell_z = lax.broadcasted_iota(jnp.int32, (near_cells, 128), 0).astype(f32) - 1.0
    blank = jnp.zeros((128 - near_cells, 128), bf16)

    own = 4 * tiles

    def edges(t):
        coord_x = jnp.clip(pos_ref[0, pl.ds(t, 1), :] * CX - 0.5, 0.0, CX - 1.0)
        coord_y = jnp.clip(pos_ref[1, pl.ds(t, 1), :] * CY - 0.5, 0.0, CY - 1.0)
        return coord_x, coord_y

    def deposit(t, carry):
        live = (slot < counts_ref[t]).astype(f32)
        mass = mass_ref[pl.ds(t, 1), :] * live
        for comp in range(3):
            shell_ref[own + t, comp:comp + 1, :] = pos_ref[comp, pl.ds(t, 1), :]
        shell_ref[own + t, 3:4, :] = mass
        coord_x, coord_y = edges(t)
        start = jnp.asarray(t, jnp.int32).astype(f32)
        coord_z = (start + pos_ref[2, pl.ds(t, 1), :]) * span - 0.5 - start * span
        plane = hat(coord_x, cell_x) * hat(coord_y, cell_y) * mass
        high, low = halves(plane)
        weight_high, weight_low = halves(hat(coord_z, cell_z))
        weight_ref[t, 0] = weight_high
        weight_ref[t, 1] = weight_low
        rho_ref[t] = stacked_dot(
            high,
            low,
            jnp.concatenate([weight_high, blank], axis=0),
            jnp.concatenate([weight_low, blank], axis=0),
            ((1,), (1,)),
        )
        return carry

    with scope("b_inwait"):
        for copy in copies[:3]:
            copy.wait()
    with scope("c_deposit"):
        lax.fori_loop(0, tiles, deposit, 0, unroll=4)

    quarter = lax.broadcasted_iota(jnp.int32, (8, 128), 1) // width
    lower, even_block = quarter < 2, quarter % 2 == 0

    def exchange(blocks):
        far = [pltpu.roll(b, 64, 1) for b in blocks]
        mixed = [
            jnp.where(lower, blocks[0], far[2]),
            jnp.where(lower, blocks[1], far[3]),
            jnp.where(lower, far[0], blocks[2]),
            jnp.where(lower, far[1], blocks[3]),
        ]
        result = []
        for pair in (0, 2):
            one, two = mixed[pair], mixed[pair + 1]
            result.append(jnp.where(even_block, one, pltpu.roll(two, width, 1)))
            result.append(jnp.where(even_block, pltpu.roll(one, 128 - width, 1), two))
        return result

    with scope("d_tabwait"):
        copies[3].wait()
    with scope("e_transform"):
        rho = [rho_ref[t] for t in range(tiles)]
        half = tiles // 2
        even = [rho[0]] + [rho[t] + rho[tiles - t] for t in range(1, half)] + [rho[half]]
        odd = {t: rho[t] - rho[tiles - t] for t in range(1, half)}
        cosines, sines = tile_waves(even, odd)
        for g in range(groups):
            pair = (cosines[g], sines[g]) if g else (cosines[0], cosines[half])
            high, low = halves(jnp.concatenate(pair, axis=1))
            lines = stacked_dot(high, low, wave_ref[0, g], wave_ref[1, g])
            blocks = [lines[0:8], pltpu.roll(lines[0:8], 4, 0), lines[8:16], pltpu.roll(lines[8:16], 4, 0)]
            for i, block in enumerate(exchange(blocks)):
                spec_ref[g * pack + i] = block[0:4]

    def out_copy(d):
        return pltpu.make_async_remote_copy(
            src_ref=spec_ref.at[d, pl.ds(0, share)],
            dst_ref=got_ref.at[me, pl.ds(0, share)],
            send_sem=out_send,
            recv_sem=out_recv,
            device_id=d,
            device_id_type=LOGICAL,
        )

    def back_copy(d):
        return pltpu.make_async_remote_copy(
            src_ref=back_ref.at[d],
            dst_ref=home_ref.at[me],
            send_sem=back_send,
            recv_sem=back_recv,
            device_id=d,
            device_id_type=LOGICAL,
        )

    def start_all(make):
        def step(i, carry):
            make(other(i)).start()
            return carry

        lax.fori_loop(0, count - 1, step, 0)

    def wait_all(rest, sem):
        pltpu.make_async_copy(rest, rest, sem).wait()

    with scope("f_barwait"):
        pl.semaphore_wait(barrier, count - 1)
    with scope("g_startout"):
        start_all(out_copy)
    halos = []
    for step_x in (-1, 0, 1):
        for step_y in (-1, 0, 1):
            if step_x == 0 and step_y == 0:
                continue
            slot_there = (1 - step_x) * 3 + 1 - step_y
            halos.append(
                pltpu.make_async_remote_copy(
                    src_ref=shell_ref.at[pl.ds(own, tiles)],
                    dst_ref=shell_ref.at[pl.ds(slot_there * tiles, tiles)],
                    send_sem=halo_send.at[slot_there],
                    recv_sem=halo_recv.at[slot_there],
                    device_id=place((row + step_x + rows) % rows, (col + step_y + cols) % cols),
                    device_id_type=MESH,
                )
            )
    with scope("h_starthalo"):
        for copy in halos:
            copy.start()
    got_ref[me] = spec_ref[me]

    ones = jnp.ones((8, 128), bf16)
    block = 32

    def spread(t, carry):
        for comp in range(3):
            spread_ref[t, comp] = jnp.transpose(
                jnp.broadcast_to(pos_ref[comp, pl.ds(t, 1), :], (128, 128)), (1, 0)
            )
        return carry

    with scope("i_spread"):
        lax.fori_loop(0, tiles, spread, 0)

    def pairs(t, carry):
        sources = []
        for n in range(listed):
            entry = list_ref[n, 0, t]
            group, layer = entry // tiles, entry % tiles
            away = (layer - t + 1 + tiles) % tiles - 1
            tile = shell_ref[entry]
            sources.append(
                (
                    tile[0:1] + (group // 3 - 1).astype(f32),
                    tile[1:2] + (group % 3 - 1).astype(f32),
                    tile[2:3] + away.astype(f32),
                    tile[3:4],
                )
            )
        for b in range(128 // block):
            here = [spread_ref[t, comp, b * block:(b + 1) * block, :] for comp in range(3)]
            totals = [jnp.zeros((block, 128), f32) for comp in range(3)]
            for source in sources:
                parts = [source[comp] - here[comp] for comp in range(3)]
                square = parts[0] * parts[0] + parts[1] * parts[1] + parts[2] * parts[2]
                root = lax.rsqrt(square + softening)
                strength = source[3] * jnp.exp2(square * (-1.0 / (split_scale * math.log(2.0)))) * (root * root * root)
                totals = [totals[comp] + strength * parts[comp] for comp in range(3)]
            for comp in range(3):
                accum_ref[comp * 128 + b * block:comp * 128 + (b + 1) * block, :] = totals[comp]
        high, low = halves(accum_ref[...])
        dot = functools.partial(
            lax.dot_general,
            dimension_numbers=(((1,), (1,)), ((), ())),
            preferred_element_type=f32,
        )
        sums = dot(ones, high) + dot(ones, low)
        for comp in range(3):
            short_ref[comp, pl.ds(t, 1), :] = sums[0:1, comp * 128:(comp + 1) * 128]
        return carry

    nx, ny = rows * CX, cols * CY
    copies[4].wait()
    copies[5].wait()
    with scope("i2_green"):
        row_in = lax.broadcasted_iota(jnp.int32, (width, nx * ny), 0)
        family, member = me // pack, me % pack
        residue = jnp.where(
            member < pack // 2, family, jnp.where(family == 0, tiles // 2, tiles - family)
        )
        mode_of = tiles * (member % (pack // 2) * modes + row_in % modes) + residue
        alone = mode_of == 0
        wave_z = jnp.where(alone & (row_in >= modes), NZ // 2, mode_of).astype(f32)
        kappa = lanes_ref[0:1, :] + 4.0 * jnp.sin(wave_z * (jnp.pi / NZ)) ** 2
        scale = jnp.where(alone, 0.5, 1.0) * (1.0 / (NZ * nx * ny))
        green = -jnp.exp(-smoothing * kappa) / (kappa + screening) * scale

    early = 0
    with scope("j_waitgot"):
        wait_all(got_ref.at[pl.ds(0, count - 1), pl.ds(0, share)], out_recv)
    with scope("k_plane"):
        copies[6].wait()
        copies[7].wait()
        turned = jnp.transpose(got_ref[...].reshape(count * 4, 128), (1, 0))
        mine = jnp.concatenate(
            [turned[a * width:(a + 1) * width] for a in range(pack)], axis=1
        )
        high, low = halves(mine)
        waves = stacked_dot(high, low, into_ref[0], into_ref[1])
        high, low = halves(waves * green)
        high = jnp.concatenate([high] * pack, axis=0)
        low = jnp.concatenate([low] * pack, axis=0)
        dot = functools.partial(
            lax.dot_general,
            dimension_numbers=(((1,), (1,)), ((), ())),
            preferred_element_type=f32,
        )
        sheet = dot(outof_ref[0], high) + dot(outof_ref[0], low) + dot(outof_ref[1], high)
        for r in range(rows):
            for v in range(ny // 8):
                pick = [
                    sheet[at:at + 8]
                    for at in (((r * CX - 1 + b) % nx) * ny + v * 8 for b in range(pack))
                ]
                window = jnp.where(
                    lower,
                    jnp.where(even_block, pick[0], pick[1]),
                    jnp.where(even_block, pick[2], pick[3]),
                )
                window_ref[r, (v + 1) * 8:(v + 2) * 8, :] = window
                if v == 0:
                    window_ref[r, 8 + ny:16 + ny, :] = window
                if v == ny // 8 - 1:
                    window_ref[r, 0:8, :] = window
        for r in range(rows):
            for c in range(cols):
                d = (r // size_z * size_y + c) * size_z + r % size_z
                back_ref[d] = window_ref[r, c * CY + 7:c * CY + 15, :]
    with scope("l_startback"):
        start_all(back_copy)
    home_ref[me] = back_ref[me]

    with scope("m_waithalo"):
        for copy in halos:
            copy.wait_recv()
    with scope("n_pairs2"):
        lax.fori_loop(early, tiles, pairs, 0, unroll=2)
    with scope("o_waithome"):
        wait_all(home_ref.at[pl.ds(0, count - 1)], back_recv)

    with scope("p_lines"):
        for g in range(groups):
            lines = exchange([home_ref[g * pack + i] for i in range(pack)])
            pulls = [lines[b - 1] - lines[b + 1] for b in (1, 2)]
            pulls += [pltpu.roll(lines[b], 1, 0) - pltpu.roll(lines[b], 7, 0) for b in (1, 2)]
            high, low = halves(jnp.concatenate(pulls + [lines[1], lines[2]], axis=0))
            part = stacked_dot(high, low, wave_ref[0, g], wave_ref[1, g], ((1,), (1,)))
            part_ref[g] = part[:, :128]
            part_ref[groups + g] = part[:, 128:]
    with scope("q_invert"):
        for f in range(3):
            at = slice(f * 16, (f + 1) * 16)
            even = [part_ref[g, at] for g in range(groups)] + [part_ref[groups, at]]
            odd = {g: part_ref[groups + g, at] for g in range(1, groups)}
            cosines, sines = tile_waves(even, odd)
            for t in range(tiles):
                if t % half == 0:
                    value = cosines[t]
                elif t < half:
                    value = cosines[t] + sines[t]
                else:
                    value = cosines[tiles - t] - sines[tiles - t]
                if f == 2:
                    value = pltpu.roll(value, 1, 1) - pltpu.roll(value, 127, 1)
                high, low = halves(value)
                field_ref[t, f * 16:(f + 1) * 16, :] = high
                field_ref[t, 48 + f * 16:48 + (f + 1) * 16, :] = low

    cell_near = lax.broadcasted_iota(jnp.int32, (8, 128), 0).astype(f32) - 1.0
    copies[8].wait()

    def interpolate(t, carry):
        coord_x, coord_y = edges(t)
        left, right = hat(coord_x, 0.0), hat(coord_x, 1.0)
        along = hat(coord_y, cell_near)
        here = stacked_dot(
            field_ref[t, 0:48],
            field_ref[t, 48:96],
            jnp.concatenate([weight_ref[t, 0], blank], axis=0),
            jnp.concatenate([weight_ref[t, 1], blank], axis=0),
        )
        live = (slot < counts_ref[t]).astype(f32)
        for f in range(3):
            mixed = here[f * 16:f * 16 + 8] * left + here[f * 16 + 8:f * 16 + 16] * right
            pull = jnp.sum(mixed * along, axis=0, keepdims=True)
            at = (f, pl.ds(t, 1), slice(None))
            out_ref[at] = vel_ref[at] + live * (long_kick * pull + short_kick * short_ref[at])
        return carry

    with scope("r_interp"):
        lax.fori_loop(0, tiles, interpolate, 0, unroll=4)
    with scope("s_tail"):
        for copy in halos:
            copy.wait_send()
        wait_all(got_ref.at[pl.ds(0, count - 1), pl.ds(0, share)], out_send)
        wait_all(home_ref.at[pl.ds(0, count - 1)], back_send)


def fused_shards(sizes, positions, masses, velocities, tile_counts, neighbour_list):
    size_x, size_y, size_z, tiles, listed = sizes
    rows, cols = size_x * size_z, size_y
    count = rows * cols
    groups = tiles // 2
    near_cells = -(-(NZ // tiles + 3) // 16) * 16
    with jax.ensure_compile_time_eval():
        wave, into, outof, lanes = tables(size_x, size_y, size_z, tiles)
    anywhere = pl.BlockSpec(memory_space=pl.ANY)
    dma = pltpu.SemaphoreType.DMA
    kicked = pl.pallas_call(
        functools.partial(kick_kernel, sizes),
        out_shape=pltpu.VMEM((3, tiles, 128), f32),
        in_specs=[anywhere] * 9,
        out_specs=pl.BlockSpec(memory_space=pltpu.VMEM),
        scratch_shapes=[
            pltpu.VMEM((3, tiles, 128), f32),
            pltpu.VMEM((tiles, 128), f32),
            pltpu.VMEM((3, tiles, 128), f32),
            pltpu.VMEM(lanes.shape, f32),
            pltpu.SMEM((tiles,), jnp.int32),
            pltpu.SMEM((listed, 1, tiles), jnp.int32),
            pltpu.VMEM(wave.shape, bf16),
            pltpu.VMEM(into.shape, bf16),
            pltpu.VMEM(outof.shape, bf16),
            pltpu.VMEM((9 * tiles, 4, 128), f32),
            pltpu.VMEM((tiles, 16, 128), f32),
            pltpu.VMEM((tiles, 2, near_cells, 128), bf16),
            pltpu.VMEM((count, 4, 128), f32),
            pltpu.VMEM((count, 4, 128), f32),
            pltpu.VMEM((rows, cols * CY + 16, 128), f32),
            pltpu.VMEM((count, 8, 128), f32),
            pltpu.VMEM((count, 8, 128), f32),
            pltpu.VMEM((2 * groups, 48, 128), f32),
            pltpu.VMEM((tiles, 96, 128), bf16),
            pltpu.VMEM((tiles, 3, 128, 128), f32),
            pltpu.VMEM((384, 128), f32),
            pltpu.VMEM((3, tiles, 128), f32),
            dma((9,)),
            dma((9,)),
            dma((9,)),
            dma,
            dma,
            dma,
            dma,
        ],
        compiler_params=pltpu.CompilerParams(collective_id=0, has_side_effects=True),
        name="kick",
    )(
        jnp.transpose(positions[0, 0], (1, 0, 2)),
        masses.reshape(tiles, 128),
        jnp.transpose(velocities[0, 0], (1, 0, 2)),
        lanes,
        tile_counts.reshape(tiles),
        jnp.transpose(neighbour_list[0], (2, 0, 1)),
        wave,
        into,
        outof,
    )
    return jnp.transpose(kicked, (1, 0, 2))[None, None]


def fits(sizes):
    size_x, size_y, size_z, tiles, listed = sizes
    count = size_x * size_y * size_z
    if CX != 2 or CY != 6 or count != 32 or tiles != 16 or size_y * CY % 8:
        return False
    return NZ // 2 == 16 * count and NZ // tiles + 3 < 127


def solution(mesh):
    placed = (
        P(("gx", "gz"), "gy", None, None, None),
        P(("gx", "gz"), "gy", None, None),
        P(("gx", "gz"), "gy", None, None, None),
        P(("gx", "gz"), "gy", None),
        P(("gx", "gz"), "gy", None, None),
    )

    def local(positions, masses, velocities, tile_counts, neighbour_list):
        sizes = tuple(mesh.shape[axis] for axis in ("gx", "gy", "gz"))
        sizes = sizes + (positions.shape[2], neighbour_list.shape[3])
        part = functools.partial(fused_shards, sizes) if fits(sizes) else shards
        return part(positions, masses, velocities, tile_counts, neighbour_list)

    return jax.shard_map(
        local,
        mesh=mesh,
        in_specs=placed,
        out_specs=P(("gx", "gz"), "gy", None, None, None),
        check_vma=False,
    )
```

```python
import contextlib
import functools
import math

import jax
import jax.numpy as jnp
import numpy as np
from jax import lax
from jax.experimental import pallas as pl
from jax.experimental.pallas import tpu as pltpu
from jax.sharding import PartitionSpec as P

CX = 2
CY = 6
NZ = 1024


smoothing = 0.1
screening = 0.01
split_scale = 2.0
softening = 0.05
long_kick = 1.0
short_kick = 0.05
highest = lax.Precision.HIGHEST


def padded(cells, sides, width):
    for axis, dim in sides:
        count = lax.axis_size(axis)
        head = lax.slice_in_dim(cells, 0, width, axis=dim)
        tail = lax.slice_in_dim(cells, cells.shape[dim] - width, cells.shape[dim], axis=dim)
        cells = jnp.concatenate(
            [
                lax.ppermute(tail, axis, [(i, (i + 1) % count) for i in range(count)]),
                cells,
                lax.ppermute(head, axis, [((i + 1) % count, i) for i in range(count)]),
            ],
            axis=dim,
        )
    return cells


def wave_terms(length, first_index, extent):
    wavenum = (first_index + jnp.arange(extent, dtype=jnp.int32)).astype(jnp.float32)
    angles = wavenum * (2.0 * jnp.pi / length)
    return (4.0 * jnp.sin(0.5 * angles) ** 2, jnp.sin(angles))


def cloud_stencil(positions, cells_x, cells_y, cells_z, tiles):
    span = cells_z // tiles
    tile_row = jnp.arange(tiles, dtype=jnp.int32)[:, None]
    coord_x = positions[..., 0, :] * cells_x - 0.5
    base_x = jnp.clip(jnp.floor(coord_x), 0, cells_x - 2)
    frac_x = jnp.clip(coord_x - base_x, 0.0, 1.0)
    coord_y = positions[..., 1, :] * cells_y - 0.5
    base_y = jnp.clip(jnp.floor(coord_y), 0, cells_y - 2)
    frac_y = jnp.clip(coord_y - base_y, 0.0, 1.0)
    coord_z = (tile_row + positions[..., 2, :]) * span - 0.5
    base_z = jnp.floor(coord_z)
    frac_z = coord_z - base_z
    index_x = base_x.astype(jnp.int32)
    index_y = base_y.astype(jnp.int32)
    index_z = base_z.astype(jnp.int32) % cells_z
    cell_list = []
    weight_list = []
    for offset_x in (0, 1):
        for offset_y in (0, 1):
            for offset_z in (0, 1):
                weight_x = frac_x if offset_x else 1.0 - frac_x
                weight_y = frac_y if offset_y else 1.0 - frac_y
                weight_z = frac_z if offset_z else 1.0 - frac_z
                cell_list.append(
                    ((index_x + offset_x) * cells_y + index_y + offset_y) * cells_z
                    + (index_z + offset_z) % cells_z
                )
                weight_list.append(weight_x * weight_y * weight_z)
    return (jnp.stack(cell_list, axis=-2), jnp.stack(weight_list, axis=-2))


def pair_accel(receivers, sources, shifts):
    parts = []
    for comp in range(3):
        parts.append(
            shifts[:, :, comp, None, None]
            + sources[:, :, comp, None, :]
            - receivers[:, None, comp, :, None]
        )
    square = parts[0] * parts[0] + parts[1] * parts[1] + parts[2] * parts[2]
    strength = (
        sources[:, :, 3, None, :] * jnp.exp(-square / split_scale) * (square + softening) ** (-1.5)
    )
    return jnp.stack([jnp.sum(strength * parts[comp], axis=(1, 3)) for comp in range(3)], axis=1)


def split_length(length):
    divisor = 1
    for factor in range(1, math.isqrt(length) + 1):
        if length % factor == 0:
            divisor = factor
    return divisor


def dft_table(length):
    indices = jnp.arange(length, dtype=jnp.int32)
    phases = indices[:, None] * indices[None, :] % length
    angles = phases.astype(jnp.float32) * (2.0 * jnp.pi / length)
    return (jnp.cos(angles), jnp.sin(angles))


def twiddle_table(outer, inner):
    length = outer * inner
    phases = (
        jnp.arange(outer, dtype=jnp.int32)[:, None]
        * jnp.arange(inner, dtype=jnp.int32)[None, :]
        % length
    )
    angles = phases.astype(jnp.float32) * (2.0 * jnp.pi / length)
    return (jnp.cos(angles), jnp.sin(angles))


def complex_mix(real, imag, cosine, sine_table, sign, form):
    real_cos = jnp.einsum(form, real, cosine, precision=highest)
    real_sin = jnp.einsum(form, real, sine_table, precision=highest)
    imag_cos = jnp.einsum(form, imag, cosine, precision=highest)
    imag_sin = jnp.einsum(form, imag, sine_table, precision=highest)
    return (real_cos - sign * imag_sin, imag_cos + sign * real_sin)


def transform_last(real, imag, sign):
    length = real.shape[-1]
    outer = split_length(length)
    inner = length // outer
    leading = real.shape[:-1]
    real = real.reshape(leading + (outer, inner))
    imag = imag.reshape(leading + (outer, inner))
    cos_outer, sin_outer = dft_table(outer)
    real, imag = complex_mix(real, imag, cos_outer, sin_outer, sign, "...pq,pk->...kq")
    turn_cos, turn_sin = twiddle_table(outer, inner)
    real, imag = (
        real * turn_cos - sign * imag * turn_sin,
        imag * turn_cos + sign * real * turn_sin,
    )
    cos_inner, sin_inner = dft_table(inner)
    real, imag = complex_mix(real, imag, cos_inner, sin_inner, sign, "...kq,qm->...mk")
    return (real.reshape(leading + (length,)), imag.reshape(leading + (length,)))


def transform_axis(fields, axis, sign):
    real = jnp.moveaxis(fields[:, 0], axis, -1)
    imag = jnp.moveaxis(fields[:, 1], axis, -1)
    real, imag = transform_last(real, imag, sign)
    return jnp.stack([jnp.moveaxis(real, -1, axis), jnp.moveaxis(imag, -1, axis)], axis=1)


def rotate(fields, factor):
    return jnp.stack([factor * fields[:, 1], -factor * fields[:, 0]], axis=1)


def shards(positions, masses, velocities, tile_counts, neighbour_list):
    tiles = positions.shape[2]
    listed = neighbour_list.shape[3]
    slot_index = jnp.arange(128, dtype=jnp.int32)
    live_mask = (slot_index < tile_counts[..., None]).astype(jnp.float32)
    mass_live = masses * live_mask
    packed = jnp.concatenate([positions, mass_live[:, :, :, None, :]], axis=3)
    shell = padded(packed, ((("gx", "gz"), 0), ("gy", 1)), 1)
    cell_index, cloud_weights = cloud_stencil(positions, CX, CY, NZ, tiles)
    amounts = cloud_weights * mass_live[:, :, :, None, :]
    density = jax.ops.segment_sum(
        amounts.reshape(-1), cell_index.reshape(-1), num_segments=CX * CY * NZ
    ).reshape(CX, CY, NZ)
    spectrum = jnp.stack([density, jnp.zeros_like(density)], axis=0)[None]
    spectrum = transform_axis(spectrum, 3, -1.0)
    spectrum = lax.all_to_all(spectrum, "gy", split_axis=4, concat_axis=3, tiled=True)
    span_y = spectrum.shape[3]
    spectrum = transform_axis(spectrum, 2, -1.0)
    spectrum = lax.all_to_all(spectrum, ("gx", "gz"), split_axis=3, concat_axis=2, tiled=True)
    span_x = spectrum.shape[2]
    spectrum = transform_axis(spectrum, 1, -1.0)
    block_y = spectrum.shape[3]
    block_z = spectrum.shape[4]
    kappa_x, sine_x = wave_terms(span_x, 0, span_x)
    kappa_y, sine_y = wave_terms(span_y, lax.axis_index(("gx", "gz")) * block_y, block_y)
    kappa_z, sine_z = wave_terms(NZ, lax.axis_index("gy") * block_z, block_z)
    kappa_sum = kappa_x[:, None, None] + kappa_y[None, :, None] + kappa_z[None, None, :]
    potential = spectrum * (-jnp.exp(-smoothing * kappa_sum) / (kappa_sum + screening))
    fields = jnp.concatenate([rotate(potential, sine_x[:, None, None]), potential], axis=0)
    fields = transform_axis(fields, 1, 1.0) / span_x
    fields = lax.all_to_all(fields, ("gx", "gz"), split_axis=2, concat_axis=3, tiled=True)
    whole_sine_y = wave_terms(span_y, 0, span_y)[1]
    fields = jnp.concatenate(
        [fields[0:1], rotate(fields[1:2], whole_sine_y[None, :, None]), fields[1:2]], axis=0
    )
    fields = transform_axis(fields, 2, 1.0) / span_y
    fields = lax.all_to_all(fields, "gy", split_axis=3, concat_axis=4, tiled=True)
    whole_sine_z = wave_terms(NZ, 0, NZ)[1]
    fields = jnp.concatenate(
        [fields[0:2], rotate(fields[2:3], whole_sine_z[None, None, :])], axis=0
    )
    fields = transform_axis(fields, 3, 1.0) / NZ
    forces = fields[:, 0]
    flat_forces = forces.reshape(3, -1)
    picked = flat_forces[:, cell_index]
    long_accel = jnp.moveaxis(jnp.sum(cloud_weights[None] * picked, axis=4), 0, 3)
    flat_shell = shell.reshape(9 * tiles, 4, 128)
    own_list = neighbour_list[0, 0]
    sources = flat_shell[own_list]
    groups = own_list // tiles
    layers = own_list % tiles
    tile_row = jnp.arange(tiles, dtype=jnp.int32)[:, None]
    shifts = jnp.stack(
        [groups // 3 - 1, groups % 3 - 1, (layers - tile_row + 1) % tiles - 1], axis=-1
    ).astype(jnp.float32)
    short_accel = lax.map(
        lambda pieces: pair_accel(*pieces),
        (
            positions[0, 0].reshape(tiles, 1, 3, 128),
            sources.reshape(tiles, 1, listed, 4, 128),
            shifts.reshape(tiles, 1, listed, 3),
        ),
    )
    short_accel = short_accel.reshape(1, 1, tiles, 3, 128)
    return velocities + live_mask[:, :, :, None, :] * (
        long_kick * long_accel + short_kick * short_accel
    )


MESH = pl.DeviceIdType.MESH
LOGICAL = pl.DeviceIdType.LOGICAL
f32 = jnp.float32
bf16 = jnp.bfloat16


def halves(x):
    high = x.astype(bf16)
    return high, (x - high.astype(f32)).astype(bf16)


def dot3(a, b, dims=((1,), (0,))):
    dot = functools.partial(
        lax.dot_general, dimension_numbers=(dims, ((), ())), preferred_element_type=f32
    )
    return dot(a[0], b[0]) + dot(a[1], b[0]) + dot(a[0], b[1])


def scope(name):
    return contextlib.nullcontext()


def hat(coord, cell):
    return jnp.maximum(0.0, 1.0 - jnp.abs(coord - cell))


def np_halves(table):
    table = jnp.asarray(np.asarray(table, np.float32))
    return jnp.stack(halves(table))


def stacked_dot(high, low, table_high, table_low, dims=((1,), (0,))):
    dot = functools.partial(
        lax.dot_general, dimension_numbers=(dims, ((), ())), preferred_element_type=f32
    )
    rows = high.shape[0]
    both = dot(jnp.concatenate([high, low], axis=0), table_high)
    return both[:rows] + both[rows:] + dot(high, table_low)


def tables(size_x, size_y, size_z, tiles):
    rows, cols = size_x * size_z, size_y
    count = rows * cols
    modes = NZ // 2 // count
    pack = 128 // (2 * modes)
    groups = tiles // 2
    lane = np.arange(128)
    member, imag, slot = lane // (2 * modes), lane % (2 * modes) >= modes, lane % modes
    cells = np.arange(128) - 1
    cells[127] = -2
    used = cells <= NZ // tiles + 1
    waves = []
    for g in range(groups):
        plus = member < pack // 2
        residue = np.where(plus, g, tiles - g if g else tiles // 2)
        mode = tiles * (member % (pack // 2) * modes + slot) + residue
        angle = 2 * np.pi * ((cells[:, None] * mode[None]) % NZ) / NZ
        direct = np.where(imag[None], -np.sin(angle), np.cos(angle))
        crossed = np.where(imag[None], np.cos(angle), np.sin(angle))
        crossed = np.where(plus[None], -crossed, crossed)
        if g == 0:
            nyquist = (mode == 0) & imag
            direct = np.where(nyquist[None], np.cos(np.pi * (cells % 2))[:, None], direct)
            direct, crossed = (
                np.where(plus[None], direct, 0.0),
                np.where(plus[None], 0.0, direct),
            )
        both = np.stack([direct, crossed])
        waves.append(np.where(used[None, :, None], both, 0.0).reshape(256, 128))
    nx, ny = rows * CX, cols * CY
    index = np.arange(4 * count * 4)
    device, row = index // 4 % count, index // (4 * count) * (CX * CY // 4) + index % 4
    real = index % 4 < CX * CY // 4
    place_x = device // (size_y * size_z) * size_z + device % size_z
    place_y = device // size_z % size_y
    here_x = np.where(real, place_x * CX + row // CY, 0)
    here_y = np.where(real, place_y * CY + row % CY, 0)
    wave_x, wave_y = np.arange(nx * ny) // ny, np.arange(nx * ny) % ny

    def cas(x, y):
        ax = 2 * np.pi * (x[:, None] * wave_x[None] % nx) / nx
        ay = 2 * np.pi * (y[:, None] * wave_y[None] % ny) / ny
        return (np.cos(ax) + np.sin(ax)) * (np.cos(ay) + np.sin(ay))

    into = cas(here_x, here_y) * real[:, None]
    outof = cas(wave_x, wave_y)
    lanes = np.zeros((8, nx * ny))
    lanes[:] = 4 * np.sin(np.pi * wave_x / nx) ** 2 + 4 * np.sin(np.pi * wave_y / ny) ** 2
    return np_halves(np.stack(waves)), np_halves(lane_tiles(into)), np_halves(lane_tiles(outof)), jnp.asarray(lanes, f32)


def lane_tiles(table):
    return np.stack(np.split(table, table.shape[1] // 128, axis=1))


def tile_waves(even, odd):
    half = len(even) - 1
    ring, quarter = 2 * half, half // 2

    def total(terms):
        result = None
        for factor, value in terms:
            if abs(factor) < 1e-12:
                continue
            if abs(abs(factor) - 1.0) < 1e-12:
                if result is None:
                    result = value if factor > 0 else -value
                else:
                    result = result + value if factor > 0 else result - value
            else:
                part = value * float(abs(factor))
                if result is None:
                    result = part if factor > 0 else -part
                else:
                    result = result + part if factor > 0 else result - part
        return result

    sums = [even[t] + even[half - t] for t in range(quarter)]
    gaps = [even[t] - even[half - t] for t in range(quarter)]
    odd_sums = {t: odd[t] + odd[half - t] for t in range(1, quarter)}
    odd_gaps = {t: odd[t] - odd[half - t] for t in range(1, quarter)}
    cosines, sines = [], {}
    for r in range(half + 1):
        cos = [math.cos(2 * math.pi * r * t / ring) for t in range(quarter + 1)]
        sin = [math.sin(2 * math.pi * r * t / ring) for t in range(quarter + 1)]
        terms = [(cos[t], (gaps if r % 2 else sums)[t]) for t in range(quarter)]
        if r % 2 == 0:
            terms.append((cos[quarter], even[quarter]))
        cosines.append(total(terms))
        if 0 < r < half:
            terms = [(sin[t], (odd_sums if r % 2 else odd_gaps)[t]) for t in range(1, quarter)]
            if r % 2:
                terms.append((sin[quarter], odd[quarter]))
            sines[r] = total(terms)
    return cosines, sines


def kick_kernel(
    sizes,
    pos_hbm, mass_hbm, vel_hbm, lanes_hbm, counts_hbm, list_hbm, wave_hbm, into_hbm, outof_hbm,
    out_ref,
    pos_ref, mass_ref, vel_ref, lanes_ref, counts_ref, list_ref, wave_ref, into_ref, outof_ref,
    shell_ref, rho_ref, weight_ref, spec_ref, got_ref, window_ref,
    back_ref, home_ref, part_ref, field_ref, spread_ref, theirs_0, theirs_1, pull_0, pull_1, strength_0, strength_1, short_ref,
    input_sem, halo_send, halo_recv, out_send, out_recv, back_send, back_recv,
):
    size_x, size_y, size_z, tiles, listed = sizes
    rows, cols = size_x * size_z, size_y
    count = rows * cols
    modes = NZ // 2 // count
    width = 2 * modes
    pack = 128 // width
    groups = tiles // 2
    span = NZ // tiles
    near_cells = -(-(span + 3) // 16) * 16
    share = CX * CY // 4
    flat = size_y * size_z
    gx, gy, gz = lax.axis_index("gx"), lax.axis_index("gy"), lax.axis_index("gz")
    row, col = gx * size_z + gz, gy
    me = (gx * size_y + gy) * size_z + gz

    copies = [
        pltpu.make_async_copy(a, b, input_sem.at[i])
        for i, (a, b) in enumerate(
            (
                (pos_hbm, pos_ref),
                (mass_hbm, mass_ref),
                (counts_hbm, counts_ref),
                (wave_hbm, wave_ref),
                (list_hbm, list_ref),
                (lanes_hbm, lanes_ref),
                (into_hbm, into_ref),
                (outof_hbm, outof_ref),
                (vel_hbm, vel_ref),
            )
        )
    ]
    for copy in copies[:3]:
        copy.start()

    def place(r, c):
        return (r // size_z, c, r % size_z)

    first = size_x - 1 - gx
    second = lax.rem(gx + size_x // 2, size_x)
    third = size_x - 1 - second
    spot_here = gy * size_z + gz

    turns = [lax.rem(spot_here + i, flat) for i in range(flat)]

    def for_others(act):
        def some(members):
            def step(p, carry):
                if size_x == 4:
                    plane = jnp.where(
                        p == 0, first, jnp.where(p == 1, second, jnp.where(p == 2, third, gx))
                    )
                else:
                    plane = lax.rem(gx + p + 1, size_x)
                for i in members:
                    act(plane * flat + turns[i])
                return carry

            return step

        lax.fori_loop(0, size_x, some(range(1, flat)), 0)
        lax.fori_loop(0, size_x - 1, some(range(1)), 0)

    got_ref[...] = jnp.zeros((count, 4, 128), f32)
    barrier = pltpu.get_barrier_semaphore()

    with scope("a_greet"):
        for_others(
            lambda d: pl.semaphore_signal(barrier, inc=1, device_id=d, device_id_type=LOGICAL)
        )
    for copy in copies[3:]:
        copy.start()

    slot = lax.broadcasted_iota(jnp.int32, (1, 128), 1)
    row_of = lax.broadcasted_iota(jnp.int32, (16, 128), 0)
    cell_of = row_of // 4 * share + row_of % 4
    cell_x = jnp.where(row_of % 4 < share, cell_of // CY, -8).astype(f32)
    cell_y = (cell_of % CY).astype(f32)
    cell_z = lax.broadcasted_iota(jnp.int32, (near_cells, 128), 0).astype(f32) - 1.0
    blank = jnp.zeros((128 - near_cells, 128), bf16)

    own = 4 * tiles

    def edges(t):
        coord_x = jnp.clip(pos_ref[0, pl.ds(t, 1), :] * CX - 0.5, 0.0, CX - 1.0)
        coord_y = jnp.clip(pos_ref[1, pl.ds(t, 1), :] * CY - 0.5, 0.0, CY - 1.0)
        return coord_x, coord_y

    def deposit(t, carry):
        live = (slot < counts_ref[t]).astype(f32)
        mass = mass_ref[pl.ds(t, 1), :] * live
        for comp in range(3):
            shell_ref[own + t, comp:comp + 1, :] = pos_ref[comp, pl.ds(t, 1), :]
        shell_ref[own + t, 3:4, :] = mass
        coord_x, coord_y = edges(t)
        start = jnp.asarray(t, jnp.int32).astype(f32)
        coord_z = (start + pos_ref[2, pl.ds(t, 1), :]) * span - 0.5 - start * span
        plane = hat(coord_x, cell_x) * hat(coord_y, cell_y) * mass
        high, low = halves(plane)
        weight_high, weight_low = halves(hat(coord_z, cell_z))
        weight_ref[t, 0] = weight_high
        weight_ref[t, 1] = weight_low
        rho_ref[t] = stacked_dot(
            high,
            low,
            jnp.concatenate([weight_high, blank], axis=0),
            jnp.concatenate([weight_low, blank], axis=0),
            ((1,), (1,)),
        )
        return carry

    with scope("b_inwait"):
        for copy in copies[:3]:
            copy.wait()
    with scope("c_deposit"):
        lax.fori_loop(0, tiles, deposit, 0, unroll=4)

    quarter = lax.broadcasted_iota(jnp.int32, (8, 128), 1) // width
    lower, even_block = quarter < 2, quarter % 2 == 0

    def exchange(blocks):
        far = [pltpu.roll(b, 64, 1) for b in blocks]
        mixed = [
            jnp.where(lower, blocks[0], far[2]),
            jnp.where(lower, blocks[1], far[3]),
            jnp.where(lower, far[0], blocks[2]),
            jnp.where(lower, far[1], blocks[3]),
        ]
        result = []
        for pair in (0, 2):
            one, two = mixed[pair], mixed[pair + 1]
            result.append(jnp.where(even_block, one, pltpu.roll(two, width, 1)))
            result.append(jnp.where(even_block, pltpu.roll(one, 128 - width, 1), two))
        return result

    with scope("d_tabwait"):
        copies[3].wait()
    with scope("e_transform"):
        rho = [rho_ref[t] for t in range(tiles)]
        half = tiles // 2
        even = [rho[0]] + [rho[t] + rho[tiles - t] for t in range(1, half)] + [rho[half]]
        odd = {t: rho[t] - rho[tiles - t] for t in range(1, half)}
        cosines, sines = tile_waves(even, odd)
        for g in range(groups):
            pair = (cosines[g], sines[g]) if g else (cosines[0], cosines[half])
            high, low = halves(jnp.concatenate(pair, axis=1))
            lines = stacked_dot(high, low, wave_ref[0, g], wave_ref[1, g])
            blocks = [lines[0:8], pltpu.roll(lines[0:8], 4, 0), lines[8:16], pltpu.roll(lines[8:16], 4, 0)]
            for i, block in enumerate(exchange(blocks)):
                spec_ref[g * pack + i] = block[0:4]

    def out_copy(d):
        return pltpu.make_async_remote_copy(
            src_ref=spec_ref.at[d, pl.ds(0, share)],
            dst_ref=got_ref.at[me, pl.ds(0, share)],
            send_sem=out_send,
            recv_sem=out_recv,
            device_id=d,
            device_id_type=LOGICAL,
        )

    def back_copy(d):
        return pltpu.make_async_remote_copy(
            src_ref=back_ref.at[d],
            dst_ref=home_ref.at[me],
            send_sem=back_send,
            recv_sem=back_recv,
            device_id=d,
            device_id_type=LOGICAL,
        )

    def start_all(make):
        for_others(lambda d: make(d).start())

    def wait_all(rest, sem):
        pltpu.make_async_copy(rest, rest, sem).wait()

    with scope("f_barwait"):
        pl.semaphore_wait(barrier, count - 1)
    with scope("g_startout"):
        start_all(out_copy)
    halos = []
    for step_x in (-1, 0, 1):
        for step_y in (-1, 0, 1):
            if step_x == 0 and step_y == 0:
                continue
            slot_there = (1 - step_x) * 3 + 1 - step_y
            halos.append(
                pltpu.make_async_remote_copy(
                    src_ref=shell_ref.at[pl.ds(own, tiles)],
                    dst_ref=shell_ref.at[pl.ds(slot_there * tiles, tiles)],
                    send_sem=halo_send.at[slot_there],
                    recv_sem=halo_recv.at[slot_there],
                    device_id=place((row + step_x + rows) % rows, (col + step_y + cols) % cols),
                    device_id_type=MESH,
                )
            )
    with scope("h_starthalo"):
        for copy in halos:
            copy.start()
    got_ref[me] = spec_ref[me]

    theirs, pulls, strengths = (theirs_0, theirs_1), (pull_0, pull_1), (strength_0, strength_1)
    line_of = lax.broadcasted_iota(jnp.int32, (8, 128), 0)
    first_lines, one_line = line_of < 3, line_of == 3
    square_lines = (line_of > 3) & (line_of < 7)

    def thirds(x):
        high = x.astype(bf16).astype(f32)
        rest = x - high
        middle = rest.astype(bf16).astype(f32)
        return high, middle, rest - middle

    def spread(t, carry):
        tile = shell_ref[own + t]
        spot = jnp.where(first_lines, jnp.concatenate([tile, tile], axis=0) - 0.5, 0.0)
        norm = jnp.sum(spot * spot, axis=0, keepdims=True) + softening
        mine = jnp.where(one_line, norm, jnp.where(square_lines, 1.0, -2.0 * spot))
        high, middle, low = thirds(mine)
        terms = [high, high, middle, high, low, middle, jnp.zeros((80, 128), f32)]
        spread_ref[t] = jnp.transpose(jnp.concatenate(terms, axis=0), (1, 0)).astype(bf16)
        return carry

    with scope("i_spread"):
        lax.fori_loop(0, tiles, spread, 0, unroll=2)

    def describe(t, theirs_ref, pull_ref):
        for n in range(listed):
            entry = list_ref[n, 0, t]
            group = lax.div(entry, tiles)
            layer = entry - group * tiles
            step_x = lax.div(group * 11, 32)
            step_y = group - 3 * step_x
            away = lax.rem(layer - t + 1 + tiles, tiles)
            tile = shell_ref[entry]
            shift = jnp.where(
                line_of % 4 == 0,
                step_x.astype(f32),
                jnp.where(line_of % 4 == 1, step_y.astype(f32), away.astype(f32)),
            )
            spot = jnp.concatenate([tile, tile], axis=0) + (shift - 1.5)
            theirs = jnp.where(
                first_lines, spot, jnp.where(one_line, 1.0, jnp.where(square_lines, spot * spot, 0.0))
            )
            high, middle, low = thirds(theirs)
            one = jnp.concatenate([high, middle], axis=0).astype(bf16)
            two = jnp.concatenate([high, low], axis=0).astype(bf16)
            theirs_ref[n] = jnp.concatenate([one, two, one], axis=0)
            pull = jnp.concatenate(halves(theirs * tile[3:4]), axis=0)
            pull_ref[n] = pull

    product = functools.partial(lax.dot_general, preferred_element_type=f32)

    def attract(t, theirs_ref, strength_ref):
        for n in range(0, listed, 2):
            square = product(
                spread_ref[t][:, :48],
                jnp.concatenate([theirs_ref[n], theirs_ref[n + 1]], axis=1),
                (((1,), (0,)), ((), ())),
            )
            root = lax.rsqrt(square)
            strength = jnp.exp2(square * (-1.0 / (split_scale * math.log(2.0)))) * (root * root * root)
            high, low = halves(strength)
            for k in range(2):
                at = slice(k * 128, (k + 1) * 128)
                strength_ref[2 * (n + k)] = high[:, at]
                strength_ref[2 * (n + k) + 1] = low[:, at]

    def collect(t, pull_ref, strength_ref):
        total = product(
            jnp.concatenate([strength_ref[i] for i in range(2 * listed)], axis=1),
            jnp.concatenate([pull_ref[i // 2] for i in range(2 * listed)], axis=1),
             (((1,), (1,)), ((), ())))
        total = jnp.transpose(total, (1, 0))
        total = total[0:8] + total[8:16]
        tile = shell_ref[own + t]
        spot = jnp.concatenate([tile, tile], axis=0) - 0.5
        short_ref[t] = (total - spot * total[3:4]) * (short_kick * math.exp(softening / split_scale))

    nx, ny = rows * CX, cols * CY
    copies[4].wait()
    copies[5].wait()
    with scope("i2_green"):
        row_in = lax.broadcasted_iota(jnp.int32, (width, nx * ny), 0)
        family, member = me // pack, me % pack
        residue = jnp.where(
            member < pack // 2, family, jnp.where(family == 0, tiles // 2, tiles - family)
        )
        mode_of = tiles * (member % (pack // 2) * modes + row_in % modes) + residue
        alone = mode_of == 0
        wave_z = jnp.where(alone & (row_in >= modes), NZ // 2, mode_of).astype(f32)
        kappa = lanes_ref[0:1, :] + 4.0 * jnp.sin(wave_z * (jnp.pi / NZ)) ** 2
        scale = jnp.where(alone, 0.5, 1.0) * (1.0 / (NZ * nx * ny))
        green = -jnp.exp(-smoothing * kappa) / (kappa + screening) * scale

    with scope("j_waitgot"):
        wait_all(got_ref.at[pl.ds(0, count - 1), pl.ds(0, share)], out_recv)
    with scope("k_plane"):
        copies[6].wait()
        copies[7].wait()
        turned = jnp.transpose(got_ref[...].reshape(count * 4, 128), (1, 0))
        mine = jnp.concatenate(
            [turned[a * width:(a + 1) * width] for a in range(pack)], axis=1
        )
        high, low = halves(mine)
        joined = lambda ref, part: jnp.concatenate([ref[part, i] for i in range(nx * ny // 128)], axis=1)
        waves = stacked_dot(high, low, joined(into_ref, 0), joined(into_ref, 1))
        high, low = halves(waves * green)
        high = jnp.concatenate([high] * pack, axis=0)
        low = jnp.concatenate([low] * pack, axis=0)
        dot = functools.partial(
            lax.dot_general,
            dimension_numbers=(((1,), (1,)), ((), ())),
            preferred_element_type=f32,
        )
        sheet = dot(joined(outof_ref, 0), high) + dot(joined(outof_ref, 0), low) + dot(joined(outof_ref, 1), high)
        for r in range(rows):
            for v in range(ny // 8):
                pick = [
                    sheet[at:at + 8]
                    for at in (((r * CX - 1 + b) % nx) * ny + v * 8 for b in range(pack))
                ]
                window = jnp.where(
                    lower,
                    jnp.where(even_block, pick[0], pick[1]),
                    jnp.where(even_block, pick[2], pick[3]),
                )
                window_ref[r, (v + 1) * 8:(v + 2) * 8, :] = window
                if v == 0:
                    window_ref[r, 8 + ny:16 + ny, :] = window
                if v == ny // 8 - 1:
                    window_ref[r, 0:8, :] = window
        for r in range(rows):
            for c in range(cols):
                d = (r // size_z * size_y + c) * size_z + r % size_z
                back_ref[d] = window_ref[r, c * CY + 7:c * CY + 15, :]
    with scope("l_startback"):
        start_all(back_copy)
    home_ref[me] = back_ref[me]

    with scope("m_waithalo"):
        for copy in halos:
            copy.wait_recv()
    def pairs(k, carry):
        for odd in (0, 1):
            t = 2 * k + odd
            attract(t, theirs[odd], strengths[odd])
            collect(lax.rem(t + tiles - 1, tiles), pulls[1 - odd], strengths[1 - odd])
            describe(lax.rem(t + 1, tiles), theirs[1 - odd], pulls[1 - odd])
        return carry

    with scope("n_pairs"):
        describe(0, theirs[0], pulls[0])
        lax.fori_loop(0, tiles // 2, pairs, 0)
        collect(tiles - 1, pulls[1], strengths[1])
    with scope("o_waithome"):
        wait_all(home_ref.at[pl.ds(0, count - 1)], back_recv)

    with scope("p_lines"):
        for g in range(groups):
            lines = exchange([home_ref[g * pack + i] for i in range(pack)])
            pulls = [lines[b - 1] - lines[b + 1] for b in (1, 2)]
            pulls += [pltpu.roll(lines[b], 1, 0) - pltpu.roll(lines[b], 7, 0) for b in (1, 2)]
            high, low = halves(jnp.concatenate(pulls + [lines[1], lines[2]], axis=0))
            part = stacked_dot(high, low, wave_ref[0, g], wave_ref[1, g], ((1,), (1,)))
            part_ref[g] = part[:, :128]
            part_ref[groups + g] = part[:, 128:]
    with scope("q_invert"):
        for f in range(3):
            at = slice(f * 16, (f + 1) * 16)
            even = [part_ref[g, at] for g in range(groups)] + [part_ref[groups, at]]
            odd = {g: part_ref[groups + g, at] for g in range(1, groups)}
            cosines, sines = tile_waves(even, odd)
            for t in range(tiles):
                if t % half == 0:
                    value = cosines[t]
                elif t < half:
                    value = cosines[t] + sines[t]
                else:
                    value = cosines[tiles - t] - sines[tiles - t]
                if f == 2:
                    value = pltpu.roll(value, 1, 1) - pltpu.roll(value, 127, 1)
                high, low = halves(value)
                field_ref[t, f * 16:(f + 1) * 16, :] = high
                field_ref[t, 48 + f * 16:48 + (f + 1) * 16, :] = low

    cell_near = lax.broadcasted_iota(jnp.int32, (8, 128), 0).astype(f32) - 1.0
    copies[8].wait()

    def interpolate(t, carry):
        coord_x, coord_y = edges(t)
        left, right = hat(coord_x, 0.0), hat(coord_x, 1.0)
        along = hat(coord_y, cell_near)
        here = stacked_dot(
            field_ref[t, 0:48],
            field_ref[t, 48:96],
            jnp.concatenate([weight_ref[t, 0], blank], axis=0),
            jnp.concatenate([weight_ref[t, 1], blank], axis=0),
        )
        live = (slot < counts_ref[t]).astype(f32)
        for f in range(3):
            mixed = here[f * 16:f * 16 + 8] * left + here[f * 16 + 8:f * 16 + 16] * right
            pull = jnp.sum(mixed * along, axis=0, keepdims=True)
            at = (f, pl.ds(t, 1), slice(None))
            out_ref[at] = vel_ref[at] + live * (long_kick * pull + short_ref[t, f:f + 1, :])
        return carry

    with scope("r_interp"):
        lax.fori_loop(0, tiles, interpolate, 0, unroll=4)
    with scope("s_tail"):
        for copy in halos:
            copy.wait_send()
        wait_all(got_ref.at[pl.ds(0, count - 1), pl.ds(0, share)], out_send)
        wait_all(home_ref.at[pl.ds(0, count - 1)], back_send)


def fused_shards(sizes, positions, masses, velocities, tile_counts, neighbour_list):
    size_x, size_y, size_z, tiles, listed = sizes
    rows, cols = size_x * size_z, size_y
    count = rows * cols
    groups = tiles // 2
    near_cells = -(-(NZ // tiles + 3) // 16) * 16
    with jax.ensure_compile_time_eval():
        wave, into, outof, lanes = tables(size_x, size_y, size_z, tiles)
    anywhere = pl.BlockSpec(memory_space=pl.ANY)
    dma = pltpu.SemaphoreType.DMA
    kicked = pl.pallas_call(
        functools.partial(kick_kernel, sizes),
        out_shape=pltpu.VMEM((3, tiles, 128), f32),
        in_specs=[anywhere] * 9,
        out_specs=pl.BlockSpec(memory_space=pltpu.VMEM),
        scratch_shapes=[
            pltpu.VMEM((3, tiles, 128), f32),
            pltpu.VMEM((tiles, 128), f32),
            pltpu.VMEM((3, tiles, 128), f32),
            pltpu.VMEM(lanes.shape, f32),
            pltpu.SMEM((tiles,), jnp.int32),
            pltpu.SMEM((listed, 1, tiles), jnp.int32),
            pltpu.VMEM(wave.shape, bf16),
            pltpu.VMEM(into.shape, bf16),
            pltpu.VMEM(outof.shape, bf16),
            pltpu.VMEM((9 * tiles, 4, 128), f32),
            pltpu.VMEM((tiles, 16, 128), f32),
            pltpu.VMEM((tiles, 2, near_cells, 128), bf16),
            pltpu.VMEM((count, 4, 128), f32),
            pltpu.VMEM((count, 4, 128), f32),
            pltpu.VMEM((rows, cols * CY + 16, 128), f32),
            pltpu.VMEM((count, 8, 128), f32),
            pltpu.VMEM((count, 8, 128), f32),
            pltpu.VMEM((2 * groups, 48, 128), f32),
            pltpu.VMEM((tiles, 96, 128), bf16),
            pltpu.VMEM((tiles, 128, 128), bf16),
            pltpu.VMEM((listed, 48, 128), bf16),
            pltpu.VMEM((listed, 48, 128), bf16),
            pltpu.VMEM((listed, 16, 128), bf16),
            pltpu.VMEM((listed, 16, 128), bf16),
            pltpu.VMEM((2 * listed, 128, 128), bf16),
            pltpu.VMEM((2 * listed, 128, 128), bf16),
            pltpu.VMEM((tiles, 8, 128), f32),
            dma((9,)),
            dma((9,)),
            dma((9,)),
            dma,
            dma,
            dma,
            dma,
        ],
        compiler_params=pltpu.CompilerParams(collective_id=0, has_side_effects=True),
        name="kick",
    )(
        jnp.transpose(positions[0, 0], (1, 0, 2)),
        masses.reshape(tiles, 128),
        jnp.transpose(velocities[0, 0], (1, 0, 2)),
        lanes,
        tile_counts.reshape(tiles),
        jnp.transpose(neighbour_list[0], (2, 0, 1)),
        wave,
        into,
        outof,
    )
    return jnp.transpose(kicked, (1, 0, 2))[None, None]


def fits(sizes):
    size_x, size_y, size_z, tiles, listed = sizes
    count = size_x * size_y * size_z
    if CX != 2 or CY != 6 or count != 32 or tiles != 16 or size_y * CY % 8:
        return False
    return NZ // 2 == 16 * count and NZ // tiles + 3 < 127


def solution(mesh):
    placed = (
        P(("gx", "gz"), "gy", None, None, None),
        P(("gx", "gz"), "gy", None, None),
        P(("gx", "gz"), "gy", None, None, None),
        P(("gx", "gz"), "gy", None),
        P(("gx", "gz"), "gy", None, None),
    )

    def local(positions, masses, velocities, tile_counts, neighbour_list):
        sizes = tuple(mesh.shape[axis] for axis in ("gx", "gy", "gz"))
        sizes = sizes + (positions.shape[2], neighbour_list.shape[3])
        part = functools.partial(fused_shards, sizes) if fits(sizes) else shards
        return part(positions, masses, velocities, tile_counts, neighbour_list)

    return jax.shard_map(
        local,
        mesh=mesh,
        in_specs=placed,
        out_specs=P(("gx", "gz"), "gy", None, None, None),
        check_vma=False,
    )
```

```python
import contextlib
import functools
import math

import jax
import jax.numpy as jnp
import numpy as np
from jax import lax
from jax.experimental import pallas as pl
from jax.experimental.pallas import tpu as pltpu
from jax.sharding import PartitionSpec as P

CX = 2
CY = 6
NZ = 1024


smoothing = 0.1
screening = 0.01
split_scale = 2.0
softening = 0.05
long_kick = 1.0
short_kick = 0.05
highest = lax.Precision.HIGHEST


def padded(cells, sides, width):
    for axis, dim in sides:
        count = lax.axis_size(axis)
        head = lax.slice_in_dim(cells, 0, width, axis=dim)
        tail = lax.slice_in_dim(cells, cells.shape[dim] - width, cells.shape[dim], axis=dim)
        cells = jnp.concatenate(
            [
                lax.ppermute(tail, axis, [(i, (i + 1) % count) for i in range(count)]),
                cells,
                lax.ppermute(head, axis, [((i + 1) % count, i) for i in range(count)]),
            ],
            axis=dim,
        )
    return cells


def wave_terms(length, first_index, extent):
    wavenum = (first_index + jnp.arange(extent, dtype=jnp.int32)).astype(jnp.float32)
    angles = wavenum * (2.0 * jnp.pi / length)
    return (4.0 * jnp.sin(0.5 * angles) ** 2, jnp.sin(angles))


def cloud_stencil(positions, cells_x, cells_y, cells_z, tiles):
    span = cells_z // tiles
    tile_row = jnp.arange(tiles, dtype=jnp.int32)[:, None]
    coord_x = positions[..., 0, :] * cells_x - 0.5
    base_x = jnp.clip(jnp.floor(coord_x), 0, cells_x - 2)
    frac_x = jnp.clip(coord_x - base_x, 0.0, 1.0)
    coord_y = positions[..., 1, :] * cells_y - 0.5
    base_y = jnp.clip(jnp.floor(coord_y), 0, cells_y - 2)
    frac_y = jnp.clip(coord_y - base_y, 0.0, 1.0)
    coord_z = (tile_row + positions[..., 2, :]) * span - 0.5
    base_z = jnp.floor(coord_z)
    frac_z = coord_z - base_z
    index_x = base_x.astype(jnp.int32)
    index_y = base_y.astype(jnp.int32)
    index_z = base_z.astype(jnp.int32) % cells_z
    cell_list = []
    weight_list = []
    for offset_x in (0, 1):
        for offset_y in (0, 1):
            for offset_z in (0, 1):
                weight_x = frac_x if offset_x else 1.0 - frac_x
                weight_y = frac_y if offset_y else 1.0 - frac_y
                weight_z = frac_z if offset_z else 1.0 - frac_z
                cell_list.append(
                    ((index_x + offset_x) * cells_y + index_y + offset_y) * cells_z
                    + (index_z + offset_z) % cells_z
                )
                weight_list.append(weight_x * weight_y * weight_z)
    return (jnp.stack(cell_list, axis=-2), jnp.stack(weight_list, axis=-2))


def pair_accel(receivers, sources, shifts):
    parts = []
    for comp in range(3):
        parts.append(
            shifts[:, :, comp, None, None]
            + sources[:, :, comp, None, :]
            - receivers[:, None, comp, :, None]
        )
    square = parts[0] * parts[0] + parts[1] * parts[1] + parts[2] * parts[2]
    strength = (
        sources[:, :, 3, None, :] * jnp.exp(-square / split_scale) * (square + softening) ** (-1.5)
    )
    return jnp.stack([jnp.sum(strength * parts[comp], axis=(1, 3)) for comp in range(3)], axis=1)


def split_length(length):
    divisor = 1
    for factor in range(1, math.isqrt(length) + 1):
        if length % factor == 0:
            divisor = factor
    return divisor


def dft_table(length):
    indices = jnp.arange(length, dtype=jnp.int32)
    phases = indices[:, None] * indices[None, :] % length
    angles = phases.astype(jnp.float32) * (2.0 * jnp.pi / length)
    return (jnp.cos(angles), jnp.sin(angles))


def twiddle_table(outer, inner):
    length = outer * inner
    phases = (
        jnp.arange(outer, dtype=jnp.int32)[:, None]
        * jnp.arange(inner, dtype=jnp.int32)[None, :]
        % length
    )
    angles = phases.astype(jnp.float32) * (2.0 * jnp.pi / length)
    return (jnp.cos(angles), jnp.sin(angles))


def complex_mix(real, imag, cosine, sine_table, sign, form):
    real_cos = jnp.einsum(form, real, cosine, precision=highest)
    real_sin = jnp.einsum(form, real, sine_table, precision=highest)
    imag_cos = jnp.einsum(form, imag, cosine, precision=highest)
    imag_sin = jnp.einsum(form, imag, sine_table, precision=highest)
    return (real_cos - sign * imag_sin, imag_cos + sign * real_sin)


def transform_last(real, imag, sign):
    length = real.shape[-1]
    outer = split_length(length)
    inner = length // outer
    leading = real.shape[:-1]
    real = real.reshape(leading + (outer, inner))
    imag = imag.reshape(leading + (outer, inner))
    cos_outer, sin_outer = dft_table(outer)
    real, imag = complex_mix(real, imag, cos_outer, sin_outer, sign, "...pq,pk->...kq")
    turn_cos, turn_sin = twiddle_table(outer, inner)
    real, imag = (
        real * turn_cos - sign * imag * turn_sin,
        imag * turn_cos + sign * real * turn_sin,
    )
    cos_inner, sin_inner = dft_table(inner)
    real, imag = complex_mix(real, imag, cos_inner, sin_inner, sign, "...kq,qm->...mk")
    return (real.reshape(leading + (length,)), imag.reshape(leading + (length,)))


def transform_axis(fields, axis, sign):
    real = jnp.moveaxis(fields[:, 0], axis, -1)
    imag = jnp.moveaxis(fields[:, 1], axis, -1)
    real, imag = transform_last(real, imag, sign)
    return jnp.stack([jnp.moveaxis(real, -1, axis), jnp.moveaxis(imag, -1, axis)], axis=1)


def rotate(fields, factor):
    return jnp.stack([factor * fields[:, 1], -factor * fields[:, 0]], axis=1)


def shards(positions, masses, velocities, tile_counts, neighbour_list):
    tiles = positions.shape[2]
    listed = neighbour_list.shape[3]
    slot_index = jnp.arange(128, dtype=jnp.int32)
    live_mask = (slot_index < tile_counts[..., None]).astype(jnp.float32)
    mass_live = masses * live_mask
    packed = jnp.concatenate([positions, mass_live[:, :, :, None, :]], axis=3)
    shell = padded(packed, ((("gx", "gz"), 0), ("gy", 1)), 1)
    cell_index, cloud_weights = cloud_stencil(positions, CX, CY, NZ, tiles)
    amounts = cloud_weights * mass_live[:, :, :, None, :]
    density = jax.ops.segment_sum(
        amounts.reshape(-1), cell_index.reshape(-1), num_segments=CX * CY * NZ
    ).reshape(CX, CY, NZ)
    spectrum = jnp.stack([density, jnp.zeros_like(density)], axis=0)[None]
    spectrum = transform_axis(spectrum, 3, -1.0)
    spectrum = lax.all_to_all(spectrum, "gy", split_axis=4, concat_axis=3, tiled=True)
    span_y = spectrum.shape[3]
    spectrum = transform_axis(spectrum, 2, -1.0)
    spectrum = lax.all_to_all(spectrum, ("gx", "gz"), split_axis=3, concat_axis=2, tiled=True)
    span_x = spectrum.shape[2]
    spectrum = transform_axis(spectrum, 1, -1.0)
    block_y = spectrum.shape[3]
    block_z = spectrum.shape[4]
    kappa_x, sine_x = wave_terms(span_x, 0, span_x)
    kappa_y, sine_y = wave_terms(span_y, lax.axis_index(("gx", "gz")) * block_y, block_y)
    kappa_z, sine_z = wave_terms(NZ, lax.axis_index("gy") * block_z, block_z)
    kappa_sum = kappa_x[:, None, None] + kappa_y[None, :, None] + kappa_z[None, None, :]
    potential = spectrum * (-jnp.exp(-smoothing * kappa_sum) / (kappa_sum + screening))
    fields = jnp.concatenate([rotate(potential, sine_x[:, None, None]), potential], axis=0)
    fields = transform_axis(fields, 1, 1.0) / span_x
    fields = lax.all_to_all(fields, ("gx", "gz"), split_axis=2, concat_axis=3, tiled=True)
    whole_sine_y = wave_terms(span_y, 0, span_y)[1]
    fields = jnp.concatenate(
        [fields[0:1], rotate(fields[1:2], whole_sine_y[None, :, None]), fields[1:2]], axis=0
    )
    fields = transform_axis(fields, 2, 1.0) / span_y
    fields = lax.all_to_all(fields, "gy", split_axis=3, concat_axis=4, tiled=True)
    whole_sine_z = wave_terms(NZ, 0, NZ)[1]
    fields = jnp.concatenate(
        [fields[0:2], rotate(fields[2:3], whole_sine_z[None, None, :])], axis=0
    )
    fields = transform_axis(fields, 3, 1.0) / NZ
    forces = fields[:, 0]
    flat_forces = forces.reshape(3, -1)
    picked = flat_forces[:, cell_index]
    long_accel = jnp.moveaxis(jnp.sum(cloud_weights[None] * picked, axis=4), 0, 3)
    flat_shell = shell.reshape(9 * tiles, 4, 128)
    own_list = neighbour_list[0, 0]
    sources = flat_shell[own_list]
    groups = own_list // tiles
    layers = own_list % tiles
    tile_row = jnp.arange(tiles, dtype=jnp.int32)[:, None]
    shifts = jnp.stack(
        [groups // 3 - 1, groups % 3 - 1, (layers - tile_row + 1) % tiles - 1], axis=-1
    ).astype(jnp.float32)
    short_accel = lax.map(
        lambda pieces: pair_accel(*pieces),
        (
            positions[0, 0].reshape(tiles, 1, 3, 128),
            sources.reshape(tiles, 1, listed, 4, 128),
            shifts.reshape(tiles, 1, listed, 3),
        ),
    )
    short_accel = short_accel.reshape(1, 1, tiles, 3, 128)
    return velocities + live_mask[:, :, :, None, :] * (
        long_kick * long_accel + short_kick * short_accel
    )


MESH = pl.DeviceIdType.MESH
LOGICAL = pl.DeviceIdType.LOGICAL
f32 = jnp.float32
bf16 = jnp.bfloat16


def halves(x):
    high = x.astype(bf16)
    return high, (x - high.astype(f32)).astype(bf16)


def dot3(a, b, dims=((1,), (0,))):
    dot = functools.partial(
        lax.dot_general, dimension_numbers=(dims, ((), ())), preferred_element_type=f32
    )
    return dot(a[0], b[0]) + dot(a[1], b[0]) + dot(a[0], b[1])


def scope(name):
    return contextlib.nullcontext()


def hat(coord, cell):
    return jnp.maximum(0.0, 1.0 - jnp.abs(coord - cell))


def np_halves(table):
    table = jnp.asarray(np.asarray(table, np.float32))
    return jnp.stack(halves(table))


def stacked_dot(high, low, table_high, table_low, dims=((1,), (0,))):
    dot = functools.partial(
        lax.dot_general, dimension_numbers=(dims, ((), ())), preferred_element_type=f32
    )
    rows = high.shape[0]
    both = dot(jnp.concatenate([high, low], axis=0), table_high)
    return both[:rows] + both[rows:] + dot(high, table_low)


def joint_dot(high, low, table_high, table_low):
    rows = high.shape[0]
    left = jnp.concatenate(
        [
            jnp.concatenate([high, high], axis=1),
            jnp.concatenate([low, jnp.zeros_like(low)], axis=1),
        ],
        axis=0,
    )
    both = lax.dot_general(
        left,
        jnp.concatenate([table_high, table_low], axis=0),
        (((1,), (0,)), ((), ())),
        preferred_element_type=f32,
    )
    return both[:rows] + both[rows:]


def tables(size_x, size_y, size_z, tiles):
    rows, cols = size_x * size_z, size_y
    count = rows * cols
    modes = NZ // 2 // count
    pack = 128 // (2 * modes)
    groups = tiles // 2
    lane = np.arange(128)
    member, imag, slot = lane // (2 * modes), lane % (2 * modes) >= modes, lane % modes
    cells = np.arange(128) - 1
    cells[127] = -2
    used = cells <= NZ // tiles + 1
    waves = []
    for g in range(groups):
        plus = member < pack // 2
        residue = np.where(plus, g, tiles - g if g else tiles // 2)
        mode = tiles * (member % (pack // 2) * modes + slot) + residue
        angle = 2 * np.pi * ((cells[:, None] * mode[None]) % NZ) / NZ
        direct = np.where(imag[None], -np.sin(angle), np.cos(angle))
        crossed = np.where(imag[None], np.cos(angle), np.sin(angle))
        crossed = np.where(plus[None], -crossed, crossed)
        if g == 0:
            nyquist = (mode == 0) & imag
            direct = np.where(nyquist[None], np.cos(np.pi * (cells % 2))[:, None], direct)
            direct, crossed = (
                np.where(plus[None], direct, 0.0),
                np.where(plus[None], 0.0, direct),
            )
        both = np.stack([direct, crossed])
        waves.append(np.where(used[None, :, None], both, 0.0).reshape(256, 128))
    nx, ny = rows * CX, cols * CY
    index = np.arange(4 * count * 4)
    device, row = index // 4 % count, index // (4 * count) * (CX * CY // 4) + index % 4
    real = index % 4 < CX * CY // 4
    place_x = device // (size_y * size_z) * size_z + device % size_z
    place_y = device // size_z % size_y
    here_x = np.where(real, place_x * CX + row // CY, 0)
    here_y = np.where(real, place_y * CY + row % CY, 0)
    wave_x, wave_y = np.arange(nx * ny) // ny, np.arange(nx * ny) % ny

    def cas(x, y):
        ax = 2 * np.pi * (x[:, None] * wave_x[None] % nx) / nx
        ay = 2 * np.pi * (y[:, None] * wave_y[None] % ny) / ny
        return (np.cos(ax) + np.sin(ax)) * (np.cos(ay) + np.sin(ay))

    into = cas(here_x, here_y) * real[:, None]
    outof = cas(wave_x, wave_y)
    lanes = np.zeros((8, nx * ny))
    lanes[:] = 4 * np.sin(np.pi * wave_x / nx) ** 2 + 4 * np.sin(np.pi * wave_y / ny) ** 2
    waves = np.stack(waves)
    unwaves = waves.reshape(groups, 2, 128, 128).transpose(0, 1, 3, 2)
    return np_halves(waves), np_halves(unwaves), np_halves(lane_tiles(into)), np_halves(lane_tiles(outof)), jnp.asarray(lanes, f32)


def lane_tiles(table):
    return np.stack(np.split(table, table.shape[1] // 128, axis=1))


def tile_waves(even, odd):
    half = len(even) - 1
    ring, quarter = 2 * half, half // 2

    def total(terms):
        result = None
        for factor, value in terms:
            if abs(factor) < 1e-12:
                continue
            if abs(abs(factor) - 1.0) < 1e-12:
                if result is None:
                    result = value if factor > 0 else -value
                else:
                    result = result + value if factor > 0 else result - value
            else:
                part = value * float(abs(factor))
                if result is None:
                    result = part if factor > 0 else -part
                else:
                    result = result + part if factor > 0 else result - part
        return result

    sums = [even[t] + even[half - t] for t in range(quarter)]
    gaps = [even[t] - even[half - t] for t in range(quarter)]
    odd_sums = {t: odd[t] + odd[half - t] for t in range(1, quarter)}
    odd_gaps = {t: odd[t] - odd[half - t] for t in range(1, quarter)}
    cosines, sines = [], {}
    for r in range(half + 1):
        cos = [math.cos(2 * math.pi * r * t / ring) for t in range(quarter + 1)]
        sin = [math.sin(2 * math.pi * r * t / ring) for t in range(quarter + 1)]
        terms = [(cos[t], (gaps if r % 2 else sums)[t]) for t in range(quarter)]
        if r % 2 == 0:
            terms.append((cos[quarter], even[quarter]))
        cosines.append(total(terms))
        if 0 < r < half:
            terms = [(sin[t], (odd_sums if r % 2 else odd_gaps)[t]) for t in range(1, quarter)]
            if r % 2:
                terms.append((sin[quarter], odd[quarter]))
            sines[r] = total(terms)
    return cosines, sines


def kick_kernel(
    sizes,
    pos_hbm, mass_hbm, vel_hbm, lanes_hbm, counts_hbm, list_hbm, wave_hbm, into_hbm, outof_hbm, unwave_hbm,
    out_ref,
    pos_ref, mass_ref, vel_ref, lanes_ref, counts_ref, list_ref, wave_ref, into_ref, outof_ref, unwave_ref,
    shell_ref, rho_ref, weight_ref, spec_ref, got_ref, window_ref,
    back_ref, home_ref, part_ref, field_ref, spread_ref, theirs_0, theirs_1, pull_0, pull_1, strength_0, strength_1, short_ref,
    input_sem, halo_send, halo_recv, out_send, out_recv, back_send, back_recv,
):
    size_x, size_y, size_z, tiles, listed = sizes
    rows, cols = size_x * size_z, size_y
    count = rows * cols
    modes = NZ // 2 // count
    width = 2 * modes
    pack = 128 // width
    groups = tiles // 2
    span = NZ // tiles
    near_cells = -(-(span + 3) // 16) * 16
    share = CX * CY // 4
    flat = size_y * size_z
    gx, gy, gz = lax.axis_index("gx"), lax.axis_index("gy"), lax.axis_index("gz")
    row, col = gx * size_z + gz, gy
    me = (gx * size_y + gy) * size_z + gz

    copies = [
        pltpu.make_async_copy(a, b, input_sem.at[i])
        for i, (a, b) in enumerate(
            (
                (pos_hbm, pos_ref),
                (mass_hbm, mass_ref),
                (counts_hbm, counts_ref),
                (wave_hbm, wave_ref),
                (list_hbm, list_ref),
                (lanes_hbm, lanes_ref),
                (into_hbm, into_ref),
                (outof_hbm, outof_ref),
                (vel_hbm, vel_ref),
                (unwave_hbm, unwave_ref),
            )
        )
    ]
    for copy in copies[:3]:
        copy.start()

    def place(r, c):
        return (r // size_z, c, r % size_z)

    first = size_x - 1 - gx
    second = lax.rem(gx + size_x // 2, size_x)
    third = size_x - 1 - second
    spot_here = gy * size_z + gz

    turns = [lax.rem(spot_here + i, flat) for i in range(flat)]

    def for_others(act):
        def some(members):
            def step(p, carry):
                if size_x == 4:
                    plane = jnp.where(
                        p == 0, first, jnp.where(p == 1, second, jnp.where(p == 2, third, gx))
                    )
                else:
                    plane = lax.rem(gx + p + 1, size_x)
                for i in members:
                    act(plane * flat + turns[i])
                return carry

            return step

        lax.fori_loop(0, size_x, some(range(1, flat)), 0)
        lax.fori_loop(0, size_x - 1, some(range(1)), 0)

    got_ref[...] = jnp.zeros((count, 4, 128), f32)
    barrier = pltpu.get_barrier_semaphore()

    with scope("a_greet"):
        for_others(
            lambda d: pl.semaphore_signal(barrier, inc=1, device_id=d, device_id_type=LOGICAL)
        )
    for copy in copies[3:]:
        copy.start()

    slot = lax.broadcasted_iota(jnp.int32, (1, 128), 1)
    row_of = lax.broadcasted_iota(jnp.int32, (16, 128), 0)
    cell_of = row_of // 4 * share + row_of % 4
    cell_x = jnp.where(row_of % 4 < share, cell_of // CY, -8).astype(f32)
    cell_y = (cell_of % CY).astype(f32)
    cell_z = lax.broadcasted_iota(jnp.int32, (near_cells, 128), 0).astype(f32) - 1.0
    blank = jnp.zeros((128 - near_cells, 128), bf16)

    own = 4 * tiles

    def edges(t):
        coord_x = jnp.clip(pos_ref[0, pl.ds(t, 1), :] * CX - 0.5, 0.0, CX - 1.0)
        coord_y = jnp.clip(pos_ref[1, pl.ds(t, 1), :] * CY - 0.5, 0.0, CY - 1.0)
        return coord_x, coord_y

    def deposit(t, carry):
        live = (slot < counts_ref[t]).astype(f32)
        mass = mass_ref[pl.ds(t, 1), :] * live
        for comp in range(3):
            shell_ref[own + t, comp:comp + 1, :] = pos_ref[comp, pl.ds(t, 1), :]
        shell_ref[own + t, 3:4, :] = mass
        coord_x, coord_y = edges(t)
        start = jnp.asarray(t, jnp.int32).astype(f32)
        coord_z = (start + pos_ref[2, pl.ds(t, 1), :]) * span - 0.5 - start * span
        plane = hat(coord_x, cell_x) * hat(coord_y, cell_y) * mass
        high, low = halves(plane)
        weight_high, weight_low = halves(hat(coord_z, cell_z))
        weight_ref[t, 0] = weight_high
        weight_ref[t, 1] = weight_low
        rho_ref[t] = stacked_dot(
            high,
            low,
            jnp.concatenate([weight_high, blank], axis=0),
            jnp.concatenate([weight_low, blank], axis=0),
            ((1,), (1,)),
        )
        return carry

    with scope("b_inwait"):
        for copy in copies[:3]:
            copy.wait()
    with scope("c_deposit"):
        lax.fori_loop(0, tiles, deposit, 0, unroll=4)

    quarter = lax.broadcasted_iota(jnp.int32, (8, 128), 1) // width
    lower, even_block = quarter < 2, quarter % 2 == 0

    def exchange(blocks):
        far = [pltpu.roll(b, 64, 1) for b in blocks]
        mixed = [
            jnp.where(lower, blocks[0], far[2]),
            jnp.where(lower, blocks[1], far[3]),
            jnp.where(lower, far[0], blocks[2]),
            jnp.where(lower, far[1], blocks[3]),
        ]
        result = []
        for pair in (0, 2):
            one, two = mixed[pair], mixed[pair + 1]
            result.append(jnp.where(even_block, one, pltpu.roll(two, width, 1)))
            result.append(jnp.where(even_block, pltpu.roll(one, 128 - width, 1), two))
        return result

    with scope("d_tabwait"):
        copies[3].wait()
    with scope("e_transform"):
        rho = [rho_ref[t] for t in range(tiles)]
        half = tiles // 2
        even = [rho[0]] + [rho[t] + rho[tiles - t] for t in range(1, half)] + [rho[half]]
        odd = {t: rho[t] - rho[tiles - t] for t in range(1, half)}
        cosines, sines = tile_waves(even, odd)
        for g in range(groups):
            pair = (cosines[g], sines[g]) if g else (cosines[0], cosines[half])
            high, low = halves(jnp.concatenate(pair, axis=1))
            lines = stacked_dot(high, low, wave_ref[0, g], wave_ref[1, g])
            blocks = [lines[0:8], pltpu.roll(lines[0:8], 4, 0), lines[8:16], pltpu.roll(lines[8:16], 4, 0)]
            for i, block in enumerate(exchange(blocks)):
                spec_ref[g * pack + i] = block[0:4]

    def out_copy(d):
        return pltpu.make_async_remote_copy(
            src_ref=spec_ref.at[d, pl.ds(0, share)],
            dst_ref=got_ref.at[me, pl.ds(0, share)],
            send_sem=out_send,
            recv_sem=out_recv,
            device_id=d,
            device_id_type=LOGICAL,
        )

    def back_copy(d):
        return pltpu.make_async_remote_copy(
            src_ref=back_ref.at[d],
            dst_ref=home_ref.at[me],
            send_sem=back_send,
            recv_sem=back_recv,
            device_id=d,
            device_id_type=LOGICAL,
        )

    def start_all(make):
        for_others(lambda d: make(d).start())

    def wait_all(rest, sem):
        pltpu.make_async_copy(rest, rest, sem).wait()

    with scope("f_barwait"):
        pl.semaphore_wait(barrier, count - 1)
    with scope("g_startout"):
        start_all(out_copy)
    halos = []
    for step_x in (-1, 0, 1):
        for step_y in (-1, 0, 1):
            if step_x == 0 and step_y == 0:
                continue
            slot_there = (1 - step_x) * 3 + 1 - step_y
            halos.append(
                pltpu.make_async_remote_copy(
                    src_ref=shell_ref.at[pl.ds(own, tiles)],
                    dst_ref=shell_ref.at[pl.ds(slot_there * tiles, tiles)],
                    send_sem=halo_send.at[slot_there],
                    recv_sem=halo_recv.at[slot_there],
                    device_id=place((row + step_x + rows) % rows, (col + step_y + cols) % cols),
                    device_id_type=MESH,
                )
            )
    with scope("h_starthalo"):
        for copy in halos:
            copy.start()
    got_ref[me] = spec_ref[me]

    theirs, pulls, strengths = (theirs_0, theirs_1), (pull_0, pull_1), (strength_0, strength_1)
    line_of = lax.broadcasted_iota(jnp.int32, (8, 128), 0)
    first_lines, one_line = line_of < 3, line_of == 3
    square_lines = (line_of > 3) & (line_of < 7)

    def thirds(x):
        high = x.astype(bf16).astype(f32)
        rest = x - high
        middle = rest.astype(bf16).astype(f32)
        return high, middle, rest - middle

    def spread(t, carry):
        tile = shell_ref[own + t]
        spot = jnp.where(first_lines, jnp.concatenate([tile, tile], axis=0) - 0.5, 0.0)
        norm = jnp.sum(spot * spot, axis=0, keepdims=True) + softening
        mine = jnp.where(one_line, norm, jnp.where(square_lines, 1.0, -2.0 * spot))
        high, middle, low = thirds(mine)
        terms = [high, high, middle, high, low, middle, jnp.zeros((80, 128), f32)]
        spread_ref[t] = jnp.transpose(jnp.concatenate(terms, axis=0), (1, 0)).astype(bf16)
        return carry

    with scope("i_spread"):
        lax.fori_loop(0, tiles, spread, 0, unroll=2)

    def describe(t, theirs_ref, pull_ref):
        for n in range(listed):
            entry = list_ref[n, 0, t]
            group = lax.div(entry, tiles)
            layer = entry - group * tiles
            step_x = lax.div(group * 11, 32)
            step_y = group - 3 * step_x
            away = lax.rem(layer - t + 1 + tiles, tiles)
            tile = shell_ref[entry]
            shift = jnp.where(
                line_of % 4 == 0,
                step_x.astype(f32),
                jnp.where(line_of % 4 == 1, step_y.astype(f32), away.astype(f32)),
            )
            spot = jnp.concatenate([tile, tile], axis=0) + (shift - 1.5)
            theirs = jnp.where(
                first_lines, spot, jnp.where(one_line, 1.0, jnp.where(square_lines, spot * spot, 0.0))
            )
            high, middle, low = thirds(theirs)
            one = jnp.concatenate([high, middle], axis=0).astype(bf16)
            two = jnp.concatenate([high, low], axis=0).astype(bf16)
            theirs_ref[n] = jnp.concatenate([one, two, one], axis=0)
            pull = jnp.concatenate(halves(theirs * tile[3:4]), axis=0)
            pull_ref[n] = pull

    product = functools.partial(lax.dot_general, preferred_element_type=f32)

    def attract(t, theirs_ref, strength_ref):
        for n in range(0, listed, 2):
            square = product(
                spread_ref[t][:, :48],
                jnp.concatenate([theirs_ref[n], theirs_ref[n + 1]], axis=1),
                (((1,), (0,)), ((), ())),
            )
            root = lax.rsqrt(square)
            strength = jnp.exp2(square * (-1.0 / (split_scale * math.log(2.0)))) * (root * root * root)
            high, low = halves(strength)
            for k in range(2):
                at = slice(k * 128, (k + 1) * 128)
                strength_ref[2 * (n + k)] = high[:, at]
                strength_ref[2 * (n + k) + 1] = low[:, at]

    def collect(t, pull_ref, strength_ref):
        total = product(
            jnp.concatenate([strength_ref[i] for i in range(2 * listed)], axis=1),
            jnp.concatenate([pull_ref[i // 2] for i in range(2 * listed)], axis=1),
             (((1,), (1,)), ((), ())))
        total = jnp.transpose(total, (1, 0))
        total = total[0:8] + total[8:16]
        tile = shell_ref[own + t]
        spot = jnp.concatenate([tile, tile], axis=0) - 0.5
        short_ref[t] = (total - spot * total[3:4]) * (short_kick * math.exp(softening / split_scale))

    nx, ny = rows * CX, cols * CY
    copies[4].wait()
    copies[5].wait()
    with scope("i2_green"):
        row_in = lax.broadcasted_iota(jnp.int32, (width, nx * ny), 0)
        family, member = me // pack, me % pack
        residue = jnp.where(
            member < pack // 2, family, jnp.where(family == 0, tiles // 2, tiles - family)
        )
        mode_of = tiles * (member % (pack // 2) * modes + row_in % modes) + residue
        alone = mode_of == 0
        wave_z = jnp.where(alone & (row_in >= modes), NZ // 2, mode_of).astype(f32)
        kappa = lanes_ref[0:1, :] + 4.0 * jnp.sin(wave_z * (jnp.pi / NZ)) ** 2
        scale = jnp.where(alone, 0.5, 1.0) * (1.0 / (NZ * nx * ny))
        green = -jnp.exp(-smoothing * kappa) / (kappa + screening) * scale

    with scope("j_waitgot"):
        wait_all(got_ref.at[pl.ds(0, count - 1), pl.ds(0, share)], out_recv)
    with scope("k_plane"):
        copies[6].wait()
        copies[7].wait()
        turned = jnp.transpose(got_ref[...].reshape(count * 4, 128), (1, 0))
        mine = jnp.concatenate(
            [turned[a * width:(a + 1) * width] for a in range(pack)], axis=1
        )
        high, low = halves(mine)
        joined = lambda ref, part: jnp.concatenate([ref[part, i] for i in range(nx * ny // 128)], axis=1)
        waves = stacked_dot(high, low, joined(into_ref, 0), joined(into_ref, 1))
        high, low = halves(waves * green)
        high = jnp.concatenate([high] * pack, axis=0)
        low = jnp.concatenate([low] * pack, axis=0)
        dot = functools.partial(
            lax.dot_general,
            dimension_numbers=(((1,), (1,)), ((), ())),
            preferred_element_type=f32,
        )
        sheet = dot(
            jnp.concatenate([joined(outof_ref, 0), joined(outof_ref, 0), joined(outof_ref, 1)], axis=1),
            jnp.concatenate([high, low, high], axis=1),
        )
        for r in range(rows):
            for v in range(ny // 8):
                pick = [
                    sheet[at:at + 8]
                    for at in (((r * CX - 1 + b) % nx) * ny + v * 8 for b in range(pack))
                ]
                window = jnp.where(
                    lower,
                    jnp.where(even_block, pick[0], pick[1]),
                    jnp.where(even_block, pick[2], pick[3]),
                )
                window_ref[r, (v + 1) * 8:(v + 2) * 8, :] = window
                if v == 0:
                    window_ref[r, 8 + ny:16 + ny, :] = window
                if v == ny // 8 - 1:
                    window_ref[r, 0:8, :] = window
        for r in range(rows):
            for c in range(cols):
                d = (r // size_z * size_y + c) * size_z + r % size_z
                back_ref[d] = window_ref[r, c * CY + 7:c * CY + 15, :]
    with scope("l_startback"):
        start_all(back_copy)
    home_ref[me] = back_ref[me]

    with scope("m_waithalo"):
        for copy in halos:
            copy.wait_recv()
    def pairs(k, carry):
        for odd in (0, 1):
            t = 2 * k + odd
            attract(t, theirs[odd], strengths[odd])
            collect(lax.rem(t + tiles - 1, tiles), pulls[1 - odd], strengths[1 - odd])
            describe(lax.rem(t + 1, tiles), theirs[1 - odd], pulls[1 - odd])
        return carry

    with scope("n_pairs"):
        describe(0, theirs[0], pulls[0])
        lax.fori_loop(0, tiles // 2, pairs, 0, unroll=4)
        collect(tiles - 1, pulls[1], strengths[1])
    with scope("o_waithome"):
        wait_all(home_ref.at[pl.ds(0, count - 1)], back_recv)

    copies[9].wait()
    with scope("p_lines"):
        for g in range(groups):
            lines = exchange([home_ref[g * pack + i] for i in range(pack)])
            pulls = [lines[b - 1] - lines[b + 1] for b in (1, 2)]
            pulls += [pltpu.roll(lines[b], 1, 0) - pltpu.roll(lines[b], 7, 0) for b in (1, 2)]
            high, low = halves(jnp.concatenate(pulls + [lines[1], lines[2]], axis=0))
            part = joint_dot(
                high,
                low,
                jnp.concatenate([unwave_ref[0, g, 0], unwave_ref[0, g, 1]], axis=1),
                jnp.concatenate([unwave_ref[1, g, 0], unwave_ref[1, g, 1]], axis=1),
            )
            part_ref[g] = part[:, :128]
            part_ref[groups + g] = part[:, 128:]
    with scope("q_invert"):
        for f in range(3):
            at = slice(f * 16, (f + 1) * 16)
            even = [part_ref[g, at] for g in range(groups)] + [part_ref[groups, at]]
            odd = {g: part_ref[groups + g, at] for g in range(1, groups)}
            cosines, sines = tile_waves(even, odd)
            for t in range(tiles):
                if t % half == 0:
                    value = cosines[t]
                elif t < half:
                    value = cosines[t] + sines[t]
                else:
                    value = cosines[tiles - t] - sines[tiles - t]
                if f == 2:
                    value = pltpu.roll(value, 1, 1) - pltpu.roll(value, 127, 1)
                high, low = halves(value)
                field_ref[t, f * 16:(f + 1) * 16, :] = high
                field_ref[t, 48 + f * 16:48 + (f + 1) * 16, :] = low

    cell_near = lax.broadcasted_iota(jnp.int32, (8, 128), 0).astype(f32) - 1.0
    copies[8].wait()

    def interpolate(t, carry):
        coord_x, coord_y = edges(t)
        left, right = hat(coord_x, 0.0), hat(coord_x, 1.0)
        along = hat(coord_y, cell_near)
        here = stacked_dot(
            field_ref[t, 0:48],
            field_ref[t, 48:96],
            jnp.concatenate([weight_ref[t, 0], blank], axis=0),
            jnp.concatenate([weight_ref[t, 1], blank], axis=0),
        )
        live = (slot < counts_ref[t]).astype(f32)
        for f in range(3):
            mixed = here[f * 16:f * 16 + 8] * left + here[f * 16 + 8:f * 16 + 16] * right
            pull = jnp.sum(mixed * along, axis=0, keepdims=True)
            at = (f, pl.ds(t, 1), slice(None))
            out_ref[at] = vel_ref[at] + live * (long_kick * pull + short_ref[t, f:f + 1, :])
        return carry

    with scope("r_interp"):
        lax.fori_loop(0, tiles, interpolate, 0, unroll=16)
    with scope("s_tail"):
        for copy in halos:
            copy.wait_send()
        wait_all(got_ref.at[pl.ds(0, count - 1), pl.ds(0, share)], out_send)
        wait_all(home_ref.at[pl.ds(0, count - 1)], back_send)


def fused_shards(sizes, positions, masses, velocities, tile_counts, neighbour_list):
    size_x, size_y, size_z, tiles, listed = sizes
    rows, cols = size_x * size_z, size_y
    count = rows * cols
    groups = tiles // 2
    near_cells = -(-(NZ // tiles + 3) // 16) * 16
    with jax.ensure_compile_time_eval():
        wave, unwave, into, outof, lanes = tables(size_x, size_y, size_z, tiles)
    anywhere = pl.BlockSpec(memory_space=pl.ANY)
    dma = pltpu.SemaphoreType.DMA
    kicked = pl.pallas_call(
        functools.partial(kick_kernel, sizes),
        out_shape=pltpu.VMEM((3, tiles, 128), f32),
        in_specs=[anywhere] * 10,
        out_specs=pl.BlockSpec(memory_space=pltpu.VMEM),
        scratch_shapes=[
            pltpu.VMEM((3, tiles, 128), f32),
            pltpu.VMEM((tiles, 128), f32),
            pltpu.VMEM((3, tiles, 128), f32),
            pltpu.VMEM(lanes.shape, f32),
            pltpu.SMEM((tiles,), jnp.int32),
            pltpu.SMEM((listed, 1, tiles), jnp.int32),
            pltpu.VMEM(wave.shape, bf16),
            pltpu.VMEM(into.shape, bf16),
            pltpu.VMEM(outof.shape, bf16),
            pltpu.VMEM(unwave.shape, bf16),
            pltpu.VMEM((9 * tiles, 4, 128), f32),
            pltpu.VMEM((tiles, 16, 128), f32),
            pltpu.VMEM((tiles, 2, near_cells, 128), bf16),
            pltpu.VMEM((count, 4, 128), f32),
            pltpu.VMEM((count, 4, 128), f32),
            pltpu.VMEM((rows, cols * CY + 16, 128), f32),
            pltpu.VMEM((count, 8, 128), f32),
            pltpu.VMEM((count, 8, 128), f32),
            pltpu.VMEM((2 * groups, 48, 128), f32),
            pltpu.VMEM((tiles, 96, 128), bf16),
            pltpu.VMEM((tiles, 128, 128), bf16),
            pltpu.VMEM((listed, 48, 128), bf16),
            pltpu.VMEM((listed, 48, 128), bf16),
            pltpu.VMEM((listed, 16, 128), bf16),
            pltpu.VMEM((listed, 16, 128), bf16),
            pltpu.VMEM((2 * listed, 128, 128), bf16),
            pltpu.VMEM((2 * listed, 128, 128), bf16),
            pltpu.VMEM((tiles, 8, 128), f32),
            dma((10,)),
            dma((9,)),
            dma((9,)),
            dma,
            dma,
            dma,
            dma,
        ],
        compiler_params=pltpu.CompilerParams(collective_id=0, has_side_effects=True),
        name="kick",
    )(
        jnp.transpose(positions[0, 0], (1, 0, 2)),
        masses.reshape(tiles, 128),
        jnp.transpose(velocities[0, 0], (1, 0, 2)),
        lanes,
        tile_counts.reshape(tiles),
        jnp.transpose(neighbour_list[0], (2, 0, 1)),
        wave,
        into,
        outof,
        unwave,
    )
    return jnp.transpose(kicked, (1, 0, 2))[None, None]


def fits(sizes):
    size_x, size_y, size_z, tiles, listed = sizes
    count = size_x * size_y * size_z
    if CX != 2 or CY != 6 or count != 32 or tiles != 16 or size_y * CY % 8:
        return False
    return NZ // 2 == 16 * count and NZ // tiles + 3 < 127


def solution(mesh):
    placed = (
        P(("gx", "gz"), "gy", None, None, None),
        P(("gx", "gz"), "gy", None, None),
        P(("gx", "gz"), "gy", None, None, None),
        P(("gx", "gz"), "gy", None),
        P(("gx", "gz"), "gy", None, None),
    )

    def local(positions, masses, velocities, tile_counts, neighbour_list):
        sizes = tuple(mesh.shape[axis] for axis in ("gx", "gy", "gz"))
        sizes = sizes + (positions.shape[2], neighbour_list.shape[3])
        part = functools.partial(fused_shards, sizes) if fits(sizes) else shards
        return part(positions, masses, velocities, tile_counts, neighbour_list)

    return jax.shard_map(
        local,
        mesh=mesh,
        in_specs=placed,
        out_specs=P(("gx", "gz"), "gy", None, None, None),
        check_vma=False,
    )
```

```python
import contextlib
import functools
import math

import jax
import jax.numpy as jnp
import numpy as np
from jax import lax
from jax.experimental import pallas as pl
from jax.experimental.pallas import tpu as pltpu
from jax.sharding import PartitionSpec as P

CX = 2
CY = 6
NZ = 1024


smoothing = 0.1
screening = 0.01
split_scale = 2.0
softening = 0.05
long_kick = 1.0
short_kick = 0.05
highest = lax.Precision.HIGHEST


def padded(cells, sides, width):
    for axis, dim in sides:
        count = lax.axis_size(axis)
        head = lax.slice_in_dim(cells, 0, width, axis=dim)
        tail = lax.slice_in_dim(cells, cells.shape[dim] - width, cells.shape[dim], axis=dim)
        cells = jnp.concatenate(
            [
                lax.ppermute(tail, axis, [(i, (i + 1) % count) for i in range(count)]),
                cells,
                lax.ppermute(head, axis, [((i + 1) % count, i) for i in range(count)]),
            ],
            axis=dim,
        )
    return cells


def wave_terms(length, first_index, extent):
    wavenum = (first_index + jnp.arange(extent, dtype=jnp.int32)).astype(jnp.float32)
    angles = wavenum * (2.0 * jnp.pi / length)
    return (4.0 * jnp.sin(0.5 * angles) ** 2, jnp.sin(angles))


def cloud_stencil(positions, cells_x, cells_y, cells_z, tiles):
    span = cells_z // tiles
    tile_row = jnp.arange(tiles, dtype=jnp.int32)[:, None]
    coord_x = positions[..., 0, :] * cells_x - 0.5
    base_x = jnp.clip(jnp.floor(coord_x), 0, cells_x - 2)
    frac_x = jnp.clip(coord_x - base_x, 0.0, 1.0)
    coord_y = positions[..., 1, :] * cells_y - 0.5
    base_y = jnp.clip(jnp.floor(coord_y), 0, cells_y - 2)
    frac_y = jnp.clip(coord_y - base_y, 0.0, 1.0)
    coord_z = (tile_row + positions[..., 2, :]) * span - 0.5
    base_z = jnp.floor(coord_z)
    frac_z = coord_z - base_z
    index_x = base_x.astype(jnp.int32)
    index_y = base_y.astype(jnp.int32)
    index_z = base_z.astype(jnp.int32) % cells_z
    cell_list = []
    weight_list = []
    for offset_x in (0, 1):
        for offset_y in (0, 1):
            for offset_z in (0, 1):
                weight_x = frac_x if offset_x else 1.0 - frac_x
                weight_y = frac_y if offset_y else 1.0 - frac_y
                weight_z = frac_z if offset_z else 1.0 - frac_z
                cell_list.append(
                    ((index_x + offset_x) * cells_y + index_y + offset_y) * cells_z
                    + (index_z + offset_z) % cells_z
                )
                weight_list.append(weight_x * weight_y * weight_z)
    return (jnp.stack(cell_list, axis=-2), jnp.stack(weight_list, axis=-2))


def pair_accel(receivers, sources, shifts):
    parts = []
    for comp in range(3):
        parts.append(
            shifts[:, :, comp, None, None]
            + sources[:, :, comp, None, :]
            - receivers[:, None, comp, :, None]
        )
    square = parts[0] * parts[0] + parts[1] * parts[1] + parts[2] * parts[2]
    strength = (
        sources[:, :, 3, None, :] * jnp.exp(-square / split_scale) * (square + softening) ** (-1.5)
    )
    return jnp.stack([jnp.sum(strength * parts[comp], axis=(1, 3)) for comp in range(3)], axis=1)


def split_length(length):
    divisor = 1
    for factor in range(1, math.isqrt(length) + 1):
        if length % factor == 0:
            divisor = factor
    return divisor


def dft_table(length):
    indices = jnp.arange(length, dtype=jnp.int32)
    phases = indices[:, None] * indices[None, :] % length
    angles = phases.astype(jnp.float32) * (2.0 * jnp.pi / length)
    return (jnp.cos(angles), jnp.sin(angles))


def twiddle_table(outer, inner):
    length = outer * inner
    phases = (
        jnp.arange(outer, dtype=jnp.int32)[:, None]
        * jnp.arange(inner, dtype=jnp.int32)[None, :]
        % length
    )
    angles = phases.astype(jnp.float32) * (2.0 * jnp.pi / length)
    return (jnp.cos(angles), jnp.sin(angles))


def complex_mix(real, imag, cosine, sine_table, sign, form):
    real_cos = jnp.einsum(form, real, cosine, precision=highest)
    real_sin = jnp.einsum(form, real, sine_table, precision=highest)
    imag_cos = jnp.einsum(form, imag, cosine, precision=highest)
    imag_sin = jnp.einsum(form, imag, sine_table, precision=highest)
    return (real_cos - sign * imag_sin, imag_cos + sign * real_sin)


def transform_last(real, imag, sign):
    length = real.shape[-1]
    outer = split_length(length)
    inner = length // outer
    leading = real.shape[:-1]
    real = real.reshape(leading + (outer, inner))
    imag = imag.reshape(leading + (outer, inner))
    cos_outer, sin_outer = dft_table(outer)
    real, imag = complex_mix(real, imag, cos_outer, sin_outer, sign, "...pq,pk->...kq")
    turn_cos, turn_sin = twiddle_table(outer, inner)
    real, imag = (
        real * turn_cos - sign * imag * turn_sin,
        imag * turn_cos + sign * real * turn_sin,
    )
    cos_inner, sin_inner = dft_table(inner)
    real, imag = complex_mix(real, imag, cos_inner, sin_inner, sign, "...kq,qm->...mk")
    return (real.reshape(leading + (length,)), imag.reshape(leading + (length,)))


def transform_axis(fields, axis, sign):
    real = jnp.moveaxis(fields[:, 0], axis, -1)
    imag = jnp.moveaxis(fields[:, 1], axis, -1)
    real, imag = transform_last(real, imag, sign)
    return jnp.stack([jnp.moveaxis(real, -1, axis), jnp.moveaxis(imag, -1, axis)], axis=1)


def rotate(fields, factor):
    return jnp.stack([factor * fields[:, 1], -factor * fields[:, 0]], axis=1)


def shards(positions, masses, velocities, tile_counts, neighbour_list):
    tiles = positions.shape[2]
    listed = neighbour_list.shape[3]
    slot_index = jnp.arange(128, dtype=jnp.int32)
    live_mask = (slot_index < tile_counts[..., None]).astype(jnp.float32)
    mass_live = masses * live_mask
    packed = jnp.concatenate([positions, mass_live[:, :, :, None, :]], axis=3)
    shell = padded(packed, ((("gx", "gz"), 0), ("gy", 1)), 1)
    cell_index, cloud_weights = cloud_stencil(positions, CX, CY, NZ, tiles)
    amounts = cloud_weights * mass_live[:, :, :, None, :]
    density = jax.ops.segment_sum(
        amounts.reshape(-1), cell_index.reshape(-1), num_segments=CX * CY * NZ
    ).reshape(CX, CY, NZ)
    spectrum = jnp.stack([density, jnp.zeros_like(density)], axis=0)[None]
    spectrum = transform_axis(spectrum, 3, -1.0)
    spectrum = lax.all_to_all(spectrum, "gy", split_axis=4, concat_axis=3, tiled=True)
    span_y = spectrum.shape[3]
    spectrum = transform_axis(spectrum, 2, -1.0)
    spectrum = lax.all_to_all(spectrum, ("gx", "gz"), split_axis=3, concat_axis=2, tiled=True)
    span_x = spectrum.shape[2]
    spectrum = transform_axis(spectrum, 1, -1.0)
    block_y = spectrum.shape[3]
    block_z = spectrum.shape[4]
    kappa_x, sine_x = wave_terms(span_x, 0, span_x)
    kappa_y, sine_y = wave_terms(span_y, lax.axis_index(("gx", "gz")) * block_y, block_y)
    kappa_z, sine_z = wave_terms(NZ, lax.axis_index("gy") * block_z, block_z)
    kappa_sum = kappa_x[:, None, None] + kappa_y[None, :, None] + kappa_z[None, None, :]
    potential = spectrum * (-jnp.exp(-smoothing * kappa_sum) / (kappa_sum + screening))
    fields = jnp.concatenate([rotate(potential, sine_x[:, None, None]), potential], axis=0)
    fields = transform_axis(fields, 1, 1.0) / span_x
    fields = lax.all_to_all(fields, ("gx", "gz"), split_axis=2, concat_axis=3, tiled=True)
    whole_sine_y = wave_terms(span_y, 0, span_y)[1]
    fields = jnp.concatenate(
        [fields[0:1], rotate(fields[1:2], whole_sine_y[None, :, None]), fields[1:2]], axis=0
    )
    fields = transform_axis(fields, 2, 1.0) / span_y
    fields = lax.all_to_all(fields, "gy", split_axis=3, concat_axis=4, tiled=True)
    whole_sine_z = wave_terms(NZ, 0, NZ)[1]
    fields = jnp.concatenate(
        [fields[0:2], rotate(fields[2:3], whole_sine_z[None, None, :])], axis=0
    )
    fields = transform_axis(fields, 3, 1.0) / NZ
    forces = fields[:, 0]
    flat_forces = forces.reshape(3, -1)
    picked = flat_forces[:, cell_index]
    long_accel = jnp.moveaxis(jnp.sum(cloud_weights[None] * picked, axis=4), 0, 3)
    flat_shell = shell.reshape(9 * tiles, 4, 128)
    own_list = neighbour_list[0, 0]
    sources = flat_shell[own_list]
    groups = own_list // tiles
    layers = own_list % tiles
    tile_row = jnp.arange(tiles, dtype=jnp.int32)[:, None]
    shifts = jnp.stack(
        [groups // 3 - 1, groups % 3 - 1, (layers - tile_row + 1) % tiles - 1], axis=-1
    ).astype(jnp.float32)
    short_accel = lax.map(
        lambda pieces: pair_accel(*pieces),
        (
            positions[0, 0].reshape(tiles, 1, 3, 128),
            sources.reshape(tiles, 1, listed, 4, 128),
            shifts.reshape(tiles, 1, listed, 3),
        ),
    )
    short_accel = short_accel.reshape(1, 1, tiles, 3, 128)
    return velocities + live_mask[:, :, :, None, :] * (
        long_kick * long_accel + short_kick * short_accel
    )


MESH = pl.DeviceIdType.MESH
LOGICAL = pl.DeviceIdType.LOGICAL
f32 = jnp.float32
bf16 = jnp.bfloat16


def halves(x):
    high = x.astype(bf16)
    return high, (x - high.astype(f32)).astype(bf16)


def dot3(a, b, dims=((1,), (0,))):
    dot = functools.partial(
        lax.dot_general, dimension_numbers=(dims, ((), ())), preferred_element_type=f32
    )
    return dot(a[0], b[0]) + dot(a[1], b[0]) + dot(a[0], b[1])


def scope(name):
    return contextlib.nullcontext()


def hat(coord, cell):
    return jnp.maximum(0.0, 1.0 - jnp.abs(coord - cell))


def np_halves(table):
    table = jnp.asarray(np.asarray(table, np.float32))
    return jnp.stack(halves(table))


def stacked_dot(high, low, table_high, table_low, dims=((1,), (0,))):
    dot = functools.partial(
        lax.dot_general, dimension_numbers=(dims, ((), ())), preferred_element_type=f32
    )
    rows = high.shape[0]
    both = dot(jnp.concatenate([high, low], axis=0), table_high)
    return both[:rows] + both[rows:] + dot(high, table_low)


def joint_dot(high, low, table_high, table_low):
    rows = high.shape[0]
    left = jnp.concatenate(
        [
            jnp.concatenate([high, high], axis=1),
            jnp.concatenate([low, jnp.zeros_like(low)], axis=1),
        ],
        axis=0,
    )
    both = lax.dot_general(
        left,
        jnp.concatenate([table_high, table_low], axis=0),
        (((1,), (0,)), ((), ())),
        preferred_element_type=f32,
    )
    return both[:rows] + both[rows:]


def tables(size_x, size_y, size_z, tiles):
    rows, cols = size_x * size_z, size_y
    count = rows * cols
    modes = NZ // 2 // count
    pack = 128 // (2 * modes)
    groups = tiles // 2
    lane = np.arange(128)
    member, imag, slot = lane // (2 * modes), lane % (2 * modes) >= modes, lane % modes
    cells = np.arange(128) - 1
    cells[127] = -2
    used = cells <= NZ // tiles + 1
    waves = []
    for g in range(groups):
        plus = member < pack // 2
        residue = np.where(plus, g, tiles - g if g else tiles // 2)
        mode = tiles * (member % (pack // 2) * modes + slot) + residue
        angle = 2 * np.pi * ((cells[:, None] * mode[None]) % NZ) / NZ
        direct = np.where(imag[None], -np.sin(angle), np.cos(angle))
        crossed = np.where(imag[None], np.cos(angle), np.sin(angle))
        crossed = np.where(plus[None], -crossed, crossed)
        if g == 0:
            nyquist = (mode == 0) & imag
            direct = np.where(nyquist[None], np.cos(np.pi * (cells % 2))[:, None], direct)
            direct, crossed = (
                np.where(plus[None], direct, 0.0),
                np.where(plus[None], 0.0, direct),
            )
        both = np.stack([direct, crossed])
        waves.append(np.where(used[None, :, None], both, 0.0).reshape(256, 128))
    nx, ny = rows * CX, cols * CY
    index = np.arange(4 * count * 4)
    device, row = index // 4 % count, index // (4 * count) * (CX * CY // 4) + index % 4
    real = index % 4 < CX * CY // 4
    place_x = device // (size_y * size_z) * size_z + device % size_z
    place_y = device // size_z % size_y
    here_x = np.where(real, place_x * CX + row // CY, 0)
    here_y = np.where(real, place_y * CY + row % CY, 0)
    wave_x, wave_y = np.arange(nx * ny) // ny, np.arange(nx * ny) % ny

    def cas(x, y):
        ax = 2 * np.pi * (x[:, None] * wave_x[None] % nx) / nx
        ay = 2 * np.pi * (y[:, None] * wave_y[None] % ny) / ny
        return (np.cos(ax) + np.sin(ax)) * (np.cos(ay) + np.sin(ay))

    into = cas(here_x, here_y) * real[:, None]
    outof = cas(wave_x, wave_y)
    lanes = np.zeros((8, nx * ny))
    lanes[:] = 4 * np.sin(np.pi * wave_x / nx) ** 2 + 4 * np.sin(np.pi * wave_y / ny) ** 2
    waves = np.stack(waves)
    unwaves = waves.reshape(groups, 2, 128, 128).transpose(0, 1, 3, 2)
    return np_halves(waves), np_halves(unwaves), np_halves(lane_tiles(into)), np_halves(lane_tiles(outof)), jnp.asarray(lanes, f32)


def lane_tiles(table):
    return np.stack(np.split(table, table.shape[1] // 128, axis=1))


def tile_waves(even, odd):
    half = len(even) - 1
    ring, quarter = 2 * half, half // 2

    def total(terms):
        result = None
        for factor, value in terms:
            if abs(factor) < 1e-12:
                continue
            if abs(abs(factor) - 1.0) < 1e-12:
                if result is None:
                    result = value if factor > 0 else -value
                else:
                    result = result + value if factor > 0 else result - value
            else:
                part = value * float(abs(factor))
                if result is None:
                    result = part if factor > 0 else -part
                else:
                    result = result + part if factor > 0 else result - part
        return result

    sums = [even[t] + even[half - t] for t in range(quarter)]
    gaps = [even[t] - even[half - t] for t in range(quarter)]
    odd_sums = {t: odd[t] + odd[half - t] for t in range(1, quarter)}
    odd_gaps = {t: odd[t] - odd[half - t] for t in range(1, quarter)}
    cosines, sines = [], {}
    for r in range(half + 1):
        cos = [math.cos(2 * math.pi * r * t / ring) for t in range(quarter + 1)]
        sin = [math.sin(2 * math.pi * r * t / ring) for t in range(quarter + 1)]
        terms = [(cos[t], (gaps if r % 2 else sums)[t]) for t in range(quarter)]
        if r % 2 == 0:
            terms.append((cos[quarter], even[quarter]))
        cosines.append(total(terms))
        if 0 < r < half:
            terms = [(sin[t], (odd_sums if r % 2 else odd_gaps)[t]) for t in range(1, quarter)]
            if r % 2:
                terms.append((sin[quarter], odd[quarter]))
            sines[r] = total(terms)
    return cosines, sines


def kick_kernel(
    sizes,
    pos_hbm, mass_hbm, vel_hbm, lanes_hbm, counts_hbm, list_hbm, wave_hbm, into_hbm, outof_hbm, unwave_hbm,
    out_ref,
    pos_ref, mass_ref, vel_ref, lanes_ref, counts_ref, list_ref, wave_ref, into_ref, outof_ref, unwave_ref,
    shell_ref, rho_ref, weight_ref, spec_ref, got_ref, window_ref,
    back_ref, home_ref, part_ref, field_ref, spread_ref, theirs_0, theirs_1, pull_0, pull_1, strength_0, strength_1, short_ref,
    input_sem, halo_send, halo_recv, out_send, out_recv, back_send, back_recv,
):
    size_x, size_y, size_z, tiles, listed = sizes
    rows, cols = size_x * size_z, size_y
    count = rows * cols
    modes = NZ // 2 // count
    width = 2 * modes
    pack = 128 // width
    groups = tiles // 2
    span = NZ // tiles
    near_cells = -(-(span + 3) // 16) * 16
    share = CX * CY // 4
    flat = size_y * size_z
    gx, gy, gz = lax.axis_index("gx"), lax.axis_index("gy"), lax.axis_index("gz")
    row, col = gx * size_z + gz, gy
    me = (gx * size_y + gy) * size_z + gz

    copies = [
        pltpu.make_async_copy(a, b, input_sem.at[i])
        for i, (a, b) in enumerate(
            (
                (pos_hbm, pos_ref),
                (mass_hbm, mass_ref),
                (counts_hbm, counts_ref),
                (wave_hbm, wave_ref),
                (list_hbm, list_ref),
                (lanes_hbm, lanes_ref),
                (into_hbm, into_ref),
                (outof_hbm, outof_ref),
                (vel_hbm, vel_ref),
                (unwave_hbm, unwave_ref),
            )
        )
    ]
    for copy in copies[:3]:
        copy.start()

    def place(r, c):
        return (r // size_z, c, r % size_z)

    first = size_x - 1 - gx
    second = lax.rem(gx + size_x // 2, size_x)
    third = size_x - 1 - second
    spot_here = gy * size_z + gz

    turns = [lax.rem(spot_here + i, flat) for i in range(flat)]

    def for_others(act):
        def some(members):
            def step(p, carry):
                if size_x == 4:
                    plane = jnp.where(
                        p == 0, first, jnp.where(p == 1, second, jnp.where(p == 2, third, gx))
                    )
                else:
                    plane = lax.rem(gx + p + 1, size_x)
                for i in members:
                    act(plane * flat + turns[i])
                return carry

            return step

        lax.fori_loop(0, size_x, some(range(1, flat)), 0)
        lax.fori_loop(0, size_x - 1, some(range(1)), 0)

    got_ref[...] = jnp.zeros((count, 4, 128), f32)
    barrier = pltpu.get_barrier_semaphore()

    with scope("a_greet"):
        for_others(
            lambda d: pl.semaphore_signal(barrier, inc=1, device_id=d, device_id_type=LOGICAL)
        )
    for copy in copies[3:]:
        copy.start()

    slot = lax.broadcasted_iota(jnp.int32, (1, 128), 1)
    row_of = lax.broadcasted_iota(jnp.int32, (16, 128), 0)
    cell_of = row_of // 4 * share + row_of % 4
    cell_x = jnp.where(row_of % 4 < share, cell_of // CY, -8).astype(f32)
    cell_y = (cell_of % CY).astype(f32)
    cell_z = lax.broadcasted_iota(jnp.int32, (near_cells, 128), 0).astype(f32) - 1.0
    blank = jnp.zeros((128 - near_cells, 128), bf16)

    own = 4 * tiles

    def edges(t):
        coord_x = jnp.clip(pos_ref[0, pl.ds(t, 1), :] * CX - 0.5, 0.0, CX - 1.0)
        coord_y = jnp.clip(pos_ref[1, pl.ds(t, 1), :] * CY - 0.5, 0.0, CY - 1.0)
        return coord_x, coord_y

    def deposit(t, carry):
        live = (slot < counts_ref[t]).astype(f32)
        mass = mass_ref[pl.ds(t, 1), :] * live
        for comp in range(3):
            shell_ref[own + t, comp:comp + 1, :] = pos_ref[comp, pl.ds(t, 1), :]
        shell_ref[own + t, 3:4, :] = mass
        coord_x, coord_y = edges(t)
        start = jnp.asarray(t, jnp.int32).astype(f32)
        coord_z = (start + pos_ref[2, pl.ds(t, 1), :]) * span - 0.5 - start * span
        plane = hat(coord_x, cell_x) * hat(coord_y, cell_y) * mass
        high, low = halves(plane)
        weight_high, weight_low = halves(hat(coord_z, cell_z))
        weight_ref[t, 0] = weight_high
        weight_ref[t, 1] = weight_low
        rho_ref[t] = stacked_dot(
            high,
            low,
            jnp.concatenate([weight_high, blank], axis=0),
            jnp.concatenate([weight_low, blank], axis=0),
            ((1,), (1,)),
        )
        return carry

    with scope("b_inwait"):
        for copy in copies[:3]:
            copy.wait()
    with scope("c_deposit"):
        lax.fori_loop(0, tiles, deposit, 0, unroll=4)

    quarter = lax.broadcasted_iota(jnp.int32, (8, 128), 1) // width
    lower, even_block = quarter < 2, quarter % 2 == 0

    def exchange(blocks):
        far = [pltpu.roll(b, 64, 1) for b in blocks]
        mixed = [
            jnp.where(lower, blocks[0], far[2]),
            jnp.where(lower, blocks[1], far[3]),
            jnp.where(lower, far[0], blocks[2]),
            jnp.where(lower, far[1], blocks[3]),
        ]
        result = []
        for pair in (0, 2):
            one, two = mixed[pair], mixed[pair + 1]
            result.append(jnp.where(even_block, one, pltpu.roll(two, width, 1)))
            result.append(jnp.where(even_block, pltpu.roll(one, 128 - width, 1), two))
        return result

    with scope("d_tabwait"):
        copies[3].wait()
    with scope("e_transform"):
        rho = [rho_ref[t] for t in range(tiles)]
        half = tiles // 2
        even = [rho[0]] + [rho[t] + rho[tiles - t] for t in range(1, half)] + [rho[half]]
        odd = {t: rho[t] - rho[tiles - t] for t in range(1, half)}
        cosines, sines = tile_waves(even, odd)
        for g in range(groups):
            pair = (cosines[g], sines[g]) if g else (cosines[0], cosines[half])
            high, low = halves(jnp.concatenate(pair, axis=1))
            lines = stacked_dot(high, low, wave_ref[0, g], wave_ref[1, g])
            blocks = [lines[0:8], pltpu.roll(lines[0:8], 4, 0), lines[8:16], pltpu.roll(lines[8:16], 4, 0)]
            for i, block in enumerate(exchange(blocks)):
                spec_ref[g * pack + i] = block[0:4]

    def out_copy(d):
        return pltpu.make_async_remote_copy(
            src_ref=spec_ref.at[d, pl.ds(0, share)],
            dst_ref=got_ref.at[me, pl.ds(0, share)],
            send_sem=out_send,
            recv_sem=out_recv,
            device_id=d,
            device_id_type=LOGICAL,
        )

    def back_copy(d):
        return pltpu.make_async_remote_copy(
            src_ref=back_ref.at[d],
            dst_ref=home_ref.at[me],
            send_sem=back_send,
            recv_sem=back_recv.at[me // (count // 2)],
            device_id=d,
            device_id_type=LOGICAL,
        )

    def start_all(make):
        for_others(lambda d: make(d).start())

    def wait_all(rest, sem):
        pltpu.make_async_copy(rest, rest, sem).wait()

    with scope("f_barwait"):
        pl.semaphore_wait(barrier, count - 1)
    with scope("g_startout"):
        start_all(out_copy)
    halos = []
    for step_x in (-1, 0, 1):
        for step_y in (-1, 0, 1):
            if step_x == 0 and step_y == 0:
                continue
            slot_there = (1 - step_x) * 3 + 1 - step_y
            halos.append(
                pltpu.make_async_remote_copy(
                    src_ref=shell_ref.at[pl.ds(own, tiles)],
                    dst_ref=shell_ref.at[pl.ds(slot_there * tiles, tiles)],
                    send_sem=halo_send.at[slot_there],
                    recv_sem=halo_recv.at[slot_there],
                    device_id=place((row + step_x + rows) % rows, (col + step_y + cols) % cols),
                    device_id_type=MESH,
                )
            )
    with scope("h_starthalo"):
        for copy in halos:
            copy.start()
    got_ref[me] = spec_ref[me]

    theirs, pulls, strengths = (theirs_0, theirs_1), (pull_0, pull_1), (strength_0, strength_1)
    line_of = lax.broadcasted_iota(jnp.int32, (8, 128), 0)
    first_lines, one_line = line_of < 3, line_of == 3
    square_lines = (line_of > 3) & (line_of < 7)

    def thirds(x):
        high = x.astype(bf16).astype(f32)
        rest = x - high
        middle = rest.astype(bf16).astype(f32)
        return high, middle, rest - middle

    def spread(t, carry):
        tile = shell_ref[own + t]
        spot = jnp.where(first_lines, jnp.concatenate([tile, tile], axis=0) - 0.5, 0.0)
        norm = jnp.sum(spot * spot, axis=0, keepdims=True) + softening
        mine = jnp.where(one_line, norm, jnp.where(square_lines, 1.0, -2.0 * spot))
        high, middle, low = thirds(mine)
        terms = [high, high, middle, high, low, middle, jnp.zeros((80, 128), f32)]
        spread_ref[t] = jnp.transpose(jnp.concatenate(terms, axis=0), (1, 0)).astype(bf16)
        return carry

    with scope("i_spread"):
        lax.fori_loop(0, tiles, spread, 0, unroll=2)

    def describe(t, theirs_ref, pull_ref):
        for n in range(listed):
            entry = list_ref[n, 0, t]
            group = lax.div(entry, tiles)
            layer = entry - group * tiles
            step_x = lax.div(group * 11, 32)
            step_y = group - 3 * step_x
            away = lax.rem(layer - t + 1 + tiles, tiles)
            tile = shell_ref[entry]
            shift = jnp.where(
                line_of % 4 == 0,
                step_x.astype(f32),
                jnp.where(line_of % 4 == 1, step_y.astype(f32), away.astype(f32)),
            )
            spot = jnp.concatenate([tile, tile], axis=0) + (shift - 1.5)
            theirs = jnp.where(
                first_lines, spot, jnp.where(one_line, 1.0, jnp.where(square_lines, spot * spot, 0.0))
            )
            high, middle, low = thirds(theirs)
            one = jnp.concatenate([high, middle], axis=0).astype(bf16)
            two = jnp.concatenate([high, low], axis=0).astype(bf16)
            theirs_ref[n] = jnp.concatenate([one, two, one], axis=0)
            pull = jnp.concatenate(halves(theirs * tile[3:4]), axis=0)
            pull_ref[n] = pull

    product = functools.partial(lax.dot_general, preferred_element_type=f32)

    def attract(t, theirs_ref, strength_ref):
        for n in range(0, listed, 2):
            square = product(
                spread_ref[t][:, :48],
                jnp.concatenate([theirs_ref[n], theirs_ref[n + 1]], axis=1),
                (((1,), (0,)), ((), ())),
            )
            root = lax.rsqrt(square)
            strength = jnp.exp2(square * (-1.0 / (split_scale * math.log(2.0)))) * (root * root * root)
            high, low = halves(strength)
            for k in range(2):
                at = slice(k * 128, (k + 1) * 128)
                strength_ref[2 * (n + k)] = high[:, at]
                strength_ref[2 * (n + k) + 1] = low[:, at]

    def collect(t, pull_ref, strength_ref):
        total = product(
            jnp.concatenate([strength_ref[i] for i in range(2 * listed)], axis=1),
            jnp.concatenate([pull_ref[i // 2] for i in range(2 * listed)], axis=1),
             (((1,), (1,)), ((), ())))
        total = jnp.transpose(total, (1, 0))
        total = total[0:8] + total[8:16]
        tile = shell_ref[own + t]
        spot = jnp.concatenate([tile, tile], axis=0) - 0.5
        short_ref[t] = (total - spot * total[3:4]) * (short_kick * math.exp(softening / split_scale))

    nx, ny = rows * CX, cols * CY
    copies[4].wait()
    copies[5].wait()
    with scope("i2_green"):
        row_in = lax.broadcasted_iota(jnp.int32, (width, nx * ny), 0)
        family, member = me // pack, me % pack
        residue = jnp.where(
            member < pack // 2, family, jnp.where(family == 0, tiles // 2, tiles - family)
        )
        mode_of = tiles * (member % (pack // 2) * modes + row_in % modes) + residue
        alone = mode_of == 0
        wave_z = jnp.where(alone & (row_in >= modes), NZ // 2, mode_of).astype(f32)
        kappa = lanes_ref[0:1, :] + 4.0 * jnp.sin(wave_z * (jnp.pi / NZ)) ** 2
        scale = jnp.where(alone, 0.5, 1.0) * (1.0 / (NZ * nx * ny))
        green = -jnp.exp(-smoothing * kappa) / (kappa + screening) * scale

    with scope("j_waitgot"):
        wait_all(got_ref.at[pl.ds(0, count - 1), pl.ds(0, share)], out_recv)
    with scope("k_plane"):
        copies[6].wait()
        copies[7].wait()
        turned = jnp.transpose(got_ref[...].reshape(count * 4, 128), (1, 0))
        mine = jnp.concatenate(
            [turned[a * width:(a + 1) * width] for a in range(pack)], axis=1
        )
        high, low = halves(mine)
        joined = lambda ref, part: jnp.concatenate([ref[part, i] for i in range(nx * ny // 128)], axis=1)
        waves = stacked_dot(high, low, joined(into_ref, 0), joined(into_ref, 1))
        high, low = halves(waves * green)
        plane = stacked_dot(high, low, joined(outof_ref, 0), joined(outof_ref, 1))
        sheet = jnp.transpose(jnp.concatenate([plane] * pack, axis=0), (1, 0))
        for r in range(rows):
            for v in range(ny // 8):
                pick = [
                    sheet[at:at + 8]
                    for at in (((r * CX - 1 + b) % nx) * ny + v * 8 for b in range(pack))
                ]
                window = jnp.where(
                    lower,
                    jnp.where(even_block, pick[0], pick[1]),
                    jnp.where(even_block, pick[2], pick[3]),
                )
                window_ref[r, (v + 1) * 8:(v + 2) * 8, :] = window
                if v == 0:
                    window_ref[r, 8 + ny:16 + ny, :] = window
                if v == ny // 8 - 1:
                    window_ref[r, 0:8, :] = window
        for r in range(rows):
            for c in range(cols):
                d = (r // size_z * size_y + c) * size_z + r % size_z
                back_ref[d] = window_ref[r, c * CY + 7:c * CY + 15, :]
    with scope("l_startback"):
        start_all(back_copy)
    kept = pltpu.make_async_copy(
        back_ref.at[me], home_ref.at[me], back_recv.at[me // (count // 2)]
    )
    kept.start()

    with scope("m_waithalo"):
        for copy in halos:
            copy.wait_recv()
    def pairs(k, carry):
        for odd in (0, 1):
            t = 2 * k + odd
            attract(t, theirs[odd], strengths[odd])
            collect(lax.rem(t + tiles - 1, tiles), pulls[1 - odd], strengths[1 - odd])
            describe(lax.rem(t + 1, tiles), theirs[1 - odd], pulls[1 - odd])
        return carry

    with scope("n_pairs"):
        describe(0, theirs[0], pulls[0])
        lax.fori_loop(0, tiles // 2, pairs, 0, unroll=4)
        collect(tiles - 1, pulls[1], strengths[1])
    copies[9].wait()

    def untwist(h, carry):
        near = (me // (count // 2) + h) % 2
        with scope("o_waithome"):
            wait_all(home_ref.at[pl.ds(0, count // 2)], back_recv.at[near])
        for i in range(groups // 2):
            g = near * (groups // 2) + i
            lines = exchange([home_ref[g * pack + k] for k in range(pack)])
            pulls = [lines[b - 1] - lines[b + 1] for b in (1, 2)]
            pulls += [pltpu.roll(lines[b], 1, 0) - pltpu.roll(lines[b], 7, 0) for b in (1, 2)]
            high, low = halves(jnp.concatenate(pulls + [lines[1], lines[2]], axis=0))
            part = joint_dot(
                high,
                low,
                jnp.concatenate([unwave_ref[0, g, 0], unwave_ref[0, g, 1]], axis=1),
                jnp.concatenate([unwave_ref[1, g, 0], unwave_ref[1, g, 1]], axis=1),
            )
            part_ref[g] = part[:, :128]
            part_ref[groups + g] = part[:, 128:]
        return carry

    with scope("p_lines"):
        lax.fori_loop(0, 2, untwist, 0)
    with scope("q_invert"):
        for f in range(3):
            at = slice(f * 16, (f + 1) * 16)
            even = [part_ref[g, at] for g in range(groups)] + [part_ref[groups, at]]
            odd = {g: part_ref[groups + g, at] for g in range(1, groups)}
            cosines, sines = tile_waves(even, odd)
            for t in range(tiles):
                if t % half == 0:
                    value = cosines[t]
                elif t < half:
                    value = cosines[t] + sines[t]
                else:
                    value = cosines[tiles - t] - sines[tiles - t]
                if f == 2:
                    value = pltpu.roll(value, 1, 1) - pltpu.roll(value, 127, 1)
                high, low = halves(value)
                field_ref[t, f * 16:(f + 1) * 16, :] = high
                field_ref[t, 48 + f * 16:48 + (f + 1) * 16, :] = low

    cell_near = lax.broadcasted_iota(jnp.int32, (8, 128), 0).astype(f32) - 1.0
    copies[8].wait()

    def interpolate(t, carry):
        coord_x, coord_y = edges(t)
        left, right = hat(coord_x, 0.0), hat(coord_x, 1.0)
        along = hat(coord_y, cell_near)
        here = stacked_dot(
            field_ref[t, 0:48],
            field_ref[t, 48:96],
            jnp.concatenate([weight_ref[t, 0], blank], axis=0),
            jnp.concatenate([weight_ref[t, 1], blank], axis=0),
        )
        live = (slot < counts_ref[t]).astype(f32)
        for f in range(3):
            mixed = here[f * 16:f * 16 + 8] * left + here[f * 16 + 8:f * 16 + 16] * right
            pull = jnp.sum(mixed * along, axis=0, keepdims=True)
            at = (f, pl.ds(t, 1), slice(None))
            out_ref[at] = vel_ref[at] + live * (long_kick * pull + short_ref[t, f:f + 1, :])
        return carry

    with scope("r_interp"):
        lax.fori_loop(0, tiles, interpolate, 0, unroll=16)
    with scope("s_tail"):
        for copy in halos:
            copy.wait_send()
        wait_all(got_ref.at[pl.ds(0, count - 1), pl.ds(0, share)], out_send)
        wait_all(home_ref.at[pl.ds(0, count - 1)], back_send)


def fused_shards(sizes, positions, masses, velocities, tile_counts, neighbour_list):
    size_x, size_y, size_z, tiles, listed = sizes
    rows, cols = size_x * size_z, size_y
    count = rows * cols
    groups = tiles // 2
    near_cells = -(-(NZ // tiles + 3) // 16) * 16
    with jax.ensure_compile_time_eval():
        wave, unwave, into, outof, lanes = tables(size_x, size_y, size_z, tiles)
    anywhere = pl.BlockSpec(memory_space=pl.ANY)
    dma = pltpu.SemaphoreType.DMA
    kicked = pl.pallas_call(
        functools.partial(kick_kernel, sizes),
        out_shape=pltpu.VMEM((3, tiles, 128), f32),
        in_specs=[anywhere] * 10,
        out_specs=pl.BlockSpec(memory_space=pltpu.VMEM),
        scratch_shapes=[
            pltpu.VMEM((3, tiles, 128), f32),
            pltpu.VMEM((tiles, 128), f32),
            pltpu.VMEM((3, tiles, 128), f32),
            pltpu.VMEM(lanes.shape, f32),
            pltpu.SMEM((tiles,), jnp.int32),
            pltpu.SMEM((listed, 1, tiles), jnp.int32),
            pltpu.VMEM(wave.shape, bf16),
            pltpu.VMEM(into.shape, bf16),
            pltpu.VMEM(outof.shape, bf16),
            pltpu.VMEM(unwave.shape, bf16),
            pltpu.VMEM((9 * tiles, 4, 128), f32),
            pltpu.VMEM((tiles, 16, 128), f32),
            pltpu.VMEM((tiles, 2, near_cells, 128), bf16),
            pltpu.VMEM((count, 4, 128), f32),
            pltpu.VMEM((count, 4, 128), f32),
            pltpu.VMEM((rows, cols * CY + 16, 128), f32),
            pltpu.VMEM((count, 8, 128), f32),
            pltpu.VMEM((count, 8, 128), f32),
            pltpu.VMEM((2 * groups, 48, 128), f32),
            pltpu.VMEM((tiles, 96, 128), bf16),
            pltpu.VMEM((tiles, 128, 128), bf16),
            pltpu.VMEM((listed, 48, 128), bf16),
            pltpu.VMEM((listed, 48, 128), bf16),
            pltpu.VMEM((listed, 16, 128), bf16),
            pltpu.VMEM((listed, 16, 128), bf16),
            pltpu.VMEM((2 * listed, 128, 128), bf16),
            pltpu.VMEM((2 * listed, 128, 128), bf16),
            pltpu.VMEM((tiles, 8, 128), f32),
            dma((10,)),
            dma((9,)),
            dma((9,)),
            dma,
            dma,
            dma,
            dma((2,)),
        ],
        compiler_params=pltpu.CompilerParams(collective_id=0, has_side_effects=True),
        name="kick",
    )(
        jnp.transpose(positions[0, 0], (1, 0, 2)),
        masses.reshape(tiles, 128),
        jnp.transpose(velocities[0, 0], (1, 0, 2)),
        lanes,
        tile_counts.reshape(tiles),
        jnp.transpose(neighbour_list[0], (2, 0, 1)),
        wave,
        into,
        outof,
        unwave,
    )
    return jnp.transpose(kicked, (1, 0, 2))[None, None]


def fits(sizes):
    size_x, size_y, size_z, tiles, listed = sizes
    count = size_x * size_y * size_z
    if CX != 2 or CY != 6 or count != 32 or tiles != 16 or size_y * CY % 8:
        return False
    return NZ // 2 == 16 * count and NZ // tiles + 3 < 127


def solution(mesh):
    placed = (
        P(("gx", "gz"), "gy", None, None, None),
        P(("gx", "gz"), "gy", None, None),
        P(("gx", "gz"), "gy", None, None, None),
        P(("gx", "gz"), "gy", None),
        P(("gx", "gz"), "gy", None, None),
    )

    def local(positions, masses, velocities, tile_counts, neighbour_list):
        sizes = tuple(mesh.shape[axis] for axis in ("gx", "gy", "gz"))
        sizes = sizes + (positions.shape[2], neighbour_list.shape[3])
        part = functools.partial(fused_shards, sizes) if fits(sizes) else shards
        return part(positions, masses, velocities, tile_counts, neighbour_list)

    return jax.shard_map(
        local,
        mesh=mesh,
        in_specs=placed,
        out_specs=P(("gx", "gz"), "gy", None, None, None),
        check_vma=False,
    )
```

```python
import contextlib
import functools
import math

import jax
import jax.numpy as jnp
import numpy as np
from jax import lax
from jax.experimental import pallas as pl
from jax.experimental.pallas import tpu as pltpu
from jax.sharding import PartitionSpec as P

CX = 2
CY = 6
NZ = 1024


smoothing = 0.1
screening = 0.01
split_scale = 2.0
softening = 0.05
long_kick = 1.0
short_kick = 0.05
highest = lax.Precision.HIGHEST


def padded(cells, sides, width):
    for axis, dim in sides:
        count = lax.axis_size(axis)
        head = lax.slice_in_dim(cells, 0, width, axis=dim)
        tail = lax.slice_in_dim(cells, cells.shape[dim] - width, cells.shape[dim], axis=dim)
        cells = jnp.concatenate(
            [
                lax.ppermute(tail, axis, [(i, (i + 1) % count) for i in range(count)]),
                cells,
                lax.ppermute(head, axis, [((i + 1) % count, i) for i in range(count)]),
            ],
            axis=dim,
        )
    return cells


def wave_terms(length, first_index, extent):
    wavenum = (first_index + jnp.arange(extent, dtype=jnp.int32)).astype(jnp.float32)
    angles = wavenum * (2.0 * jnp.pi / length)
    return (4.0 * jnp.sin(0.5 * angles) ** 2, jnp.sin(angles))


def cloud_stencil(positions, cells_x, cells_y, cells_z, tiles):
    span = cells_z // tiles
    tile_row = jnp.arange(tiles, dtype=jnp.int32)[:, None]
    coord_x = positions[..., 0, :] * cells_x - 0.5
    base_x = jnp.clip(jnp.floor(coord_x), 0, cells_x - 2)
    frac_x = jnp.clip(coord_x - base_x, 0.0, 1.0)
    coord_y = positions[..., 1, :] * cells_y - 0.5
    base_y = jnp.clip(jnp.floor(coord_y), 0, cells_y - 2)
    frac_y = jnp.clip(coord_y - base_y, 0.0, 1.0)
    coord_z = (tile_row + positions[..., 2, :]) * span - 0.5
    base_z = jnp.floor(coord_z)
    frac_z = coord_z - base_z
    index_x = base_x.astype(jnp.int32)
    index_y = base_y.astype(jnp.int32)
    index_z = base_z.astype(jnp.int32) % cells_z
    cell_list = []
    weight_list = []
    for offset_x in (0, 1):
        for offset_y in (0, 1):
            for offset_z in (0, 1):
                weight_x = frac_x if offset_x else 1.0 - frac_x
                weight_y = frac_y if offset_y else 1.0 - frac_y
                weight_z = frac_z if offset_z else 1.0 - frac_z
                cell_list.append(
                    ((index_x + offset_x) * cells_y + index_y + offset_y) * cells_z
                    + (index_z + offset_z) % cells_z
                )
                weight_list.append(weight_x * weight_y * weight_z)
    return (jnp.stack(cell_list, axis=-2), jnp.stack(weight_list, axis=-2))


def pair_accel(receivers, sources, shifts):
    parts = []
    for comp in range(3):
        parts.append(
            shifts[:, :, comp, None, None]
            + sources[:, :, comp, None, :]
            - receivers[:, None, comp, :, None]
        )
    square = parts[0] * parts[0] + parts[1] * parts[1] + parts[2] * parts[2]
    strength = (
        sources[:, :, 3, None, :] * jnp.exp(-square / split_scale) * (square + softening) ** (-1.5)
    )
    return jnp.stack([jnp.sum(strength * parts[comp], axis=(1, 3)) for comp in range(3)], axis=1)


def split_length(length):
    divisor = 1
    for factor in range(1, math.isqrt(length) + 1):
        if length % factor == 0:
            divisor = factor
    return divisor


def dft_table(length):
    indices = jnp.arange(length, dtype=jnp.int32)
    phases = indices[:, None] * indices[None, :] % length
    angles = phases.astype(jnp.float32) * (2.0 * jnp.pi / length)
    return (jnp.cos(angles), jnp.sin(angles))


def twiddle_table(outer, inner):
    length = outer * inner
    phases = (
        jnp.arange(outer, dtype=jnp.int32)[:, None]
        * jnp.arange(inner, dtype=jnp.int32)[None, :]
        % length
    )
    angles = phases.astype(jnp.float32) * (2.0 * jnp.pi / length)
    return (jnp.cos(angles), jnp.sin(angles))


def complex_mix(real, imag, cosine, sine_table, sign, form):
    real_cos = jnp.einsum(form, real, cosine, precision=highest)
    real_sin = jnp.einsum(form, real, sine_table, precision=highest)
    imag_cos = jnp.einsum(form, imag, cosine, precision=highest)
    imag_sin = jnp.einsum(form, imag, sine_table, precision=highest)
    return (real_cos - sign * imag_sin, imag_cos + sign * real_sin)


def transform_last(real, imag, sign):
    length = real.shape[-1]
    outer = split_length(length)
    inner = length // outer
    leading = real.shape[:-1]
    real = real.reshape(leading + (outer, inner))
    imag = imag.reshape(leading + (outer, inner))
    cos_outer, sin_outer = dft_table(outer)
    real, imag = complex_mix(real, imag, cos_outer, sin_outer, sign, "...pq,pk->...kq")
    turn_cos, turn_sin = twiddle_table(outer, inner)
    real, imag = (
        real * turn_cos - sign * imag * turn_sin,
        imag * turn_cos + sign * real * turn_sin,
    )
    cos_inner, sin_inner = dft_table(inner)
    real, imag = complex_mix(real, imag, cos_inner, sin_inner, sign, "...kq,qm->...mk")
    return (real.reshape(leading + (length,)), imag.reshape(leading + (length,)))


def transform_axis(fields, axis, sign):
    real = jnp.moveaxis(fields[:, 0], axis, -1)
    imag = jnp.moveaxis(fields[:, 1], axis, -1)
    real, imag = transform_last(real, imag, sign)
    return jnp.stack([jnp.moveaxis(real, -1, axis), jnp.moveaxis(imag, -1, axis)], axis=1)


def rotate(fields, factor):
    return jnp.stack([factor * fields[:, 1], -factor * fields[:, 0]], axis=1)


def shards(positions, masses, velocities, tile_counts, neighbour_list):
    tiles = positions.shape[2]
    listed = neighbour_list.shape[3]
    slot_index = jnp.arange(128, dtype=jnp.int32)
    live_mask = (slot_index < tile_counts[..., None]).astype(jnp.float32)
    mass_live = masses * live_mask
    packed = jnp.concatenate([positions, mass_live[:, :, :, None, :]], axis=3)
    shell = padded(packed, ((("gx", "gz"), 0), ("gy", 1)), 1)
    cell_index, cloud_weights = cloud_stencil(positions, CX, CY, NZ, tiles)
    amounts = cloud_weights * mass_live[:, :, :, None, :]
    density = jax.ops.segment_sum(
        amounts.reshape(-1), cell_index.reshape(-1), num_segments=CX * CY * NZ
    ).reshape(CX, CY, NZ)
    spectrum = jnp.stack([density, jnp.zeros_like(density)], axis=0)[None]
    spectrum = transform_axis(spectrum, 3, -1.0)
    spectrum = lax.all_to_all(spectrum, "gy", split_axis=4, concat_axis=3, tiled=True)
    span_y = spectrum.shape[3]
    spectrum = transform_axis(spectrum, 2, -1.0)
    spectrum = lax.all_to_all(spectrum, ("gx", "gz"), split_axis=3, concat_axis=2, tiled=True)
    span_x = spectrum.shape[2]
    spectrum = transform_axis(spectrum, 1, -1.0)
    block_y = spectrum.shape[3]
    block_z = spectrum.shape[4]
    kappa_x, sine_x = wave_terms(span_x, 0, span_x)
    kappa_y, sine_y = wave_terms(span_y, lax.axis_index(("gx", "gz")) * block_y, block_y)
    kappa_z, sine_z = wave_terms(NZ, lax.axis_index("gy") * block_z, block_z)
    kappa_sum = kappa_x[:, None, None] + kappa_y[None, :, None] + kappa_z[None, None, :]
    potential = spectrum * (-jnp.exp(-smoothing * kappa_sum) / (kappa_sum + screening))
    fields = jnp.concatenate([rotate(potential, sine_x[:, None, None]), potential], axis=0)
    fields = transform_axis(fields, 1, 1.0) / span_x
    fields = lax.all_to_all(fields, ("gx", "gz"), split_axis=2, concat_axis=3, tiled=True)
    whole_sine_y = wave_terms(span_y, 0, span_y)[1]
    fields = jnp.concatenate(
        [fields[0:1], rotate(fields[1:2], whole_sine_y[None, :, None]), fields[1:2]], axis=0
    )
    fields = transform_axis(fields, 2, 1.0) / span_y
    fields = lax.all_to_all(fields, "gy", split_axis=3, concat_axis=4, tiled=True)
    whole_sine_z = wave_terms(NZ, 0, NZ)[1]
    fields = jnp.concatenate(
        [fields[0:2], rotate(fields[2:3], whole_sine_z[None, None, :])], axis=0
    )
    fields = transform_axis(fields, 3, 1.0) / NZ
    forces = fields[:, 0]
    flat_forces = forces.reshape(3, -1)
    picked = flat_forces[:, cell_index]
    long_accel = jnp.moveaxis(jnp.sum(cloud_weights[None] * picked, axis=4), 0, 3)
    flat_shell = shell.reshape(9 * tiles, 4, 128)
    own_list = neighbour_list[0, 0]
    sources = flat_shell[own_list]
    groups = own_list // tiles
    layers = own_list % tiles
    tile_row = jnp.arange(tiles, dtype=jnp.int32)[:, None]
    shifts = jnp.stack(
        [groups // 3 - 1, groups % 3 - 1, (layers - tile_row + 1) % tiles - 1], axis=-1
    ).astype(jnp.float32)
    short_accel = lax.map(
        lambda pieces: pair_accel(*pieces),
        (
            positions[0, 0].reshape(tiles, 1, 3, 128),
            sources.reshape(tiles, 1, listed, 4, 128),
            shifts.reshape(tiles, 1, listed, 3),
        ),
    )
    short_accel = short_accel.reshape(1, 1, tiles, 3, 128)
    return velocities + live_mask[:, :, :, None, :] * (
        long_kick * long_accel + short_kick * short_accel
    )


MESH = pl.DeviceIdType.MESH
LOGICAL = pl.DeviceIdType.LOGICAL
f32 = jnp.float32
bf16 = jnp.bfloat16


def halves(x):
    high = x.astype(bf16)
    return high, (x - high.astype(f32)).astype(bf16)


def dot3(a, b, dims=((1,), (0,))):
    dot = functools.partial(
        lax.dot_general, dimension_numbers=(dims, ((), ())), preferred_element_type=f32
    )
    return dot(a[0], b[0]) + dot(a[1], b[0]) + dot(a[0], b[1])


def scope(name):
    return contextlib.nullcontext()


def hat(coord, cell):
    return jnp.maximum(0.0, 1.0 - jnp.abs(coord - cell))


def np_halves(table):
    table = jnp.asarray(np.asarray(table, np.float32))
    return jnp.stack(halves(table))


def stacked_dot(high, low, table_high, table_low, dims=((1,), (0,))):
    dot = functools.partial(
        lax.dot_general, dimension_numbers=(dims, ((), ())), preferred_element_type=f32
    )
    rows = high.shape[0]
    both = dot(jnp.concatenate([high, low], axis=0), table_high)
    return both[:rows] + both[rows:] + dot(high, table_low)


def joint_dot(high, low, table_high, table_low):
    rows = high.shape[0]
    left = jnp.concatenate(
        [
            jnp.concatenate([high, high], axis=1),
            jnp.concatenate([low, jnp.zeros_like(low)], axis=1),
        ],
        axis=0,
    )
    both = lax.dot_general(
        left,
        jnp.concatenate([table_high, table_low], axis=0),
        (((1,), (0,)), ((), ())),
        preferred_element_type=f32,
    )
    return both[:rows] + both[rows:]


def tables(size_x, size_y, size_z, tiles):
    rows, cols = size_x * size_z, size_y
    count = rows * cols
    modes = NZ // 2 // count
    pack = 128 // (2 * modes)
    groups = tiles // 2
    lane = np.arange(128)
    member, imag, slot = lane // (2 * modes), lane % (2 * modes) >= modes, lane % modes
    cells = np.arange(128) - 1
    cells[127] = -2
    used = cells <= NZ // tiles + 1
    waves = []
    for g in range(groups):
        plus = member < pack // 2
        residue = np.where(plus, g, tiles - g if g else tiles // 2)
        mode = tiles * (member % (pack // 2) * modes + slot) + residue
        angle = 2 * np.pi * ((cells[:, None] * mode[None]) % NZ) / NZ
        direct = np.where(imag[None], -np.sin(angle), np.cos(angle))
        crossed = np.where(imag[None], np.cos(angle), np.sin(angle))
        crossed = np.where(plus[None], -crossed, crossed)
        if g == 0:
            nyquist = (mode == 0) & imag
            direct = np.where(nyquist[None], np.cos(np.pi * (cells % 2))[:, None], direct)
            direct, crossed = (
                np.where(plus[None], direct, 0.0),
                np.where(plus[None], 0.0, direct),
            )
        both = np.stack([direct, crossed])
        waves.append(np.where(used[None, :, None], both, 0.0).reshape(256, 128))
    nx, ny = rows * CX, cols * CY
    index = np.arange(4 * count * 4)
    device, row = index // 4 % count, index // (4 * count) * (CX * CY // 4) + index % 4
    real = index % 4 < CX * CY // 4
    place_x = device // (size_y * size_z) * size_z + device % size_z
    place_y = device // size_z % size_y
    here_x = np.where(real, place_x * CX + row // CY, 0)
    here_y = np.where(real, place_y * CY + row % CY, 0)
    wave_x, wave_y = np.arange(nx * ny) // ny, np.arange(nx * ny) % ny

    def cas(x, y):
        ax = 2 * np.pi * (x[:, None] * wave_x[None] % nx) / nx
        ay = 2 * np.pi * (y[:, None] * wave_y[None] % ny) / ny
        return (np.cos(ax) + np.sin(ax)) * (np.cos(ay) + np.sin(ay))

    into = cas(here_x, here_y) * real[:, None]
    outof = cas(wave_x, wave_y)
    lanes = np.zeros((8, nx * ny))
    lanes[:] = 4 * np.sin(np.pi * wave_x / nx) ** 2 + 4 * np.sin(np.pi * wave_y / ny) ** 2
    waves = np.stack(waves)
    unwaves = waves.reshape(groups, 2, 128, 128).transpose(0, 1, 3, 2)
    near_cells = -(-(NZ // tiles + 3) // 16) * 16
    waves = waves.reshape(groups, 2, 128, 128)[:, :, :near_cells]
    return np_halves(waves), np_halves(unwaves), np_halves(lane_tiles(into)), np_halves(lane_tiles(outof)), jnp.asarray(lanes, f32)


def lane_tiles(table):
    return np.stack(np.split(table, table.shape[1] // 128, axis=1))


def tile_waves(even, odd):
    half = len(even) - 1
    ring, quarter = 2 * half, half // 2

    def total(terms):
        result = None
        for factor, value in terms:
            if abs(factor) < 1e-12:
                continue
            if abs(abs(factor) - 1.0) < 1e-12:
                if result is None:
                    result = value if factor > 0 else -value
                else:
                    result = result + value if factor > 0 else result - value
            else:
                part = value * float(abs(factor))
                if result is None:
                    result = part if factor > 0 else -part
                else:
                    result = result + part if factor > 0 else result - part
        return result

    sums = [even[t] + even[half - t] for t in range(quarter)]
    gaps = [even[t] - even[half - t] for t in range(quarter)]
    odd_sums = {t: odd[t] + odd[half - t] for t in range(1, quarter)}
    odd_gaps = {t: odd[t] - odd[half - t] for t in range(1, quarter)}
    cosines, sines = [], {}
    for r in range(half + 1):
        cos = [math.cos(2 * math.pi * r * t / ring) for t in range(quarter + 1)]
        sin = [math.sin(2 * math.pi * r * t / ring) for t in range(quarter + 1)]
        terms = [(cos[t], (gaps if r % 2 else sums)[t]) for t in range(quarter)]
        if r % 2 == 0:
            terms.append((cos[quarter], even[quarter]))
        cosines.append(total(terms))
        if 0 < r < half:
            terms = [(sin[t], (odd_sums if r % 2 else odd_gaps)[t]) for t in range(1, quarter)]
            if r % 2:
                terms.append((sin[quarter], odd[quarter]))
            sines[r] = total(terms)
    return cosines, sines


def kick_kernel(
    sizes,
    pos_hbm, mass_hbm, vel_hbm, lanes_hbm, counts_hbm, list_hbm, wave_hbm, into_hbm, outof_hbm, unwave_hbm,
    out_ref,
    pos_ref, mass_ref, vel_ref, lanes_ref, counts_ref, list_ref, wave_ref, into_ref, outof_ref, unwave_ref,
    shell_ref, rho_ref, weight_ref, spec_ref, got_ref, window_ref,
    back_ref, home_ref, part_ref, field_ref, spread_ref, theirs_0, theirs_1, pull_0, pull_1, strength_0, strength_1, short_ref,
    input_sem, halo_send, halo_recv, out_send, out_recv, back_send, back_recv,
):
    size_x, size_y, size_z, tiles, listed = sizes
    rows, cols = size_x * size_z, size_y
    count = rows * cols
    modes = NZ // 2 // count
    width = 2 * modes
    pack = 128 // width
    groups = tiles // 2
    span = NZ // tiles
    near_cells = -(-(span + 3) // 16) * 16
    share = CX * CY // 4
    flat = size_y * size_z
    gx, gy, gz = lax.axis_index("gx"), lax.axis_index("gy"), lax.axis_index("gz")
    row, col = gx * size_z + gz, gy
    me = (gx * size_y + gy) * size_z + gz

    copies = [
        pltpu.make_async_copy(a, b, input_sem.at[i])
        for i, (a, b) in enumerate(
            (
                (pos_hbm, pos_ref),
                (mass_hbm, mass_ref),
                (counts_hbm, counts_ref),
                (wave_hbm, wave_ref),
                (list_hbm, list_ref),
                (lanes_hbm, lanes_ref),
                (into_hbm, into_ref),
                (outof_hbm, outof_ref),
                (vel_hbm, vel_ref),
                (unwave_hbm, unwave_ref),
            )
        )
    ]
    for copy in copies[:3]:
        copy.start()

    def place(r, c):
        return (r // size_z, c, r % size_z)

    first = size_x - 1 - gx
    second = lax.rem(gx + size_x // 2, size_x)
    third = size_x - 1 - second
    spot_here = gy * size_z + gz

    turns = [lax.rem(spot_here + i, flat) for i in range(flat)]

    def for_others(act):
        def some(members):
            def step(p, carry):
                if size_x == 4:
                    plane = jnp.where(
                        p == 0, first, jnp.where(p == 1, second, jnp.where(p == 2, third, gx))
                    )
                else:
                    plane = lax.rem(gx + p + 1, size_x)
                for i in members:
                    act(plane * flat + turns[i])
                return carry

            return step

        lax.fori_loop(0, size_x, some(range(1, flat)), 0)
        lax.fori_loop(0, size_x - 1, some(range(1)), 0)

    got_ref[...] = jnp.zeros((count, 4, 128), f32)
    barrier = pltpu.get_barrier_semaphore()

    with scope("a_greet"):
        for_others(
            lambda d: pl.semaphore_signal(barrier, inc=1, device_id=d, device_id_type=LOGICAL)
        )
    for copy in copies[3:]:
        copy.start()

    slot = lax.broadcasted_iota(jnp.int32, (1, 128), 1)
    row_of = lax.broadcasted_iota(jnp.int32, (16, 128), 0)
    cell_of = row_of // 4 * share + row_of % 4
    cell_x = jnp.where(row_of % 4 < share, cell_of // CY, -8).astype(f32)
    cell_y = (cell_of % CY).astype(f32)
    cell_z = lax.broadcasted_iota(jnp.int32, (near_cells, 128), 0).astype(f32) - 1.0
    blank = jnp.zeros((128 - near_cells, 128), bf16)

    own = 4 * tiles

    def edges(t):
        coord_x = jnp.clip(pos_ref[0, pl.ds(t, 1), :] * CX - 0.5, 0.0, CX - 1.0)
        coord_y = jnp.clip(pos_ref[1, pl.ds(t, 1), :] * CY - 0.5, 0.0, CY - 1.0)
        return coord_x, coord_y

    def deposit(t, carry):
        live = (slot < counts_ref[t]).astype(f32)
        mass = mass_ref[pl.ds(t, 1), :] * live
        for comp in range(3):
            shell_ref[own + t, comp:comp + 1, :] = pos_ref[comp, pl.ds(t, 1), :]
        shell_ref[own + t, 3:4, :] = mass
        coord_x, coord_y = edges(t)
        start = jnp.asarray(t, jnp.int32).astype(f32)
        coord_z = (start + pos_ref[2, pl.ds(t, 1), :]) * span - 0.5 - start * span
        plane = hat(coord_x, cell_x) * hat(coord_y, cell_y) * mass
        high, low = halves(plane)
        weight_high, weight_low = halves(hat(coord_z, cell_z))
        weight_ref[t, 0] = weight_high
        weight_ref[t, 1] = weight_low
        rho_ref[t] = stacked_dot(
            high,
            low,
            jnp.concatenate([weight_high, blank], axis=0),
            jnp.concatenate([weight_low, blank], axis=0),
            ((1,), (1,)),
        )
        return carry

    with scope("b_inwait"):
        for copy in copies[:3]:
            copy.wait()
    with scope("c_deposit"):
        lax.fori_loop(0, tiles, deposit, 0, unroll=4)

    quarter = lax.broadcasted_iota(jnp.int32, (8, 128), 1) // width
    lower, even_block = quarter < 2, quarter % 2 == 0

    def exchange(blocks):
        far = [pltpu.roll(b, 64, 1) for b in blocks]
        mixed = [
            jnp.where(lower, blocks[0], far[2]),
            jnp.where(lower, blocks[1], far[3]),
            jnp.where(lower, far[0], blocks[2]),
            jnp.where(lower, far[1], blocks[3]),
        ]
        result = []
        for pair in (0, 2):
            one, two = mixed[pair], mixed[pair + 1]
            result.append(jnp.where(even_block, one, pltpu.roll(two, width, 1)))
            result.append(jnp.where(even_block, pltpu.roll(one, 128 - width, 1), two))
        return result

    with scope("d_tabwait"):
        copies[3].wait()
    with scope("e_transform"):
        rho = [rho_ref[t] for t in range(tiles)]
        half = tiles // 2
        even = [rho[0]] + [rho[t] + rho[tiles - t] for t in range(1, half)] + [rho[half]]
        odd = {t: rho[t] - rho[tiles - t] for t in range(1, half)}
        cosines, sines = tile_waves(even, odd)
        for g in range(groups):
            pair = (cosines[g], sines[g]) if g else (cosines[0], cosines[half])
            high, low = halves(jnp.concatenate(pair, axis=1))
            waves = [
                jnp.concatenate([wave_ref[part, g, 0], blank, wave_ref[part, g, 1], blank], axis=0)
                for part in range(2)
            ]
            lines = stacked_dot(high, low, waves[0], waves[1])
            blocks = [lines[0:8], pltpu.roll(lines[0:8], 4, 0), lines[8:16], pltpu.roll(lines[8:16], 4, 0)]
            for i, block in enumerate(exchange(blocks)):
                spec_ref[g * pack + i] = block[0:4]

    def out_copy(d):
        return pltpu.make_async_remote_copy(
            src_ref=spec_ref.at[d, pl.ds(0, share)],
            dst_ref=got_ref.at[me, pl.ds(0, share)],
            send_sem=out_send,
            recv_sem=out_recv,
            device_id=d,
            device_id_type=LOGICAL,
        )

    def back_copy(d):
        return pltpu.make_async_remote_copy(
            src_ref=back_ref.at[d],
            dst_ref=home_ref.at[me],
            send_sem=back_send,
            recv_sem=back_recv.at[me // (count // 2)],
            device_id=d,
            device_id_type=LOGICAL,
        )

    def start_all(make):
        for_others(lambda d: make(d).start())

    def wait_all(rest, sem):
        pltpu.make_async_copy(rest, rest, sem).wait()

    with scope("f_barwait"):
        pl.semaphore_wait(barrier, count - 1)
    with scope("g_startout"):
        start_all(out_copy)
    halos = []
    for step_x in (-1, 0, 1):
        for step_y in (-1, 0, 1):
            if step_x == 0 and step_y == 0:
                continue
            slot_there = (1 - step_x) * 3 + 1 - step_y
            halos.append(
                pltpu.make_async_remote_copy(
                    src_ref=shell_ref.at[pl.ds(own, tiles)],
                    dst_ref=shell_ref.at[pl.ds(slot_there * tiles, tiles)],
                    send_sem=halo_send.at[slot_there],
                    recv_sem=halo_recv.at[slot_there],
                    device_id=place((row + step_x + rows) % rows, (col + step_y + cols) % cols),
                    device_id_type=MESH,
                )
            )
    got_ref[me] = spec_ref[me]

    theirs, pulls, strengths = (theirs_0, theirs_1), (pull_0, pull_1), (strength_0, strength_1)
    line_of = lax.broadcasted_iota(jnp.int32, (8, 128), 0)
    first_lines, one_line = line_of < 3, line_of == 3
    square_lines = (line_of > 3) & (line_of < 7)

    def thirds(x):
        high = x.astype(bf16).astype(f32)
        rest = x - high
        middle = rest.astype(bf16).astype(f32)
        return high, middle, rest - middle

    def spread(t, carry):
        tile = shell_ref[own + t]
        spot = jnp.where(first_lines, jnp.concatenate([tile, tile], axis=0) - 0.5, 0.0)
        norm = jnp.sum(spot * spot, axis=0, keepdims=True) + softening
        mine = jnp.where(one_line, norm, jnp.where(square_lines, 1.0, -2.0 * spot))
        high, middle, low = thirds(mine)
        terms = [high, high, middle, high, low, middle, jnp.zeros((80, 128), f32)]
        spread_ref[t] = jnp.transpose(jnp.concatenate(terms, axis=0), (1, 0)).astype(bf16)
        return carry

    with scope("i_spread"):
        lax.fori_loop(0, tiles // 2, spread, 0, unroll=2)
    with scope("h_starthalo"):
        for copy in halos:
            copy.start()
    with scope("i_spreadb"):
        lax.fori_loop(tiles // 2, tiles, spread, 0, unroll=2)

    def describe(t, theirs_ref, pull_ref):
        for n in range(listed):
            entry = list_ref[n, 0, t]
            group = lax.div(entry, tiles)
            layer = entry - group * tiles
            step_x = lax.div(group * 11, 32)
            step_y = group - 3 * step_x
            away = lax.rem(layer - t + 1 + tiles, tiles)
            tile = shell_ref[entry]
            shift = jnp.where(
                line_of % 4 == 0,
                step_x.astype(f32),
                jnp.where(line_of % 4 == 1, step_y.astype(f32), away.astype(f32)),
            )
            spot = jnp.concatenate([tile, tile], axis=0) + (shift - 1.5)
            theirs = jnp.where(
                first_lines, spot, jnp.where(one_line, 1.0, jnp.where(square_lines, spot * spot, 0.0))
            )
            high, middle, low = thirds(theirs)
            one = jnp.concatenate([high, middle], axis=0).astype(bf16)
            two = jnp.concatenate([high, low], axis=0).astype(bf16)
            theirs_ref[n] = jnp.concatenate([one, two, one], axis=0)
            pull = jnp.concatenate(halves(theirs * tile[3:4]), axis=0)
            pull_ref[n] = pull

    product = functools.partial(lax.dot_general, preferred_element_type=f32)

    def attract(t, theirs_ref, strength_ref):
        for n in range(0, listed, 2):
            square = product(
                spread_ref[t][:, :48],
                jnp.concatenate([theirs_ref[n], theirs_ref[n + 1]], axis=1),
                (((1,), (0,)), ((), ())),
            )
            root = lax.rsqrt(square)
            strength = jnp.exp2(square * (-1.0 / (split_scale * math.log(2.0)))) * (root * root * root)
            high, low = halves(strength)
            for k in range(2):
                at = slice(k * 128, (k + 1) * 128)
                strength_ref[2 * (n + k)] = high[:, at]
                strength_ref[2 * (n + k) + 1] = low[:, at]

    def collect(t, pull_ref, strength_ref):
        total = product(
            jnp.concatenate([strength_ref[i] for i in range(2 * listed)], axis=1),
            jnp.concatenate([pull_ref[i // 2] for i in range(2 * listed)], axis=1),
             (((1,), (1,)), ((), ())))
        total = jnp.transpose(total, (1, 0))
        total = total[0:8] + total[8:16]
        tile = shell_ref[own + t]
        spot = jnp.concatenate([tile, tile], axis=0) - 0.5
        short_ref[t] = (total - spot * total[3:4]) * (short_kick * math.exp(softening / split_scale))

    nx, ny = rows * CX, cols * CY
    copies[4].wait()
    copies[5].wait()
    with scope("i2_green"):
        row_in = lax.broadcasted_iota(jnp.int32, (width, nx * ny), 0)
        family, member = me // pack, me % pack
        residue = jnp.where(
            member < pack // 2, family, jnp.where(family == 0, tiles // 2, tiles - family)
        )
        mode_of = tiles * (member % (pack // 2) * modes + row_in % modes) + residue
        alone = mode_of == 0
        wave_z = jnp.where(alone & (row_in >= modes), NZ // 2, mode_of).astype(f32)
        kappa = lanes_ref[0:1, :] + 4.0 * jnp.sin(wave_z * (jnp.pi / NZ)) ** 2
        scale = jnp.where(alone, 0.5, 1.0) * (1.0 / (NZ * nx * ny))
        green = -jnp.exp(-smoothing * kappa) / (kappa + screening) * scale

    with scope("j_waitgot"):
        wait_all(got_ref.at[pl.ds(0, count - 1), pl.ds(0, share)], out_recv)
    with scope("k_plane"):
        copies[6].wait()
        copies[7].wait()
        turned = jnp.transpose(got_ref[...].reshape(count * 4, 128), (1, 0))
        mine = jnp.concatenate(
            [turned[a * width:(a + 1) * width] for a in range(pack)], axis=1
        )
        high, low = halves(mine)
        joined = lambda ref, part: jnp.concatenate([ref[part, i] for i in range(nx * ny // 128)], axis=1)
        waves = stacked_dot(high, low, joined(into_ref, 0), joined(into_ref, 1))
        high, low = halves(waves * green)
        plane = stacked_dot(high, low, joined(outof_ref, 0), joined(outof_ref, 1))
        sheet = jnp.transpose(jnp.concatenate([plane] * pack, axis=0), (1, 0))
        for r in range(rows):
            for v in range(ny // 8):
                pick = [
                    sheet[at:at + 8]
                    for at in (((r * CX - 1 + b) % nx) * ny + v * 8 for b in range(pack))
                ]
                window = jnp.where(
                    lower,
                    jnp.where(even_block, pick[0], pick[1]),
                    jnp.where(even_block, pick[2], pick[3]),
                )
                window_ref[r, (v + 1) * 8:(v + 2) * 8, :] = window
                if v == 0:
                    window_ref[r, 8 + ny:16 + ny, :] = window
                if v == ny // 8 - 1:
                    window_ref[r, 0:8, :] = window
        for r in range(rows):
            for c in range(cols):
                d = (r // size_z * size_y + c) * size_z + r % size_z
                back_ref[d] = window_ref[r, c * CY + 7:c * CY + 15, :]
    with scope("l_startback"):
        start_all(back_copy)
    kept = pltpu.make_async_copy(
        back_ref.at[me], home_ref.at[me], back_recv.at[me // (count // 2)]
    )
    kept.start()

    with scope("m_waithalo"):
        for copy in halos:
            copy.wait_recv()
    def pairs(k, carry):
        for odd in (0, 1):
            t = 2 * k + odd
            attract(t, theirs[odd], strengths[odd])
            collect(lax.rem(t + tiles - 1, tiles), pulls[1 - odd], strengths[1 - odd])
            describe(lax.rem(t + 1, tiles), theirs[1 - odd], pulls[1 - odd])
        return carry

    with scope("n_pairs"):
        describe(0, theirs[0], pulls[0])
        lax.fori_loop(0, tiles // 2, pairs, 0, unroll=8)
        collect(tiles - 1, pulls[1], strengths[1])
    copies[9].wait()

    def untwist(h, carry):
        near = (me // (count // 2) + h) % 2
        with scope("o_waithome"):
            wait_all(home_ref.at[pl.ds(0, count // 2)], back_recv.at[near])
        for i in range(groups // 2):
            g = near * (groups // 2) + i
            lines = exchange([home_ref[g * pack + k] for k in range(pack)])
            pulls = [lines[b - 1] - lines[b + 1] for b in (1, 2)]
            pulls += [pltpu.roll(lines[b], 1, 0) - pltpu.roll(lines[b], 7, 0) for b in (1, 2)]
            high, low = halves(jnp.concatenate(pulls + [lines[1], lines[2]], axis=0))
            part = joint_dot(
                high,
                low,
                jnp.concatenate([unwave_ref[0, g, 0], unwave_ref[0, g, 1]], axis=1),
                jnp.concatenate([unwave_ref[1, g, 0], unwave_ref[1, g, 1]], axis=1),
            )
            part_ref[g] = part[:, :128]
            part_ref[groups + g] = part[:, 128:]
        return carry

    with scope("p_lines"):
        lax.fori_loop(0, 2, untwist, 0)
    with scope("q_invert"):
        for f in range(3):
            at = slice(f * 16, (f + 1) * 16)
            even = [part_ref[g, at] for g in range(groups)] + [part_ref[groups, at]]
            odd = {g: part_ref[groups + g, at] for g in range(1, groups)}
            cosines, sines = tile_waves(even, odd)
            for t in range(tiles):
                if t % half == 0:
                    value = cosines[t]
                elif t < half:
                    value = cosines[t] + sines[t]
                else:
                    value = cosines[tiles - t] - sines[tiles - t]
                if f == 2:
                    value = pltpu.roll(value, 1, 1) - pltpu.roll(value, 127, 1)
                high, low = halves(value)
                field_ref[t, f * 16:(f + 1) * 16, :] = high
                field_ref[t, 48 + f * 16:48 + (f + 1) * 16, :] = low

    cell_near = lax.broadcasted_iota(jnp.int32, (8, 128), 0).astype(f32) - 1.0
    copies[8].wait()

    def interpolate(t, carry):
        coord_x, coord_y = edges(t)
        left, right = hat(coord_x, 0.0), hat(coord_x, 1.0)
        along = hat(coord_y, cell_near)
        here = stacked_dot(
            field_ref[t, 0:48],
            field_ref[t, 48:96],
            jnp.concatenate([weight_ref[t, 0], blank], axis=0),
            jnp.concatenate([weight_ref[t, 1], blank], axis=0),
        )
        live = (slot < counts_ref[t]).astype(f32)
        for f in range(3):
            mixed = here[f * 16:f * 16 + 8] * left + here[f * 16 + 8:f * 16 + 16] * right
            pull = jnp.sum(mixed * along, axis=0, keepdims=True)
            at = (f, pl.ds(t, 1), slice(None))
            out_ref[at] = vel_ref[at] + live * (long_kick * pull + short_ref[t, f:f + 1, :])
        return carry

    with scope("r_interp"):
        lax.fori_loop(0, tiles, interpolate, 0, unroll=16)
    with scope("s_tail"):
        for copy in halos:
            copy.wait_send()
        wait_all(got_ref.at[pl.ds(0, count - 1), pl.ds(0, share)], out_send)
        wait_all(home_ref.at[pl.ds(0, count - 1)], back_send)


def fused_shards(sizes, positions, masses, velocities, tile_counts, neighbour_list):
    size_x, size_y, size_z, tiles, listed = sizes
    rows, cols = size_x * size_z, size_y
    count = rows * cols
    groups = tiles // 2
    near_cells = -(-(NZ // tiles + 3) // 16) * 16
    with jax.ensure_compile_time_eval():
        wave, unwave, into, outof, lanes = tables(size_x, size_y, size_z, tiles)
    anywhere = pl.BlockSpec(memory_space=pl.ANY)
    dma = pltpu.SemaphoreType.DMA
    kicked = pl.pallas_call(
        functools.partial(kick_kernel, sizes),
        out_shape=pltpu.VMEM((3, tiles, 128), f32),
        in_specs=[anywhere] * 10,
        out_specs=pl.BlockSpec(memory_space=pltpu.VMEM),
        scratch_shapes=[
            pltpu.VMEM((3, tiles, 128), f32),
            pltpu.VMEM((tiles, 128), f32),
            pltpu.VMEM((3, tiles, 128), f32),
            pltpu.VMEM(lanes.shape, f32),
            pltpu.SMEM((tiles,), jnp.int32),
            pltpu.SMEM((listed, 1, tiles), jnp.int32),
            pltpu.VMEM(wave.shape, bf16),
            pltpu.VMEM(into.shape, bf16),
            pltpu.VMEM(outof.shape, bf16),
            pltpu.VMEM(unwave.shape, bf16),
            pltpu.VMEM((9 * tiles, 4, 128), f32),
            pltpu.VMEM((tiles, 16, 128), f32),
            pltpu.VMEM((tiles, 2, near_cells, 128), bf16),
            pltpu.VMEM((count, 4, 128), f32),
            pltpu.VMEM((count, 4, 128), f32),
            pltpu.VMEM((rows, cols * CY + 16, 128), f32),
            pltpu.VMEM((count, 8, 128), f32),
            pltpu.VMEM((count, 8, 128), f32),
            pltpu.VMEM((2 * groups, 48, 128), f32),
            pltpu.VMEM((tiles, 96, 128), bf16),
            pltpu.VMEM((tiles, 128, 128), bf16),
            pltpu.VMEM((listed, 48, 128), bf16),
            pltpu.VMEM((listed, 48, 128), bf16),
            pltpu.VMEM((listed, 16, 128), bf16),
            pltpu.VMEM((listed, 16, 128), bf16),
            pltpu.VMEM((2 * listed, 128, 128), bf16),
            pltpu.VMEM((2 * listed, 128, 128), bf16),
            pltpu.VMEM((tiles, 8, 128), f32),
            dma((10,)),
            dma((9,)),
            dma((9,)),
            dma,
            dma,
            dma,
            dma((2,)),
        ],
        compiler_params=pltpu.CompilerParams(collective_id=0, has_side_effects=True),
        name="kick",
    )(
        jnp.transpose(positions[0, 0], (1, 0, 2)),
        masses.reshape(tiles, 128),
        jnp.transpose(velocities[0, 0], (1, 0, 2)),
        lanes,
        tile_counts.reshape(tiles),
        jnp.transpose(neighbour_list[0], (2, 0, 1)),
        wave,
        into,
        outof,
        unwave,
    )
    return jnp.transpose(kicked, (1, 0, 2))[None, None]


def fits(sizes):
    size_x, size_y, size_z, tiles, listed = sizes
    count = size_x * size_y * size_z
    if CX != 2 or CY != 6 or count != 32 or tiles != 16 or size_y * CY % 8:
        return False
    return NZ // 2 == 16 * count and NZ // tiles + 3 < 127


def solution(mesh):
    placed = (
        P(("gx", "gz"), "gy", None, None, None),
        P(("gx", "gz"), "gy", None, None),
        P(("gx", "gz"), "gy", None, None, None),
        P(("gx", "gz"), "gy", None),
        P(("gx", "gz"), "gy", None, None),
    )

    def local(positions, masses, velocities, tile_counts, neighbour_list):
        sizes = tuple(mesh.shape[axis] for axis in ("gx", "gy", "gz"))
        sizes = sizes + (positions.shape[2], neighbour_list.shape[3])
        part = functools.partial(fused_shards, sizes) if fits(sizes) else shards
        return part(positions, masses, velocities, tile_counts, neighbour_list)

    return jax.shard_map(
        local,
        mesh=mesh,
        in_specs=placed,
        out_specs=P(("gx", "gz"), "gy", None, None, None),
        check_vma=False,
    )
```

```python
import contextlib
import functools
import math

import jax
import jax.numpy as jnp
import numpy as np
from jax import lax
from jax.experimental import pallas as pl
from jax.experimental.pallas import tpu as pltpu
from jax.sharding import PartitionSpec as P

CX = 2
CY = 6
NZ = 1024


smoothing = 0.1
screening = 0.01
split_scale = 2.0
softening = 0.05
long_kick = 1.0
short_kick = 0.05
highest = lax.Precision.HIGHEST


def padded(cells, sides, width):
    for axis, dim in sides:
        count = lax.axis_size(axis)
        head = lax.slice_in_dim(cells, 0, width, axis=dim)
        tail = lax.slice_in_dim(cells, cells.shape[dim] - width, cells.shape[dim], axis=dim)
        cells = jnp.concatenate(
            [
                lax.ppermute(tail, axis, [(i, (i + 1) % count) for i in range(count)]),
                cells,
                lax.ppermute(head, axis, [((i + 1) % count, i) for i in range(count)]),
            ],
            axis=dim,
        )
    return cells


def wave_terms(length, first_index, extent):
    wavenum = (first_index + jnp.arange(extent, dtype=jnp.int32)).astype(jnp.float32)
    angles = wavenum * (2.0 * jnp.pi / length)
    return (4.0 * jnp.sin(0.5 * angles) ** 2, jnp.sin(angles))


def cloud_stencil(positions, cells_x, cells_y, cells_z, tiles):
    span = cells_z // tiles
    tile_row = jnp.arange(tiles, dtype=jnp.int32)[:, None]
    coord_x = positions[..., 0, :] * cells_x - 0.5
    base_x = jnp.clip(jnp.floor(coord_x), 0, cells_x - 2)
    frac_x = jnp.clip(coord_x - base_x, 0.0, 1.0)
    coord_y = positions[..., 1, :] * cells_y - 0.5
    base_y = jnp.clip(jnp.floor(coord_y), 0, cells_y - 2)
    frac_y = jnp.clip(coord_y - base_y, 0.0, 1.0)
    coord_z = (tile_row + positions[..., 2, :]) * span - 0.5
    base_z = jnp.floor(coord_z)
    frac_z = coord_z - base_z
    index_x = base_x.astype(jnp.int32)
    index_y = base_y.astype(jnp.int32)
    index_z = base_z.astype(jnp.int32) % cells_z
    cell_list = []
    weight_list = []
    for offset_x in (0, 1):
        for offset_y in (0, 1):
            for offset_z in (0, 1):
                weight_x = frac_x if offset_x else 1.0 - frac_x
                weight_y = frac_y if offset_y else 1.0 - frac_y
                weight_z = frac_z if offset_z else 1.0 - frac_z
                cell_list.append(
                    ((index_x + offset_x) * cells_y + index_y + offset_y) * cells_z
                    + (index_z + offset_z) % cells_z
                )
                weight_list.append(weight_x * weight_y * weight_z)
    return (jnp.stack(cell_list, axis=-2), jnp.stack(weight_list, axis=-2))


def pair_accel(receivers, sources, shifts):
    parts = []
    for comp in range(3):
        parts.append(
            shifts[:, :, comp, None, None]
            + sources[:, :, comp, None, :]
            - receivers[:, None, comp, :, None]
        )
    square = parts[0] * parts[0] + parts[1] * parts[1] + parts[2] * parts[2]
    strength = (
        sources[:, :, 3, None, :] * jnp.exp(-square / split_scale) * (square + softening) ** (-1.5)
    )
    return jnp.stack([jnp.sum(strength * parts[comp], axis=(1, 3)) for comp in range(3)], axis=1)


def split_length(length):
    divisor = 1
    for factor in range(1, math.isqrt(length) + 1):
        if length % factor == 0:
            divisor = factor
    return divisor


def dft_table(length):
    indices = jnp.arange(length, dtype=jnp.int32)
    phases = indices[:, None] * indices[None, :] % length
    angles = phases.astype(jnp.float32) * (2.0 * jnp.pi / length)
    return (jnp.cos(angles), jnp.sin(angles))


def twiddle_table(outer, inner):
    length = outer * inner
    phases = (
        jnp.arange(outer, dtype=jnp.int32)[:, None]
        * jnp.arange(inner, dtype=jnp.int32)[None, :]
        % length
    )
    angles = phases.astype(jnp.float32) * (2.0 * jnp.pi / length)
    return (jnp.cos(angles), jnp.sin(angles))


def complex_mix(real, imag, cosine, sine_table, sign, form):
    real_cos = jnp.einsum(form, real, cosine, precision=highest)
    real_sin = jnp.einsum(form, real, sine_table, precision=highest)
    imag_cos = jnp.einsum(form, imag, cosine, precision=highest)
    imag_sin = jnp.einsum(form, imag, sine_table, precision=highest)
    return (real_cos - sign * imag_sin, imag_cos + sign * real_sin)


def transform_last(real, imag, sign):
    length = real.shape[-1]
    outer = split_length(length)
    inner = length // outer
    leading = real.shape[:-1]
    real = real.reshape(leading + (outer, inner))
    imag = imag.reshape(leading + (outer, inner))
    cos_outer, sin_outer = dft_table(outer)
    real, imag = complex_mix(real, imag, cos_outer, sin_outer, sign, "...pq,pk->...kq")
    turn_cos, turn_sin = twiddle_table(outer, inner)
    real, imag = (
        real * turn_cos - sign * imag * turn_sin,
        imag * turn_cos + sign * real * turn_sin,
    )
    cos_inner, sin_inner = dft_table(inner)
    real, imag = complex_mix(real, imag, cos_inner, sin_inner, sign, "...kq,qm->...mk")
    return (real.reshape(leading + (length,)), imag.reshape(leading + (length,)))


def transform_axis(fields, axis, sign):
    real = jnp.moveaxis(fields[:, 0], axis, -1)
    imag = jnp.moveaxis(fields[:, 1], axis, -1)
    real, imag = transform_last(real, imag, sign)
    return jnp.stack([jnp.moveaxis(real, -1, axis), jnp.moveaxis(imag, -1, axis)], axis=1)


def rotate(fields, factor):
    return jnp.stack([factor * fields[:, 1], -factor * fields[:, 0]], axis=1)


def shards(positions, masses, velocities, tile_counts, neighbour_list):
    tiles = positions.shape[2]
    listed = neighbour_list.shape[3]
    slot_index = jnp.arange(128, dtype=jnp.int32)
    live_mask = (slot_index < tile_counts[..., None]).astype(jnp.float32)
    mass_live = masses * live_mask
    packed = jnp.concatenate([positions, mass_live[:, :, :, None, :]], axis=3)
    shell = padded(packed, ((("gx", "gz"), 0), ("gy", 1)), 1)
    cell_index, cloud_weights = cloud_stencil(positions, CX, CY, NZ, tiles)
    amounts = cloud_weights * mass_live[:, :, :, None, :]
    density = jax.ops.segment_sum(
        amounts.reshape(-1), cell_index.reshape(-1), num_segments=CX * CY * NZ
    ).reshape(CX, CY, NZ)
    spectrum = jnp.stack([density, jnp.zeros_like(density)], axis=0)[None]
    spectrum = transform_axis(spectrum, 3, -1.0)
    spectrum = lax.all_to_all(spectrum, "gy", split_axis=4, concat_axis=3, tiled=True)
    span_y = spectrum.shape[3]
    spectrum = transform_axis(spectrum, 2, -1.0)
    spectrum = lax.all_to_all(spectrum, ("gx", "gz"), split_axis=3, concat_axis=2, tiled=True)
    span_x = spectrum.shape[2]
    spectrum = transform_axis(spectrum, 1, -1.0)
    block_y = spectrum.shape[3]
    block_z = spectrum.shape[4]
    kappa_x, sine_x = wave_terms(span_x, 0, span_x)
    kappa_y, sine_y = wave_terms(span_y, lax.axis_index(("gx", "gz")) * block_y, block_y)
    kappa_z, sine_z = wave_terms(NZ, lax.axis_index("gy") * block_z, block_z)
    kappa_sum = kappa_x[:, None, None] + kappa_y[None, :, None] + kappa_z[None, None, :]
    potential = spectrum * (-jnp.exp(-smoothing * kappa_sum) / (kappa_sum + screening))
    fields = jnp.concatenate([rotate(potential, sine_x[:, None, None]), potential], axis=0)
    fields = transform_axis(fields, 1, 1.0) / span_x
    fields = lax.all_to_all(fields, ("gx", "gz"), split_axis=2, concat_axis=3, tiled=True)
    whole_sine_y = wave_terms(span_y, 0, span_y)[1]
    fields = jnp.concatenate(
        [fields[0:1], rotate(fields[1:2], whole_sine_y[None, :, None]), fields[1:2]], axis=0
    )
    fields = transform_axis(fields, 2, 1.0) / span_y
    fields = lax.all_to_all(fields, "gy", split_axis=3, concat_axis=4, tiled=True)
    whole_sine_z = wave_terms(NZ, 0, NZ)[1]
    fields = jnp.concatenate(
        [fields[0:2], rotate(fields[2:3], whole_sine_z[None, None, :])], axis=0
    )
    fields = transform_axis(fields, 3, 1.0) / NZ
    forces = fields[:, 0]
    flat_forces = forces.reshape(3, -1)
    picked = flat_forces[:, cell_index]
    long_accel = jnp.moveaxis(jnp.sum(cloud_weights[None] * picked, axis=4), 0, 3)
    flat_shell = shell.reshape(9 * tiles, 4, 128)
    own_list = neighbour_list[0, 0]
    sources = flat_shell[own_list]
    groups = own_list // tiles
    layers = own_list % tiles
    tile_row = jnp.arange(tiles, dtype=jnp.int32)[:, None]
    shifts = jnp.stack(
        [groups // 3 - 1, groups % 3 - 1, (layers - tile_row + 1) % tiles - 1], axis=-1
    ).astype(jnp.float32)
    short_accel = lax.map(
        lambda pieces: pair_accel(*pieces),
        (
            positions[0, 0].reshape(tiles, 1, 3, 128),
            sources.reshape(tiles, 1, listed, 4, 128),
            shifts.reshape(tiles, 1, listed, 3),
        ),
    )
    short_accel = short_accel.reshape(1, 1, tiles, 3, 128)
    return velocities + live_mask[:, :, :, None, :] * (
        long_kick * long_accel + short_kick * short_accel
    )


MESH = pl.DeviceIdType.MESH
LOGICAL = pl.DeviceIdType.LOGICAL
f32 = jnp.float32
bf16 = jnp.bfloat16


def halves(x):
    high = x.astype(bf16)
    return high, (x - high.astype(f32)).astype(bf16)


def dot3(a, b, dims=((1,), (0,))):
    dot = functools.partial(
        lax.dot_general, dimension_numbers=(dims, ((), ())), preferred_element_type=f32
    )
    return dot(a[0], b[0]) + dot(a[1], b[0]) + dot(a[0], b[1])


def scope(name):
    return contextlib.nullcontext()


def hat(coord, cell):
    return jnp.maximum(0.0, 1.0 - jnp.abs(coord - cell))


def np_halves(table):
    table = jnp.asarray(np.asarray(table, np.float32))
    return jnp.stack(halves(table))


def stacked_dot(high, low, table_high, table_low, dims=((1,), (0,))):
    dot = functools.partial(
        lax.dot_general, dimension_numbers=(dims, ((), ())), preferred_element_type=f32
    )
    rows = high.shape[0]
    both = dot(jnp.concatenate([high, low], axis=0), table_high)
    return both[:rows] + both[rows:] + dot(high, table_low)


def joint_dot(high, low, table_high, table_low):
    rows = high.shape[0]
    left = jnp.concatenate(
        [
            jnp.concatenate([high, high], axis=1),
            jnp.concatenate([low, jnp.zeros_like(low)], axis=1),
        ],
        axis=0,
    )
    both = lax.dot_general(
        left,
        jnp.concatenate([table_high, table_low], axis=0),
        (((1,), (0,)), ((), ())),
        preferred_element_type=f32,
    )
    return both[:rows] + both[rows:]


def tables(size_x, size_y, size_z, tiles):
    rows, cols = size_x * size_z, size_y
    count = rows * cols
    modes = NZ // 2 // count
    pack = 128 // (2 * modes)
    groups = tiles // 2
    lane = np.arange(128)
    member, imag, slot = lane // (2 * modes), lane % (2 * modes) >= modes, lane % modes
    cells = np.arange(128) - 1
    cells[127] = -2
    used = cells <= NZ // tiles + 1
    waves = []
    for g in range(groups):
        plus = member < pack // 2
        residue = np.where(plus, g, tiles - g if g else tiles // 2)
        mode = tiles * (member % (pack // 2) * modes + slot) + residue
        angle = 2 * np.pi * ((cells[:, None] * mode[None]) % NZ) / NZ
        direct = np.where(imag[None], -np.sin(angle), np.cos(angle))
        crossed = np.where(imag[None], np.cos(angle), np.sin(angle))
        crossed = np.where(plus[None], -crossed, crossed)
        if g == 0:
            nyquist = (mode == 0) & imag
            direct = np.where(nyquist[None], np.cos(np.pi * (cells % 2))[:, None], direct)
            direct, crossed = (
                np.where(plus[None], direct, 0.0),
                np.where(plus[None], 0.0, direct),
            )
        both = np.stack([direct, crossed])
        waves.append(np.where(used[None, :, None], both, 0.0).reshape(256, 128))
    nx, ny = rows * CX, cols * CY
    index = np.arange(4 * count * 4)
    device, row = index // 4 % count, index // (4 * count) * (CX * CY // 4) + index % 4
    real = index % 4 < CX * CY // 4
    place_x = device // (size_y * size_z) * size_z + device % size_z
    place_y = device // size_z % size_y
    here_x = np.where(real, place_x * CX + row // CY, 0)
    here_y = np.where(real, place_y * CY + row % CY, 0)
    wave_x, wave_y = np.arange(nx * ny) // ny, np.arange(nx * ny) % ny

    def cas(x, y):
        ax = 2 * np.pi * (x[:, None] * wave_x[None] % nx) / nx
        ay = 2 * np.pi * (y[:, None] * wave_y[None] % ny) / ny
        return (np.cos(ax) + np.sin(ax)) * (np.cos(ay) + np.sin(ay))

    into = cas(here_x, here_y) * real[:, None]
    outof = cas(wave_x, wave_y)
    lanes = np.zeros((8, nx * ny))
    lanes[:] = 4 * np.sin(np.pi * wave_x / nx) ** 2 + 4 * np.sin(np.pi * wave_y / ny) ** 2
    waves = np.stack(waves)
    unwaves = waves.reshape(groups, 2, 128, 128).transpose(0, 1, 3, 2)
    near_cells = -(-(NZ // tiles + 3) // 16) * 16
    waves = waves.reshape(groups, 2, 128, 128)[:, :, :near_cells]
    return np_halves(waves), np_halves(unwaves), np_halves(lane_tiles(into)), np_halves(lane_tiles(outof)), jnp.asarray(lanes, f32)


def lane_tiles(table):
    return np.stack(np.split(table, table.shape[1] // 128, axis=1))


def tile_waves(even, odd):
    half = len(even) - 1
    ring, quarter = 2 * half, half // 2

    def total(terms):
        result = None
        for factor, value in terms:
            if abs(factor) < 1e-12:
                continue
            if abs(abs(factor) - 1.0) < 1e-12:
                if result is None:
                    result = value if factor > 0 else -value
                else:
                    result = result + value if factor > 0 else result - value
            else:
                part = value * float(abs(factor))
                if result is None:
                    result = part if factor > 0 else -part
                else:
                    result = result + part if factor > 0 else result - part
        return result

    sums = [even[t] + even[half - t] for t in range(quarter)]
    gaps = [even[t] - even[half - t] for t in range(quarter)]
    odd_sums = {t: odd[t] + odd[half - t] for t in range(1, quarter)}
    odd_gaps = {t: odd[t] - odd[half - t] for t in range(1, quarter)}
    cosines, sines = [], {}
    for r in range(half + 1):
        cos = [math.cos(2 * math.pi * r * t / ring) for t in range(quarter + 1)]
        sin = [math.sin(2 * math.pi * r * t / ring) for t in range(quarter + 1)]
        terms = [(cos[t], (gaps if r % 2 else sums)[t]) for t in range(quarter)]
        if r % 2 == 0:
            terms.append((cos[quarter], even[quarter]))
        cosines.append(total(terms))
        if 0 < r < half:
            terms = [(sin[t], (odd_sums if r % 2 else odd_gaps)[t]) for t in range(1, quarter)]
            if r % 2:
                terms.append((sin[quarter], odd[quarter]))
            sines[r] = total(terms)
    return cosines, sines


def kick_kernel(
    sizes,
    pos_hbm, mass_hbm, vel_hbm, lanes_hbm, counts_hbm, list_hbm, wave_hbm, into_hbm, outof_hbm, unwave_hbm,
    out_ref,
    pos_ref, mass_ref, vel_ref, lanes_ref, counts_ref, list_ref, wave_ref, into_ref, outof_ref, unwave_ref,
    shell_ref, rho_ref, weight_ref, spec_ref, got_ref, window_ref,
    back_ref, home_ref, part_ref, field_ref, spread_ref, theirs_0, theirs_1, pull_0, pull_1, strength_0, strength_1, short_ref,
    input_sem, halo_send, halo_recv, out_send, out_recv, back_send, back_recv,
):
    size_x, size_y, size_z, tiles, listed = sizes
    rows, cols = size_x * size_z, size_y
    count = rows * cols
    modes = NZ // 2 // count
    width = 2 * modes
    pack = 128 // width
    groups = tiles // 2
    span = NZ // tiles
    near_cells = -(-(span + 3) // 16) * 16
    share = CX * CY // 4
    flat = size_y * size_z
    gx, gy, gz = lax.axis_index("gx"), lax.axis_index("gy"), lax.axis_index("gz")
    row, col = gx * size_z + gz, gy
    me = (gx * size_y + gy) * size_z + gz

    copies = [
        pltpu.make_async_copy(a, b, input_sem.at[i])
        for i, (a, b) in enumerate(
            (
                (pos_hbm, pos_ref),
                (mass_hbm, mass_ref),
                (counts_hbm, counts_ref),
                (wave_hbm, wave_ref),
                (list_hbm, list_ref),
                (lanes_hbm, lanes_ref),
                (into_hbm, into_ref),
                (outof_hbm, outof_ref),
                (vel_hbm, vel_ref),
                (unwave_hbm, unwave_ref),
            )
        )
    ]
    def place(r, c):
        return (r // size_z, c, r % size_z)

    first = size_x - 1 - gx
    second = lax.rem(gx + size_x // 2, size_x)
    third = size_x - 1 - second
    spot_here = gy * size_z + gz

    turns = [lax.rem(spot_here + i, flat) for i in range(flat)]

    def for_others(act):
        def some(members):
            def step(p, carry):
                if size_x == 4:
                    plane = jnp.where(
                        p == 0, first, jnp.where(p == 1, second, jnp.where(p == 2, third, gx))
                    )
                else:
                    plane = lax.rem(gx + p + 1, size_x)
                for i in members:
                    act(plane * flat + turns[i])
                return carry

            return step

        lax.fori_loop(0, size_x, some(range(1, flat)), 0)
        lax.fori_loop(0, size_x - 1, some(range(1)), 0)

    got_ref[...] = jnp.zeros((count, 4, 128), f32)
    barrier = pltpu.get_barrier_semaphore()

    with scope("a_greet"):
        for_others(
            lambda d: pl.semaphore_signal(barrier, inc=1, device_id=d, device_id_type=LOGICAL)
        )
    for copy in copies:
        copy.start()

    slot = lax.broadcasted_iota(jnp.int32, (1, 128), 1)
    row_of = lax.broadcasted_iota(jnp.int32, (16, 128), 0)
    cell_of = row_of // 4 * share + row_of % 4
    cell_x = jnp.where(row_of % 4 < share, cell_of // CY, -8).astype(f32)
    cell_y = (cell_of % CY).astype(f32)
    cell_z = lax.broadcasted_iota(jnp.int32, (near_cells, 128), 0).astype(f32) - 1.0
    blank = jnp.zeros((128 - near_cells, 128), bf16)

    own = 4 * tiles

    def edges(t):
        coord_x = jnp.clip(pos_ref[0, pl.ds(t, 1), :] * CX - 0.5, 0.0, CX - 1.0)
        coord_y = jnp.clip(pos_ref[1, pl.ds(t, 1), :] * CY - 0.5, 0.0, CY - 1.0)
        return coord_x, coord_y

    def deposit(t, carry):
        live = (slot < counts_ref[t]).astype(f32)
        mass = mass_ref[pl.ds(t, 1), :] * live
        for comp in range(3):
            shell_ref[own + t, comp:comp + 1, :] = pos_ref[comp, pl.ds(t, 1), :]
        shell_ref[own + t, 3:4, :] = mass
        coord_x, coord_y = edges(t)
        start = jnp.asarray(t, jnp.int32).astype(f32)
        coord_z = (start + pos_ref[2, pl.ds(t, 1), :]) * span - 0.5 - start * span
        plane = hat(coord_x, cell_x) * hat(coord_y, cell_y) * mass
        high, low = halves(plane)
        weight_high, weight_low = halves(hat(coord_z, cell_z))
        weight_ref[t, 0] = weight_high
        weight_ref[t, 1] = weight_low
        rho_ref[t] = stacked_dot(
            high,
            low,
            jnp.concatenate([weight_high, blank], axis=0),
            jnp.concatenate([weight_low, blank], axis=0),
            ((1,), (1,)),
        )
        return carry

    with scope("b_inwait"):
        for copy in copies[:3]:
            copy.wait()
    with scope("c_deposit"):
        lax.fori_loop(0, tiles, deposit, 0, unroll=4)

    quarter = lax.broadcasted_iota(jnp.int32, (8, 128), 1) // width
    lower, even_block = quarter < 2, quarter % 2 == 0

    def exchange(blocks):
        far = [pltpu.roll(b, 64, 1) for b in blocks]
        mixed = [
            jnp.where(lower, blocks[0], far[2]),
            jnp.where(lower, blocks[1], far[3]),
            jnp.where(lower, far[0], blocks[2]),
            jnp.where(lower, far[1], blocks[3]),
        ]
        result = []
        for pair in (0, 2):
            one, two = mixed[pair], mixed[pair + 1]
            result.append(jnp.where(even_block, one, pltpu.roll(two, width, 1)))
            result.append(jnp.where(even_block, pltpu.roll(one, 128 - width, 1), two))
        return result

    with scope("d_tabwait"):
        copies[3].wait()
    with scope("e_transform"):
        rho = [rho_ref[t] for t in range(tiles)]
        half = tiles // 2
        even = [rho[0]] + [rho[t] + rho[tiles - t] for t in range(1, half)] + [rho[half]]
        odd = {t: rho[t] - rho[tiles - t] for t in range(1, half)}
        cosines, sines = tile_waves(even, odd)
        for g in range(groups):
            pair = (cosines[g], sines[g]) if g else (cosines[0], cosines[half])
            high, low = halves(jnp.concatenate(pair, axis=1))
            waves = [
                jnp.concatenate([wave_ref[part, g, 0], blank, wave_ref[part, g, 1], blank], axis=0)
                for part in range(2)
            ]
            lines = stacked_dot(high, low, waves[0], waves[1])
            blocks = [lines[0:8], pltpu.roll(lines[0:8], 4, 0), lines[8:16], pltpu.roll(lines[8:16], 4, 0)]
            for i, block in enumerate(exchange(blocks)):
                spec_ref[g * pack + i] = block[0:4]

    def out_copy(d):
        return pltpu.make_async_remote_copy(
            src_ref=spec_ref.at[d, pl.ds(0, share)],
            dst_ref=got_ref.at[me, pl.ds(0, share)],
            send_sem=out_send,
            recv_sem=out_recv,
            device_id=d,
            device_id_type=LOGICAL,
        )

    def back_copy(d):
        return pltpu.make_async_remote_copy(
            src_ref=back_ref.at[d],
            dst_ref=home_ref.at[me],
            send_sem=back_send,
            recv_sem=back_recv.at[me // (count // 2)],
            device_id=d,
            device_id_type=LOGICAL,
        )

    def start_all(make):
        for_others(lambda d: make(d).start())

    def wait_all(rest, sem):
        pltpu.make_async_copy(rest, rest, sem).wait()

    with scope("f_barwait"):
        pl.semaphore_wait(barrier, count - 1)
    with scope("g_startout"):
        start_all(out_copy)
    halos = []
    for step_x in (-1, 0, 1):
        for step_y in (-1, 0, 1):
            if step_x == 0 and step_y == 0:
                continue
            slot_there = (1 - step_x) * 3 + 1 - step_y
            halos.append(
                pltpu.make_async_remote_copy(
                    src_ref=shell_ref.at[pl.ds(own, tiles)],
                    dst_ref=shell_ref.at[pl.ds(slot_there * tiles, tiles)],
                    send_sem=halo_send.at[slot_there],
                    recv_sem=halo_recv.at[slot_there],
                    device_id=place((row + step_x + rows) % rows, (col + step_y + cols) % cols),
                    device_id_type=MESH,
                )
            )
    got_ref[me] = spec_ref[me]

    theirs, pulls, strengths = (theirs_0, theirs_1), (pull_0, pull_1), (strength_0, strength_1)
    line_of = lax.broadcasted_iota(jnp.int32, (8, 128), 0)
    first_lines, one_line = line_of < 3, line_of == 3
    square_lines = (line_of > 3) & (line_of < 7)

    def thirds(x):
        high = x.astype(bf16).astype(f32)
        rest = x - high
        middle = rest.astype(bf16).astype(f32)
        return high, middle, rest - middle

    def spread(t, carry):
        tile = shell_ref[own + t]
        spot = jnp.where(first_lines, jnp.concatenate([tile, tile], axis=0) - 0.5, 0.0)
        norm = jnp.sum(spot * spot, axis=0, keepdims=True) + softening
        mine = jnp.where(one_line, norm, jnp.where(square_lines, 1.0, -2.0 * spot))
        high, middle, low = thirds(mine)
        terms = [high, high, middle, high, low, middle, jnp.zeros((80, 128), f32)]
        spread_ref[t] = jnp.transpose(jnp.concatenate(terms, axis=0), (1, 0)).astype(bf16)
        return carry

    with scope("i_spread"):
        lax.fori_loop(0, tiles // 2, spread, 0, unroll=2)
    with scope("h_starthalo"):
        for copy in halos:
            copy.start()
    with scope("i_spreadb"):
        lax.fori_loop(tiles // 2, tiles, spread, 0, unroll=2)

    def describe(t, theirs_ref, pull_ref):
        for n in range(listed):
            entry = list_ref[n, 0, t]
            group = lax.div(entry, tiles)
            layer = entry - group * tiles
            step_x = lax.div(group * 11, 32)
            step_y = group - 3 * step_x
            away = lax.rem(layer - t + 1 + tiles, tiles)
            tile = shell_ref[entry]
            shift = jnp.where(
                line_of % 4 == 0,
                step_x.astype(f32),
                jnp.where(line_of % 4 == 1, step_y.astype(f32), away.astype(f32)),
            )
            spot = jnp.concatenate([tile, tile], axis=0) + (shift - 1.5)
            theirs = jnp.where(
                first_lines, spot, jnp.where(one_line, 1.0, jnp.where(square_lines, spot * spot, 0.0))
            )
            high, middle, low = thirds(theirs)
            one = jnp.concatenate([high, middle], axis=0).astype(bf16)
            two = jnp.concatenate([high, low], axis=0).astype(bf16)
            theirs_ref[n] = jnp.concatenate([one, two, one], axis=0)
            pull = jnp.concatenate(halves(theirs * tile[3:4]), axis=0)
            pull_ref[n] = pull

    product = functools.partial(lax.dot_general, preferred_element_type=f32)

    def attract(t, theirs_ref, strength_ref):
        for n in range(0, listed, 2):
            square = product(
                spread_ref[t][:, :48],
                jnp.concatenate([theirs_ref[n], theirs_ref[n + 1]], axis=1),
                (((1,), (0,)), ((), ())),
            )
            root = lax.rsqrt(square)
            strength = jnp.exp2(square * (-1.0 / (split_scale * math.log(2.0)))) * (root * root * root)
            high, low = halves(strength)
            for k in range(2):
                at = slice(k * 128, (k + 1) * 128)
                strength_ref[2 * (n + k)] = high[:, at]
                strength_ref[2 * (n + k) + 1] = low[:, at]

    def collect(t, pull_ref, strength_ref):
        total = product(
            jnp.concatenate([strength_ref[i] for i in range(2 * listed)], axis=1),
            jnp.concatenate([pull_ref[i // 2] for i in range(2 * listed)], axis=1),
             (((1,), (1,)), ((), ())))
        total = jnp.transpose(total, (1, 0))
        total = total[0:8] + total[8:16]
        tile = shell_ref[own + t]
        spot = jnp.concatenate([tile, tile], axis=0) - 0.5
        short_ref[t] = (total - spot * total[3:4]) * (short_kick * math.exp(softening / split_scale))

    nx, ny = rows * CX, cols * CY
    copies[4].wait()
    copies[5].wait()
    with scope("i2_green"):
        row_in = lax.broadcasted_iota(jnp.int32, (width, nx * ny), 0)
        family, member = me // pack, me % pack
        residue = jnp.where(
            member < pack // 2, family, jnp.where(family == 0, tiles // 2, tiles - family)
        )
        mode_of = tiles * (member % (pack // 2) * modes + row_in % modes) + residue
        alone = mode_of == 0
        wave_z = jnp.where(alone & (row_in >= modes), NZ // 2, mode_of).astype(f32)
        kappa = lanes_ref[0:1, :] + 4.0 * jnp.sin(wave_z * (jnp.pi / NZ)) ** 2
        scale = jnp.where(alone, 0.5, 1.0) * (1.0 / (NZ * nx * ny))
        green = -jnp.exp(-smoothing * kappa) / (kappa + screening) * scale

    with scope("j_waitgot"):
        wait_all(got_ref.at[pl.ds(0, count - 1), pl.ds(0, share)], out_recv)
    with scope("k_plane"):
        copies[6].wait()
        copies[7].wait()
        turned = jnp.transpose(got_ref[...].reshape(count * 4, 128), (1, 0))
        mine = jnp.concatenate(
            [turned[a * width:(a + 1) * width] for a in range(pack)], axis=1
        )
        high, low = halves(mine)
        joined = lambda ref, part: jnp.concatenate([ref[part, i] for i in range(nx * ny // 128)], axis=1)
        waves = stacked_dot(high, low, joined(into_ref, 0), joined(into_ref, 1))
        high, low = halves(waves * green)
        plane = stacked_dot(high, low, joined(outof_ref, 0), joined(outof_ref, 1))
        sheet = jnp.transpose(jnp.concatenate([plane] * pack, axis=0), (1, 0))
        for r in range(rows):
            for v in range(ny // 8):
                pick = [
                    sheet[at:at + 8]
                    for at in (((r * CX - 1 + b) % nx) * ny + v * 8 for b in range(pack))
                ]
                window = jnp.where(
                    lower,
                    jnp.where(even_block, pick[0], pick[1]),
                    jnp.where(even_block, pick[2], pick[3]),
                )
                window_ref[r, (v + 1) * 8:(v + 2) * 8, :] = window
                if v == 0:
                    window_ref[r, 8 + ny:16 + ny, :] = window
                if v == ny // 8 - 1:
                    window_ref[r, 0:8, :] = window
        for r in range(rows):
            for c in range(cols):
                d = (r // size_z * size_y + c) * size_z + r % size_z
                back_ref[d] = window_ref[r, c * CY + 7:c * CY + 15, :]
    with scope("l_startback"):
        start_all(back_copy)
    kept = pltpu.make_async_copy(
        back_ref.at[me], home_ref.at[me], back_recv.at[me // (count // 2)]
    )
    kept.start()

    with scope("m_waithalo"):
        for copy in halos:
            copy.wait_recv()
    def pairs(k, carry):
        for odd in (0, 1):
            t = 2 * k + odd
            attract(t, theirs[odd], strengths[odd])
            collect(lax.rem(t + tiles - 1, tiles), pulls[1 - odd], strengths[1 - odd])
            describe(lax.rem(t + 1, tiles), theirs[1 - odd], pulls[1 - odd])
        return carry

    with scope("n_pairs"):
        describe(0, theirs[0], pulls[0])
        lax.fori_loop(0, tiles // 2, pairs, 0, unroll=8)
        collect(tiles - 1, pulls[1], strengths[1])
    copies[9].wait()

    def untwist(h, carry):
        near = (me // (count // 2) + h) % 2
        with scope("o_waithome"):
            wait_all(home_ref.at[pl.ds(0, count // 2)], back_recv.at[near])
        for i in range(groups // 2):
            g = near * (groups // 2) + i
            lines = exchange([home_ref[g * pack + k] for k in range(pack)])
            pulls = [lines[b - 1] - lines[b + 1] for b in (1, 2)]
            pulls += [pltpu.roll(lines[b], 1, 0) - pltpu.roll(lines[b], 7, 0) for b in (1, 2)]
            high, low = halves(jnp.concatenate(pulls + [lines[1], lines[2]], axis=0))
            part = joint_dot(
                high,
                low,
                jnp.concatenate([unwave_ref[0, g, 0], unwave_ref[0, g, 1]], axis=1),
                jnp.concatenate([unwave_ref[1, g, 0], unwave_ref[1, g, 1]], axis=1),
            )
            part_ref[g] = part[:, :128]
            part_ref[groups + g] = part[:, 128:]
        return carry

    with scope("p_lines"):
        lax.fori_loop(0, 2, untwist, 0)
    with scope("q_invert"):
        for f in range(3):
            at = slice(f * 16, (f + 1) * 16)
            even = [part_ref[g, at] for g in range(groups)] + [part_ref[groups, at]]
            odd = {g: part_ref[groups + g, at] for g in range(1, groups)}
            cosines, sines = tile_waves(even, odd)
            for t in range(tiles):
                if t % half == 0:
                    value = cosines[t]
                elif t < half:
                    value = cosines[t] + sines[t]
                else:
                    value = cosines[tiles - t] - sines[tiles - t]
                if f == 2:
                    value = pltpu.roll(value, 1, 1) - pltpu.roll(value, 127, 1)
                high, low = halves(value)
                field_ref[t, f * 16:(f + 1) * 16, :] = high
                field_ref[t, 48 + f * 16:48 + (f + 1) * 16, :] = low

    cell_near = lax.broadcasted_iota(jnp.int32, (8, 128), 0).astype(f32) - 1.0
    copies[8].wait()

    def interpolate(t, carry):
        coord_x, coord_y = edges(t)
        left, right = hat(coord_x, 0.0), hat(coord_x, 1.0)
        along = hat(coord_y, cell_near)
        here = stacked_dot(
            field_ref[t, 0:48],
            field_ref[t, 48:96],
            jnp.concatenate([weight_ref[t, 0], blank], axis=0),
            jnp.concatenate([weight_ref[t, 1], blank], axis=0),
        )
        live = (slot < counts_ref[t]).astype(f32)
        for f in range(3):
            mixed = here[f * 16:f * 16 + 8] * left + here[f * 16 + 8:f * 16 + 16] * right
            pull = jnp.sum(mixed * along, axis=0, keepdims=True)
            at = (f, pl.ds(t, 1), slice(None))
            out_ref[at] = vel_ref[at] + live * (long_kick * pull + short_ref[t, f:f + 1, :])
        return carry

    with scope("r_interp"):
        lax.fori_loop(0, tiles, interpolate, 0, unroll=16)
    with scope("s_tail"):
        for copy in halos:
            copy.wait_send()
        wait_all(got_ref.at[pl.ds(0, count - 1), pl.ds(0, share)], out_send)
        wait_all(home_ref.at[pl.ds(0, count - 1)], back_send)


def fused_shards(sizes, positions, masses, velocities, tile_counts, neighbour_list):
    size_x, size_y, size_z, tiles, listed = sizes
    rows, cols = size_x * size_z, size_y
    count = rows * cols
    groups = tiles // 2
    near_cells = -(-(NZ // tiles + 3) // 16) * 16
    with jax.ensure_compile_time_eval():
        wave, unwave, into, outof, lanes = tables(size_x, size_y, size_z, tiles)
    anywhere = pl.BlockSpec(memory_space=pl.ANY)
    dma = pltpu.SemaphoreType.DMA
    kicked = pl.pallas_call(
        functools.partial(kick_kernel, sizes),
        out_shape=pltpu.VMEM((3, tiles, 128), f32),
        in_specs=[anywhere] * 10,
        out_specs=pl.BlockSpec(memory_space=pltpu.VMEM),
        scratch_shapes=[
            pltpu.VMEM((3, tiles, 128), f32),
            pltpu.VMEM((tiles, 128), f32),
            pltpu.VMEM((3, tiles, 128), f32),
            pltpu.VMEM(lanes.shape, f32),
            pltpu.SMEM((tiles,), jnp.int32),
            pltpu.SMEM((listed, 1, tiles), jnp.int32),
            pltpu.VMEM(wave.shape, bf16),
            pltpu.VMEM(into.shape, bf16),
            pltpu.VMEM(outof.shape, bf16),
            pltpu.VMEM(unwave.shape, bf16),
            pltpu.VMEM((9 * tiles, 4, 128), f32),
            pltpu.VMEM((tiles, 16, 128), f32),
            pltpu.VMEM((tiles, 2, near_cells, 128), bf16),
            pltpu.VMEM((count, 4, 128), f32),
            pltpu.VMEM((count, 4, 128), f32),
            pltpu.VMEM((rows, cols * CY + 16, 128), f32),
            pltpu.VMEM((count, 8, 128), f32),
            pltpu.VMEM((count, 8, 128), f32),
            pltpu.VMEM((2 * groups, 48, 128), f32),
            pltpu.VMEM((tiles, 96, 128), bf16),
            pltpu.VMEM((tiles, 128, 128), bf16),
            pltpu.VMEM((listed, 48, 128), bf16),
            pltpu.VMEM((listed, 48, 128), bf16),
            pltpu.VMEM((listed, 16, 128), bf16),
            pltpu.VMEM((listed, 16, 128), bf16),
            pltpu.VMEM((2 * listed, 128, 128), bf16),
            pltpu.VMEM((2 * listed, 128, 128), bf16),
            pltpu.VMEM((tiles, 8, 128), f32),
            dma((10,)),
            dma((9,)),
            dma((9,)),
            dma,
            dma,
            dma,
            dma((2,)),
        ],
        compiler_params=pltpu.CompilerParams(collective_id=0, has_side_effects=True),
        name="kick",
    )(
        jnp.transpose(positions[0, 0], (1, 0, 2)),
        masses.reshape(tiles, 128),
        jnp.transpose(velocities[0, 0], (1, 0, 2)),
        lanes,
        tile_counts.reshape(tiles),
        jnp.transpose(neighbour_list[0], (2, 0, 1)),
        wave,
        into,
        outof,
        unwave,
    )
    return jnp.transpose(kicked, (1, 0, 2))[None, None]


def fits(sizes):
    size_x, size_y, size_z, tiles, listed = sizes
    count = size_x * size_y * size_z
    if CX != 2 or CY != 6 or count != 32 or tiles != 16 or size_y * CY % 8:
        return False
    return NZ // 2 == 16 * count and NZ // tiles + 3 < 127


def solution(mesh):
    placed = (
        P(("gx", "gz"), "gy", None, None, None),
        P(("gx", "gz"), "gy", None, None),
        P(("gx", "gz"), "gy", None, None, None),
        P(("gx", "gz"), "gy", None),
        P(("gx", "gz"), "gy", None, None),
    )

    def local(positions, masses, velocities, tile_counts, neighbour_list):
        sizes = tuple(mesh.shape[axis] for axis in ("gx", "gy", "gz"))
        sizes = sizes + (positions.shape[2], neighbour_list.shape[3])
        part = functools.partial(fused_shards, sizes) if fits(sizes) else shards
        return part(positions, masses, velocities, tile_counts, neighbour_list)

    return jax.shard_map(
        local,
        mesh=mesh,
        in_specs=placed,
        out_specs=P(("gx", "gz"), "gy", None, None, None),
        check_vma=False,
    )
```
